64 devices in a mesh: rep: 4 (over x, y), dp: 16 (over z, core).
Axes of the slice: x: 2, y: 2, z: 8, core: 2. Of those that a mesh axis runs over, the one named last changes fastest.
The devices are a block of a 4x4x8 slice.
Arguments:
- x: bfloat16 [64, 2048, 512], P(('rep', 'dp')), parts along dimension 0
- dy: bfloat16 [64, 2048, 512], P(('rep', 'dp')), parts along dimension 0
- wq: bfloat16 [2, 512, 512], P(None, 'dp')
- wk: bfloat16 [2, 512, 512], P(None, 'dp')
- wv: bfloat16 [2, 512, 512], P(None, 'dp')
- wo: bfloat16 [2, 512, 512], P(None, 'dp')
- w_gate: bfloat16 [2, 512, 2048], P(None, 'dp')
- w_up: bfloat16 [2, 512, 2048], P(None, 'dp')
- w_down: bfloat16 [2, 2048, 512], P(None, 'dp')
- m_wq: float32 [2, 512, 512], P(None, 'dp')
- m_wk: float32 [2, 512, 512], P(None, 'dp')
- m_wv: float32 [2, 512, 512], P(None, 'dp')
- m_wo: float32 [2, 512, 512], P(None, 'dp')
- m_w_gate: float32 [2, 512, 2048], P(None, 'dp')
- m_w_up: float32 [2, 512, 2048], P(None, 'dp')
- m_w_down: float32 [2, 2048, 512], P(None, 'dp')
- v_wq: float32 [2, 512, 512], P(None, 'dp')
- v_wk: float32 [2, 512, 512], P(None, 'dp')
- v_wv: float32 [2, 512, 512], P(None, 'dp')
- v_wo: float32 [2, 512, 512], P(None, 'dp')
- v_w_gate: float32 [2, 512, 2048], P(None, 'dp')
- v_w_up: float32 [2, 512, 2048], P(None, 'dp')
- v_w_down: float32 [2, 2048, 512], P(None, 'dp')
Outputs:
- output 1: bfloat16 [8, 512, 512], P('rep', 'dp'), parts along dimension 0
- output 2: bfloat16 [8, 512, 512], P('rep', 'dp'), parts along dimension 0
- output 3: bfloat16 [8, 512, 512], P('rep', 'dp'), parts along dimension 0
- output 4: bfloat16 [8, 512, 512], P('rep', 'dp'), parts along dimension 0
- output 5: bfloat16 [8, 512, 2048], P('rep', 'dp'), parts along dimension 0
- output 6: bfloat16 [8, 512, 2048], P('rep', 'dp'), parts along dimension 0
- output 7: bfloat16 [8, 2048, 512], P('rep', 'dp'), parts along dimension 0
- output 8: float32 [8, 512, 512], P('rep', 'dp'), parts along dimension 0
- output 9: float32 [8, 512, 512], P('rep', 'dp'), parts along dimension 0
- output 10: float32 [8, 512, 512], P('rep', 'dp'), parts along dimension 0
- output 11: float32 [8, 512, 512], P('rep', 'dp'), parts along dimension 0
- output 12: float32 [8, 512, 2048], P('rep', 'dp'), parts along dimension 0
- output 13: float32 [8, 512, 2048], P('rep', 'dp'), parts along dimension 0
- output 14: float32 [8, 2048, 512], P('rep', 'dp'), parts along dimension 0
- output 15: float32 [8, 512, 512], P('rep', 'dp'), parts along dimension 0
- output 16: float32 [8, 512, 512], P('rep', 'dp'), parts along dimension 0
- output 17: float32 [8, 512, 512], P('rep', 'dp'), parts along dimension 0
- output 18: float32 [8, 512, 512], P('rep', 'dp'), parts along dimension 0
- output 19: float32 [8, 512, 2048], P('rep', 'dp'), parts along dimension 0
- output 20: float32 [8, 512, 2048], P('rep', 'dp'), parts along dimension 0
- output 21: float32 [8, 2048, 512], P('rep', 'dp'), parts along dimension 0
There are 4 independent parts. The reference program is written for one: setup_inputs(seed, part) draws one part's arguments, and reference() takes and returns one part's arrays. A program takes and returns all parts, laid end to end along the dimension named above; an argument that names none is the same for every part.
All inputs are finite; a program needn't handle non-finite values.
Results may differ from the reference program's by a relative error of at most 0.0251.
Values are sent between devices in bfloat16 or wider.
A program may use at most 768 MiB of HBM per device.

```python
import jax
import jax.numpy as jnp
from jax import lax

SEQUENCES = 16
TOKENS = 2048
D = 512
HEADS = 4
KV_HEADS = 4
HEAD = 128
FF = 2048
LAYERS = 2
THETA = 10000
NAMES = ("wq", "wk", "wv", "wo", "w_gate", "w_up", "w_down")
SHAPES = {
    "wq": (LAYERS, D, HEADS * HEAD),
    "wk": (LAYERS, D, KV_HEADS * HEAD),
    "wv": (LAYERS, D, KV_HEADS * HEAD),
    "wo": (LAYERS, HEADS * HEAD, D),
    "w_gate": (LAYERS, D, FF),
    "w_up": (LAYERS, D, FF),
    "w_down": (LAYERS, FF, D),
}


def bump(key, n, height):
    away = (jnp.arange(n, dtype=jnp.int32) - jax.random.randint(key, (), 0, n, jnp.int32)) % n
    return jnp.where(away < n // 8, height, 1.0)


def together(key, own, strength):
    shared = jax.random.normal(key, own.shape[1:], jnp.float32)
    return (own + strength * shared) * lax.rsqrt(1 + strength * strength)


def setup_inputs(seed: int = 0, part: int = 0) -> dict:
    kx, kdy, ka, kb, kz, kf, kh, kl, *keys = jax.random.split(jax.random.key(seed), 8 + 3 * len(NAMES))
    kx, kdy, ka, kb = (jax.random.fold_in(k, part) for k in (kx, kdy, ka, kb))
    kw, km, kv = (keys[i::3] for i in range(3))
    shape = (SEQUENCES, TOKENS, D)
    much_x, much_dy = jax.random.uniform(kz, (2,), jnp.float32, 0.0, 1.0)
    loud = 2.0 ** jax.random.uniform(jax.random.fold_in(kz, 1), (), jnp.float32, -1.0, 2.0)
    layers = 2.0 ** jax.random.uniform(kl, (LAYERS, 1, 1), jnp.float32, -1.0, 1.0)
    times = {"wq": 1.0, "wk": 1.0, "wv": 2.0, "wo": layers, "w_gate": 1.0, "w_up": bump(kh, FF, 4.0), "w_down": layers}
    x = together(ka, jax.random.normal(kx, shape, jnp.float32), much_x) * bump(kf, D, 4.0)
    dy = together(kb, jax.random.normal(kdy, shape, jnp.float32), much_dy)
    drawn = {"x": x.astype(jnp.bfloat16), "dy": (loud * dy * (SEQUENCES * TOKENS) ** -0.5).astype(jnp.bfloat16)}
    for key, name in zip(kw, NAMES, strict=True):
        drawn[name] = (jax.random.normal(key, SHAPES[name], jnp.float32) * SHAPES[name][1] ** -0.5 * times[name]).astype(jnp.bfloat16)
    for key, name in zip(km, NAMES, strict=True):
        drawn[f"m_{name}"] = 0.1 * jax.random.normal(key, SHAPES[name], jnp.float32)
    for key, name in zip(kv, NAMES, strict=True):
        drawn[f"v_{name}"] = loud * loud * jax.random.uniform(key, SHAPES[name], jnp.float32, 0.2, 0.6)
    return drawn


def matmul(a, w):
    return jnp.dot(a, w, preferred_element_type=jnp.float32).astype(jnp.bfloat16)


def normed(h):
    wide = h.astype(jnp.float32)
    scale = lax.rsqrt(jnp.mean(wide**2, -1, keepdims=True) + 1e-6)
    return (wide * scale).astype(jnp.bfloat16)


def turned(t, theta):
    half = t.shape[-1] // 2
    angle = jnp.arange(t.shape[0], dtype=jnp.float32)[:, None] * theta ** (-jnp.arange(half, dtype=jnp.float32) / half)
    cos, sin = jnp.cos(angle)[:, None], jnp.sin(angle)[:, None]
    a, b = t[..., :half].astype(jnp.float32), t[..., half:].astype(jnp.float32)
    return jnp.concatenate([a * cos - b * sin, b * cos + a * sin], -1).astype(jnp.bfloat16)


def seen_by(q, k, v):
    tokens, kv = q.shape[0], k.shape[1]
    q = q.reshape(tokens, kv, -1, q.shape[-1])
    scores = jnp.einsum("tgsd,ugd->gstu", q.astype(jnp.float32), k.astype(jnp.float32)) * q.shape[-1] ** -0.5
    place = jnp.arange(tokens)
    weights = jax.nn.softmax(jnp.where(place[:, None] >= place, scores, -jnp.inf), -1).astype(jnp.bfloat16)
    return jnp.einsum("gstu,ugd->tgsd", weights.astype(jnp.float32), v.astype(jnp.float32)).astype(jnp.bfloat16).reshape(tokens, -1)


def layer(h, w):
    a = normed(h)
    q, k = (turned(matmul(a, w[name]).reshape(h.shape[0], -1, HEAD), THETA) for name in ("wq", "wk"))
    h = h + matmul(seen_by(q, k, matmul(a, w["wv"]).reshape(h.shape[0], -1, HEAD)), w["wo"])
    b = normed(h)
    gate = jnp.dot(b, w["w_gate"], preferred_element_type=jnp.float32)
    up = jnp.dot(b, w["w_up"], preferred_element_type=jnp.float32)
    return h + matmul((jax.nn.silu(gate) * up).astype(jnp.bfloat16), w["w_down"])


def adamw(w, m, v, g):
    m = 0.9 * m + 0.1 * g
    v = 0.95 * v + 0.05 * g * g
    step = m * lax.rsqrt(v + 1e-8) + 0.1 * w
    return (w - 0.02 * step).astype(jnp.bfloat16), m, v


def stack(weights, h):
    return lax.scan(lambda h, w: (layer(h, w), None), h, weights)[0]


def reference(x, dy, wq, wk, wv, wo, w_gate, w_up, w_down, m_wq, m_wk, m_wv, m_wo, m_w_gate, m_w_up, m_w_down, v_wq, v_wk, v_wv, v_wo, v_w_gate, v_w_up, v_w_down):
    weights = dict(zip(NAMES, (wq, wk, wv, wo, w_gate, w_up, w_down), strict=True))

    def take(so_far, sequence):
        h, by_y = sequence
        _, back = jax.vjp(stack, weights, h)
        by_weights, by_h = back(by_y)
        return jax.tree.map(lambda total, term: total + term.astype(jnp.float32), so_far, by_weights), by_h

    none_yet = {name: jnp.zeros(w.shape, jnp.float32) for name, w in weights.items()}
    by_weights, by_x = lax.scan(take, none_yet, (x, dy))
    gradients = [by_weights[name].astype(jnp.bfloat16).astype(jnp.float32) for name in NAMES]
    first = (m_wq, m_wk, m_wv, m_wo, m_w_gate, m_w_up, m_w_down)
    second = (v_wq, v_wk, v_wv, v_wo, v_w_gate, v_w_up, v_w_down)
    new = [adamw(weights[name].astype(jnp.float32), m, v, g) for name, m, v, g in zip(NAMES, first, second, gradients, strict=True)]
    return tuple(one[which] for which in range(3) for one in new)
```

```python
import functools

import jax
import jax.numpy as jnp
from jax import lax
from jax.experimental import pallas as pl
from jax.experimental.pallas import tpu as pltpu
from jax.sharding import PartitionSpec as P

F32, BF16 = jnp.float32, jnp.bfloat16
HEAD = 128
THETA = 10000
NEG = -1e30
HIDDEN = 2 * NEG
LOG2E = 1.4426950408889634
VMEM = 60 * 2**20


def dot(a, b, ca=1, cb=0):
    return lax.dot_general(a, b, (((ca,), (cb,)), ((), ())), preferred_element_type=F32)


def params(*semantics):
    return pltpu.CompilerParams(dimension_semantics=semantics, vmem_limit_bytes=VMEM)


def cost(flops, *arrays, exps=0):
    return pl.CostEstimate(flops=flops, transcendentals=exps, bytes_accessed=sum(a.size * a.dtype.itemsize for a in arrays))


def once(shape, index):
    return pl.BlockSpec(shape, index, pipeline_mode=pl.Buffered(1))


def inverse_rms(wide):
    return lax.rsqrt(jnp.mean(wide * wide, -1, keepdims=True) + 1e-6)


def whole(w_ref, piece, pieces=1):
    w = w_ref[:, piece] if pieces == 1 else w_ref[:, piece : piece + pieces]
    return w.reshape(-1, w.shape[-1])


def _qkv(h_ref, w_ref, cos_ref, sin_ref, q_ref, k_ref, v_ref):
    wide = h_ref[...].astype(F32)
    a = (wide * inverse_rms(wide)).astype(BF16)
    cos, sin = cos_ref[...], sin_ref[...]
    for piece, o_ref in enumerate((q_ref, k_ref, v_ref)):
        y = dot(a, whole(w_ref, piece)).astype(BF16)
        if piece == 2:
            o_ref[...] = y
            continue
        for at in range(0, y.shape[1], HEAD):
            t = y[:, at : at + HEAD].astype(F32)
            o_ref[:, at : at + HEAD] = (t * cos + pltpu.roll(t, HEAD // 2, 1) * sin).astype(BF16)


def qkv(h, w, cos, sin, t=512):
    s, d = h.shape
    n, _, rows, _ = w.shape
    row = pl.BlockSpec((t, d), lambda i: (i, 0))
    table = pl.BlockSpec((t, HEAD), lambda i: (i, 0))
    return pl.pallas_call(
        _qkv,
        grid=(s // t,),
        in_specs=[row, once((n, 3, rows, d), lambda i: (0, 0, 0, 0)), table, table],
        out_specs=[row] * 3,
        out_shape=[jax.ShapeDtypeStruct((s, d), BF16)] * 3,
        compiler_params=params("arbitrary"),
        cost_estimate=cost(6 * s * d * d, h, h, h, h),
        name="qkv",
    )(h, w, cos, sin)


def _attend(q_ref, k_ref, v_ref, h_ref, wo_ref, o_ref, lse_ref, h1_ref, top_s, mix_s, *, scale, bk):
    bq, width = q_ref.shape
    heads = width // HEAD
    i = pl.program_id(0)
    e = scale * LOG2E
    top_s[...] = jnp.full_like(top_s, NEG)
    mix_s[...] = jnp.zeros_like(mix_s)

    def block(at, keys, pieces, gap):
        here = pl.ds(at, keys)
        ones = jnp.ones((8, keys), BF16)
        work = [(n, a, w) for n in range(heads) for a, w in pieces]
        scores = [dot(k_ref[here, n * HEAD : (n + 1) * HEAD], q_ref[a : a + w, n * HEAD : (n + 1) * HEAD], 1, 1) for n, a, w in work]
        weights, keeps = [], []
        for (n, a, w), s in zip(work, scores):
            if gap == a:
                ok = lax.broadcasted_iota(jnp.int32, (keys, w), 1) + (a - gap) >= lax.broadcasted_iota(jnp.int32, (keys, w), 0)
                s = jnp.where(ok, s, HIDDEN)
            old = top_s[n : n + 1, a : a + w]
            top = jnp.maximum(old, s.max(axis=0, keepdims=True))
            top_s[n : n + 1, a : a + w] = top
            weights.append(jnp.exp2((s - top) * e).astype(BF16))
            keeps.append(jnp.exp2((old - top) * e))
        for (n, a, w), p, keep in zip(work, weights, keeps):
            values = jnp.concatenate([v_ref[here, n * HEAD : (n + 1) * HEAD].T, ones], axis=0)
            mix_s[n, :, a : a + w] = mix_s[n, :, a : a + w] * keep + dot(values, p)

    lax.fori_loop(0, i * (bq // bk), lambda j, _: block(j * bk, bk, [(0, bq)], None), None)
    half = bq // 2
    block(i * bq, half, [(0, half), (half, half)], 0)
    block(i * bq + half, half, [(half, half)], half)

    for n in range(heads):
        top, total = top_s[n : n + 1, :], mix_s[n, HEAD : HEAD + 1, :]
        o_ref[:, n * HEAD : (n + 1) * HEAD] = (mix_s[n, :HEAD, :] * (1 / total)).T.astype(BF16)
        lse_ref[n : n + 1, :] = top * e + jnp.log2(total)
    y = dot(o_ref[...], whole(wo_ref, 0)).astype(BF16)
    h1_ref[...] = h_ref[...] + y


def attend(q, k, v, h, w, bq=512, bk=512):
    s, d = q.shape
    n, _, rows, _ = w.shape
    heads = d // HEAD
    row = pl.BlockSpec((bq, d), lambda i: (i, 0))
    full = once((s, d), lambda i: (0, 0))
    return pl.pallas_call(
        functools.partial(_attend, scale=HEAD**-0.5, bk=bk),
        grid=(s // bq,),
        in_specs=[row, full, full, row, once((n, 1, rows, d), lambda i: (0, 3, 0, 0))],
        out_specs=[row, pl.BlockSpec((heads, bq), lambda i: (0, i)), row],
        out_shape=[jax.ShapeDtypeStruct((s, d), BF16), jax.ShapeDtypeStruct((heads, s), F32), jax.ShapeDtypeStruct((s, d), BF16)],
        scratch_shapes=[pltpu.VMEM((heads, bq), F32), pltpu.VMEM((heads, HEAD + 8, bq), F32)],
        compiler_params=params("arbitrary"),
        cost_estimate=cost(2 * s * s * d + 2 * s * d * d, q, k, v, q, q, exps=heads * s * s // 2),
        name="attend",
    )(q, k, v, h, w)


def _feed(h_ref, w_ref, out_ref, *, n_blocks):
    n, _, rows, d = w_ref.shape
    wide = h_ref[...].astype(F32)
    b = (wide * inverse_rms(wide)).astype(BF16)
    owners = n // n_blocks
    y = None
    for j in range(n_blocks):
        gate = dot(b, whole(w_ref, 4 + j))
        up = dot(b, whole(w_ref, 4 + n_blocks + j))
        act = (gate * (1 / (1 + jnp.exp(-gate))) * up).astype(BF16)
        down = w_ref[owners * j : owners * (j + 1), 4 + 2 * n_blocks :].reshape(d, d)
        part = dot(act, down)
        y = part if y is None else y + part
    out_ref[...] = h_ref[...] + y.astype(BF16)


def feed(h, w, n_blocks, t=512):
    s, d = h.shape
    row = pl.BlockSpec((t, d), lambda i: (i, 0))
    return pl.pallas_call(
        functools.partial(_feed, n_blocks=n_blocks),
        grid=(s // t,),
        in_specs=[row, once(w.shape, lambda i: (0, 0, 0, 0))],
        out_specs=row,
        out_shape=jax.ShapeDtypeStruct((s, d), BF16),
        compiler_params=params("arbitrary"),
        cost_estimate=cost(6 * s * d * d * n_blocks, h, h, w, exps=s * d * n_blocks),
        name="feed",
    )(h, w)


def norm_back(wide, by_normed):
    r = inverse_rms(wide)
    normed = wide * r
    return r * (by_normed - normed * jnp.mean(normed * by_normed, -1, keepdims=True))


def _feed_back(h_ref, dh_ref, wg_ref, wu_ref, wd_ref, out_ref, dw_ref, b_s, bt_s, dht_s, act_s, dgate_s, dup_s, db_s, dw_s, sems, *, t):
    j, blocks = pl.program_id(0), pl.num_programs(0)
    s, d = h_ref.shape
    n, _, rows, _ = wg_ref.shape
    part = wd_ref.shape[0]
    wg, wu, wd = (r[...].reshape(d, d) for r in (wg_ref, wu_ref, wd_ref))

    def stores(j):
        per = n // part
        down = dw_ref.at[pl.ds(j * part, part), 4 + 2 * per : 4 + 3 * per]
        places = (dw_ref.at[:, 4 + j], dw_ref.at[:, 4 + per + j], down)
        return [pltpu.make_async_copy(dw_s.at[i].reshape(p.shape), p, sems.at[i]) for i, p in enumerate(places)]

    @pl.when(j == 0)
    def _():
        for a in range(0, s, t):
            wide = h_ref[a : a + t, :].astype(F32)
            b = (wide * inverse_rms(wide)).astype(BF16)
            b_s[a : a + t, :] = b
            bt_s[:, a : a + t] = b.T
            dht_s[:, a : a + t] = dh_ref[a : a + t, :].T
        db_s[...] = jnp.zeros_like(db_s)

    def tokens(i, _):
        here = pl.ds(pl.multiple_of(i * t, t), t)
        b, dh = b_s[here, :], dh_ref[here, :]
        gate, up = dot(b, wg), dot(b, wu)
        dact = dot(dh, wd, 1, 1).astype(BF16).astype(F32)
        sig = 1 / (1 + jnp.exp(-gate))
        silu = gate * sig
        act_s[here, :] = (silu * up).astype(BF16)
        dup = (dact * silu).astype(BF16)
        dgate = (dact * up * (sig + silu * (1 - sig))).astype(BF16)
        dup_s[here, :] = dup
        dgate_s[here, :] = dgate
        db_s[here, :] += dot(dgate, wg, 1, 1) + dot(dup, wu, 1, 1)

    lax.fori_loop(0, s // t, tokens, None)

    @pl.when(j > 0)
    def _():
        for copy in stores(j - 1):
            copy.wait()

    dw_s[0] = dot(bt_s[...], dgate_s[...]).astype(BF16).reshape(n, rows, d)
    dw_s[1] = dot(bt_s[...], dup_s[...]).astype(BF16).reshape(n, rows, d)
    dw_s[2] = dot(dht_s[...], act_s[...]).T.astype(BF16).reshape(n, rows, d)
    for copy in stores(j):
        copy.start()

    @pl.when(j == blocks - 1)
    def _():
        for a in range(0, s, t):
            grad = norm_back(h_ref[a : a + t, :].astype(F32), db_s[a : a + t, :].astype(BF16).astype(F32))
            out_ref[a : a + t, :] = (dh_ref[a : a + t, :].astype(F32) + grad).astype(BF16)
        for copy in stores(j):
            copy.wait()


def feed_back(h, dh, w, n_blocks, t=512):
    s, d = h.shape
    n, _, rows, _ = w.shape
    full = once((s, d), lambda j: (0, 0))
    part = n // n_blocks
    return pl.pallas_call(
        functools.partial(_feed_back, t=t),
        grid=(n_blocks,),
        in_specs=[
            full,
            full,
            pl.BlockSpec((n, 1, rows, d), lambda j: (0, 4 + j, 0, 0)),
            pl.BlockSpec((n, 1, rows, d), lambda j: (0, 4 + n_blocks + j, 0, 0)),
            pl.BlockSpec((part, n_blocks, rows, d), lambda j: (j, 3, 0, 0)),
        ],
        out_specs=[pl.BlockSpec((s, d), lambda j: (0, 0)), pl.BlockSpec(memory_space=pl.ANY)],
        out_shape=[jax.ShapeDtypeStruct((s, d), BF16), jax.ShapeDtypeStruct(w.shape, BF16)],
        scratch_shapes=[pltpu.VMEM((s, d), BF16), pltpu.VMEM((d, s), BF16), pltpu.VMEM((d, s), BF16)]
        + [pltpu.VMEM((s, d), BF16)] * 3
        + [pltpu.VMEM((s, d), F32), pltpu.VMEM((3, n, rows, d), BF16), pltpu.SemaphoreType.DMA((3,))],
        compiler_params=params("arbitrary"),
        cost_estimate=cost(16 * s * d * d * n_blocks, h, h, h, w, w, exps=s * d * n_blocks),
        name="feed_back",
    )(h, dh, w, w, w)


def _attend_back(q_ref, k_ref, v_ref, o_ref, dh_ref, lse_ref, wo_ref, dq_ref, dk_ref, dv_ref, dq_s, dk_s, dv_s, do_s, delta_s, *, scale, bk):
    bq, width = q_ref.shape
    heads = width // HEAD
    i = pl.program_id(0)
    e = scale * LOG2E

    @pl.when(i == 0)
    def _():
        dk_s[...] = jnp.zeros_like(dk_s)
        dv_s[...] = jnp.zeros_like(dv_s)

    dq_s[...] = jnp.zeros_like(dq_s)
    do = dot(dh_ref[...], whole(wo_ref, 0), 1, 1).astype(BF16)
    do_s[...] = do
    for n in range(heads):
        cut = slice(n * HEAD, (n + 1) * HEAD)
        delta_s[n : n + 1, :] = (do[:, cut].astype(F32) * o_ref[:, cut].astype(F32)).T.sum(axis=0, keepdims=True)

    def block(at, keys, pieces, gap):
        here = pl.ds(at, keys)
        work = [(slice(n * HEAD, (n + 1) * HEAD), n, a, w) for n in range(heads) for a, w in pieces]
        scores = [dot(k_ref[here, cut], q_ref[a : a + w, cut], 1, 1) for cut, n, a, w in work]
        dps = [dot(v_ref[here, cut], do_s[a : a + w, cut], 1, 1) for cut, n, a, w in work]
        for (cut, n, a, w), s, dp in zip(work, scores, dps):
            p = jnp.exp2(s * e - lse_ref[n : n + 1, a : a + w])
            if gap == a:
                ok = lax.broadcasted_iota(jnp.int32, (keys, w), 1) + (a - gap) >= lax.broadcasted_iota(jnp.int32, (keys, w), 0)
                p = jnp.where(ok, p, 0.0)
            ds = (p * (dp - delta_s[n : n + 1, a : a + w])).astype(BF16)
            dv_s[here, cut] += dot(p.astype(BF16), do_s[a : a + w, cut])
            dk_s[here, cut] += dot(ds, q_ref[a : a + w, cut])
            dq_s[n, :, a : a + w] += dot(k_ref[here, cut].T, ds)

    lax.fori_loop(0, i * (bq // bk), lambda j, _: block(pl.multiple_of(j * bk, bk), bk, [(0, bq)], None), None)
    half = bq // 2
    start = pl.multiple_of(i * bq, bq)
    block(start, half, [(0, half), (half, half)], 0)
    block(start + half, half, [(half, half)], half)
    for n in range(heads):
        dq_ref[:, n * HEAD : (n + 1) * HEAD] = (dq_s[n] * scale).T.astype(BF16)

    @pl.when(i == pl.num_programs(0) - 1)
    def _():
        dk_ref[...] = (dk_s[...] * scale).astype(BF16)
        dv_ref[...] = dv_s[...].astype(BF16)


def attend_back(q, k, v, o, dh, lse, w, bq=512, bk=512):
    s, d = q.shape
    n, _, rows, _ = w.shape
    heads = d // HEAD
    row = pl.BlockSpec((bq, d), lambda i: (i, 0))
    full = once((s, d), lambda i: (0, 0))
    out = jax.ShapeDtypeStruct((s, d), BF16)
    return pl.pallas_call(
        functools.partial(_attend_back, scale=HEAD**-0.5, bk=bk),
        grid=(s // bq,),
        in_specs=[row, full, full, row, row, pl.BlockSpec((heads, bq), lambda i: (0, i)), once((n, 1, rows, d), lambda i: (0, 3, 0, 0))],
        out_specs=[row] + [pl.BlockSpec((s, d), lambda i: (0, 0))] * 2,
        out_shape=[out, out, out],
        scratch_shapes=[pltpu.VMEM((heads, HEAD, bq), F32), pltpu.VMEM((s, d), F32), pltpu.VMEM((s, d), F32), pltpu.VMEM((bq, d), BF16),
                        pltpu.VMEM((heads, bq), F32)],
        compiler_params=params("arbitrary"),
        cost_estimate=cost(5 * s * s * d + 2 * s * d * d, q, k, v, q, q, q, k, v, exps=heads * s * s // 2),
        name="attend_back",
    )(q, k, v, o, dh, lse, w)


def _qkv_back(h_ref, dh_ref, dq_ref, dk_ref, dv_ref, o_ref, w_ref, cos_ref, sin_ref, _, *rest, by_input):
    out_ref, (dw_ref, total_s) = (rest[0], rest[1:]) if by_input else (None, rest)
    i = pl.program_id(0)
    d = h_ref.shape[1]
    wide = h_ref[...].astype(F32)
    a = (wide * inverse_rms(wide)).astype(BF16)
    cos, sin = cos_ref[...], sin_ref[...]

    def back(ref):
        parts = []
        for at in range(0, d, HEAD):
            t = ref[:, at : at + HEAD].astype(F32)
            parts.append((t * cos - pltpu.roll(t, HEAD // 2, 1) * sin).astype(BF16))
        return jnp.concatenate(parts, axis=1)

    terms = [back(dq_ref), back(dk_ref), dv_ref[...]]
    at = a.T
    grads = [dot(at, x) for x in terms] + [dot(o_ref[...].T, dh_ref[...])]

    @pl.when(i == 0)
    def _():
        for p, g in enumerate(grads):
            total_s[p] = g

    @pl.when(i > 0)
    def _():
        for p, g in enumerate(grads):
            total_s[p] += g

    if by_input:
        by_a = sum(dot(x, whole(w_ref, p), 1, 1) for p, x in enumerate(terms)).astype(BF16).astype(F32)
        out_ref[...] = (dh_ref[...].astype(F32) + norm_back(wide, by_a)).astype(BF16)

    @pl.when(i == pl.num_programs(0) - 1)
    def _():
        for p in range(4):
            dw_ref[:, p] = total_s[p].astype(BF16).reshape(dw_ref.shape[0], dw_ref.shape[2], d)


def qkv_back(h, dh, dq, dk, dv, o, w, cos, sin, dw, by_input, t=512):
    s, d = h.shape
    n, _, rows, _ = w.shape
    row = pl.BlockSpec((t, d), lambda i: (i, 0))
    table = pl.BlockSpec((t, HEAD), lambda i: (i, 0))
    grads = (n, 4, rows, d)
    return pl.pallas_call(
        functools.partial(_qkv_back, by_input=by_input),
        grid=(s // t,),
        in_specs=[row] * 6 + [once((n, 3, rows, d), lambda i: (0, 0, 0, 0)), table, table, pl.BlockSpec(memory_space=pl.ANY)],
        out_specs=[row] * by_input + [pl.BlockSpec(grads, lambda i: (0, 0, 0, 0))],
        out_shape=[jax.ShapeDtypeStruct((s, d), BF16)] * by_input + [jax.ShapeDtypeStruct(dw.shape, BF16)],
        input_output_aliases={9: int(by_input)},
        scratch_shapes=[pltpu.VMEM((4, d, d), F32)],
        compiler_params=params("arbitrary"),
        cost_estimate=cost((14 if by_input else 8) * s * d * d, h, h, h, h, h, h, h),
        name="qkv_back",
    )(h, dh, dq, dk, dv, o, w, cos, sin, dw)


def _adamw(*refs, n_blocks):
    g_ref, w_refs, m_refs, v_refs = refs[0], refs[1:8], refs[8:15], refs[15:22]
    outs = refs[22:]
    d = g_ref.shape[3]
    first = 0
    for i, (w_ref, m_ref, v_ref) in enumerate(zip(w_refs, m_refs, v_refs)):
        rows, columns = w_ref.shape[1:]
        pieces = rows * columns // (g_ref.shape[2] * d)
        for p in range(pieces):
            at = (slice(None), slice(p * d, (p + 1) * d)) if columns > d else (slice(p * g_ref.shape[2], (p + 1) * g_ref.shape[2]), slice(None))
            at = (0, *at)
            g = g_ref[0, first + p].astype(F32)
            m = 0.9 * m_ref[at] + 0.1 * g
            v = 0.95 * v_ref[at] + 0.05 * g * g
            w = w_ref[at].astype(F32)
            outs[i][at] = (w - 0.02 * (m * lax.rsqrt(v + 1e-8) + 0.1 * w)).astype(BF16)
            outs[7 + i][at] = m
            outs[14 + i][at] = v
        first += pieces


def adamw(g, weights, ms, vs, n_blocks):
    layers = g.shape[0]
    spec = lambda a: pl.BlockSpec((1, *a.shape[1:]), lambda l: (l, *(0,) * (a.ndim - 1)))
    return pl.pallas_call(
        functools.partial(_adamw, n_blocks=n_blocks),
        grid=(layers,),
        in_specs=[spec(a) for a in (g, *weights, *ms, *vs)],
        out_specs=[spec(a) for a in (*weights, *ms, *vs)],
        out_shape=[jax.ShapeDtypeStruct(a.shape, a.dtype) for a in (*weights, *ms, *vs)],
        compiler_params=params("arbitrary"),
        cost_estimate=cost(20 * g.size, g, *weights, *weights, *ms, *ms, *vs, *vs),
        name="adamw",
    )(g, *weights, *ms, *vs)


def rotary(tokens):
    half = HEAD // 2
    angle = jnp.arange(tokens, dtype=F32)[:, None] * THETA ** (-jnp.arange(half, dtype=F32) / half)
    cos, sin = jnp.cos(angle), jnp.sin(angle)
    return jnp.concatenate([cos, cos], 1), jnp.concatenate([-sin, sin], 1)


def packed(weights, number):
    rows, d = weights[0].shape[1:]
    parts = []
    for w in weights:
        block = w[number]
        if block.shape[1] > d:
            parts += [block[:, at : at + d] for at in range(0, block.shape[1], d)]
        else:
            parts += [block[at : at + rows] for at in range(0, block.shape[0], rows)]
    return jnp.stack(parts)


def solution(mesh):
    def step(x, dy, *arrays):
        weights, ms, vs = (arrays[i : i + 7] for i in (0, 7, 14))
        layers, d, ff = weights[0].shape[0], x.shape[2], weights[4].shape[2]
        blocks = ff // d
        cos, sin = rotary(x.shape[1])
        ws = [lax.all_gather(packed(weights, number), "dp", axis=0) for number in range(layers)]
        h, kept = x[0], []
        for number, w in enumerate(ws):
            q, k, v = qkv(h, w, cos, sin)
            o, lse, h1 = attend(q, k, v, h, w)
            kept.append((h, q, k, v, o, lse, h1))
            if number < layers - 1:
                h = feed(h1, w, blocks)
        by_h, mine = dy[0], [None] * layers
        for number in reversed(range(layers)):
            w = ws[number]
            h, q, k, v, o, lse, h1 = kept[number]
            by_h, dw = feed_back(h1, by_h, w, blocks)
            dq, dk, dv = attend_back(q, k, v, o, by_h, lse, w)
            *by_x, dw = qkv_back(h, by_h, dq, dk, dv, o, w, cos, sin, dw, number > 0)
            by_h = by_x[0] if number > 0 else None
            mine[number] = lax.psum_scatter(dw, "dp", scatter_dimension=0)
        return tuple(adamw(jnp.stack(mine), weights, ms, vs, blocks))

    states, cut = P(("rep", "dp"), None, None), P(None, "dp", None)
    return jax.shard_map(
        step,
        mesh=mesh,
        in_specs=(states, states) + (cut,) * 21,
        out_specs=(P("rep", "dp", None),) * 21,
        check_vma=False,
    )
```

```python
import functools

import jax
import jax.numpy as jnp
import numpy as np
from jax import lax
from jax.experimental import pallas as pl
from jax.experimental.pallas import tpu as pltpu
from jax.sharding import PartitionSpec as P

F32, BF16 = jnp.float32, jnp.bfloat16
HEAD = 128
THETA = 10000
NEG = -1e30
HIDDEN = 2 * NEG
LOG2E = 1.4426950408889634
VMEM = 62 * 2**20


def contract(a, b, ca, cb):
    return lax.dot_general(a, b, (((ca,), (cb,)), ((), ())), preferred_element_type=F32)


def dot(a, b):
    return contract(a, b, 1, 0)


def dot_t(a, b):
    return contract(a, b, 1, 1)


def comm_params(number):
    return pltpu.CompilerParams(dimension_semantics=("arbitrary",), vmem_limit_bytes=VMEM, collective_id=number, has_side_effects=number is not None)


def cost(flops, *arrays, exps=0):
    return pl.CostEstimate(flops=flops, transcendentals=exps, bytes_accessed=sum(a.size * a.dtype.itemsize for a in arrays))


def once(shape, index):
    return pl.BlockSpec(shape, index, pipeline_mode=pl.Buffered(1))


def fixed(*index):
    return lambda i: index


def held(a):
    return once(a.shape, fixed(*[0] * a.ndim))


def resident(a):
    return pl.BlockSpec(a.shape, fixed(*[0] * len(a.shape)))


def layer_of(a, layer):
    return once((None, *a.shape[1:]), fixed(layer, *[0] * (a.ndim - 1)))


ANYWHERE = pl.BlockSpec(memory_space=pl.ANY)


def inverse_rms(wide):
    return lax.rsqrt(jnp.mean(wide * wide, -1, keepdims=True) + 1e-6)


def sigmoid(x):
    return 1 / (1 + jnp.exp(-x))


def lower(keys, queries):
    place = lambda dim: lax.broadcasted_iota(jnp.int32, (keys, queries), dim)
    return place(1) >= place(0)


def due(timed, step, place):
    for at in sorted({t[0] for t in timed}):

        @pl.when(step == at)
        def _():
            for first, second, run in timed:
                if first == at and not isinstance(place, int):
                    pl.when(place == second)(run)
                elif first == at and place == second:
                    run()


class Ring:
    def __init__(self, axis):
        n, me = lax.axis_size(axis), lax.axis_index(axis)
        chip, core = lax.div(me, 2), lax.rem(me, 2)
        self.axis, self.me, self.far = axis, me, n // 4
        steps = range(-self.far, self.far + 1)
        chips = [2 * lax.rem(chip + by + n // 2, n // 2) for by in steps]
        self.own = {by: at + core for by, at in zip(steps, chips)}
        self.other = {by: at + 1 - core for by, at in zip(steps, chips)}

    def meet(self):
        barrier = pltpu.get_barrier_semaphore()
        for to in (self.own[1], self.own[-1], self.other[0]):
            pl.semaphore_signal(barrier, inc=1, device_id={self.axis: to}, device_id_type=pl.DeviceIdType.MESH)
        pl.semaphore_wait(barrier, 3)

    def copy(self, src, dst, sems, at, to):
        return pltpu.make_async_remote_copy(src, dst, sems.at[0, at], sems.at[1, at], device_id={self.axis: to}, device_id_type=pl.DeviceIdType.MESH)


class Gather:
    def __init__(self, ring, w_ref, first, pieces, sems, base):
        far, half = ring.far, pieces // 2
        every = slice(first, first + pieces)
        part = lambda number, way: every if number < far else slice(first, first + half) if way == 1 else slice(first + half, first + pieces)
        self.hops = [(number, way) for number in range(1, far + 1) for way in (1, -1)]
        self.table = {hop: (ring.own[hop[1]], ring.own[(1 - hop[0]) * hop[1]], ring.own[-hop[0] * hop[1]], part(*hop)) for hop in self.hops}
        for number, way in [(0, 1), *self.hops]:
            at = -number * way
            self.table["core", number, way] = ring.other[0], ring.own[at], ring.other[at], part(number, way)
        self.index = {key: base + at for at, key in enumerate(self.table)}
        self.ring, self.w_ref, self.sems = ring, w_ref, sems

    def copy(self, key, comes=False):
        to, sent, arriving, part = self.table[key]
        dst = self.w_ref.at[arriving if comes else sent, part]
        return self.ring.copy(dst, dst, self.sems, self.index[key], to)

    def begin(self):
        for way in (1, -1):
            self.copy((1, way)).start()
        self.copy(("core", 0, 1)).start()

    def step(self, number):
        for way in (1, -1):
            self.copy((number, way), True).wait_recv()
            if number < self.ring.far:
                self.copy((number + 1, way)).start()
            self.copy(("core", number, way)).start()

    def arrive(self):
        for key in self.table:
            if key[0] == "core":
                self.copy(key, True).wait_recv()

    def sent(self):
        for key in self.table:
            self.copy(key).wait_send()


def gather_copies(n):
    return 2 * 2 * (n // 4) + 1


PLACES = 64


def rotary_parts(tokens):
    half = HEAD // 2
    place = np.concatenate([np.arange(PLACES), np.arange(0, tokens, PLACES)]).astype(np.float32)
    angle = place[:, None] * np.float32(THETA) ** (-np.arange(half, dtype=np.float32) / half)
    return np.stack([np.concatenate([f(angle.astype(np.float64))] * 2, axis=1) for f in (np.cos, np.sin)]).astype(np.float32)


def tables(table_ref, first, count):
    near_cos, near_sin = table_ref[0, :PLACES], table_ref[1, :PLACES]
    sign = jnp.where(lax.broadcasted_iota(jnp.int32, (1, HEAD), 1) < HEAD // 2, -1.0, 1.0)
    cos, sin = [], []
    for i in range(count):
        far_cos, far_sin = (table_ref[f, pl.ds(PLACES + first + i, 1)] for f in range(2))
        cos.append(near_cos * far_cos - near_sin * far_sin)
        sin.append((near_sin * far_cos + near_cos * far_sin) * sign)
    return jnp.concatenate(cos), jnp.concatenate(sin)


class Forward:
    def __init__(self, layers, blocks):
        self.layers, self.blocks = layers, blocks
        self.steps = (3 * layers - 1) * blocks

    def at(self, step):
        layer = lax.div(step, 3 * self.blocks)
        return layer, step - 3 * self.blocks * layer

    def block(self, phase):
        return lambda step: (self.at(step)[0], jnp.clip(self.at(step)[1] - phase * self.blocks, 0, self.blocks - 1))

    def fed(self, step):
        layer, block = self.block(2)(step)
        return jnp.minimum(layer, self.layers - 2), jnp.where(layer > self.layers - 2, self.blocks - 1, block)


    def points(self):
        durations = {0: 1.9, 1: 2.0, 2: 1.25}
        time, out = 0.0, []
        for step in range(self.steps):
            phase, block = divmod(step % (3 * self.blocks), self.blocks)
            for place in range((1, block + 1, self.blocks)[phase]):
                out.append((time, step, place))
                time += durations[phase]
        return out

    def timed(self, rounds, far):
        hop, delay = 2.8, 2.2
        points, out, link, place = self.points(), [], 0.0, 0

        def add(time, kind, number, job):
            nonlocal place
            first_use = 3 * self.blocks * job[0] + (2 * self.blocks if job[1] else 0)
            while place < len(points) - 1 and points[place][0] < time and points[place + 1][1:] <= (first_use, 0):
                place += 1
            assert points[place][1:] <= (first_use, 0)
            out.append((*points[place][1:], kind, number, job))
            return max(time, points[place][0])

        def send(time, length):
            nonlocal link
            link = max(link, time) + length
            return link + delay

        came = {job: 0.0 for job in rounds[0]}
        for jobs, later in zip(rounds, rounds[1:] + [[]]):
            for number in range(1, far + 1):
                for job in jobs:
                    time = add(came[job], "step", number, job)
                    if number < far:
                        came[job] = send(time, hop if number + 1 < far else hop / 2)
                if number == far - 1:
                    for job in later:
                        came[job] = send(add(link - hop, "begin", 0, job), hop)
            for job in jobs:
                add(came[job] + 1, "arrive", 0, job)
        return out


def _forward(x_ref, table_ref, *rest, plan, scale, axis):
    shards, rest = rest[:7], rest[7:]
    q_ref, k_ref, v_ref, o_ref, lse_ref, h1_ref, h2_ref, w_ref = rest[:8]
    w_s, h_s, q_s, k_s, v_s, top_s, mix_s, x_sem, w_sems, ring_sems = rest[8:]
    step = pl.program_id(0)
    blocks = plan.blocks
    layer, within = plan.at(step)
    bq, width = q_ref.shape[1:]
    n, pieces, rows, _ = w_s.shape[1:]
    group = 4
    heads = width // HEAD
    e = scale * LOG2E
    ring = Ring(axis)
    jobs = {}
    for number in range(plan.layers):
        for first in range(0, pieces, group):
            jobs[number, first // group] = Gather(ring, w_s.at[number], first, group, ring_sems, gather_copies(n) * len(jobs))

    def put(key):
        number, first = key[0], key[1] * group
        cut = lambda ref: ref.at[number, :, first : first + group]
        return pltpu.make_async_copy(cut(w_s), cut(w_ref), w_sems.at[number, key[1]])

    def event(kind, number, key):
        job = jobs[key]
        if kind == "begin":
            job.begin()
        elif kind == "step":
            job.step(number)
        else:
            job.arrive()
            put(key).start()

    groups = pieces // group
    rounds = [[(0, at) for at in range(1, groups)]]
    for number in range(1, plan.layers):
        rounds += [[(number, at), (number, at + 1)] for at in range(0, groups, 2)]
    timed = [(*t[:2], functools.partial(event, *t[2:])) for t in plan.timed(rounds, ring.far)]

    def events(phase, place):
        due([t for t in timed if t[0] % (3 * blocks) // blocks == phase], step, place)

    def pack(number, first):
        at = 0
        for shard in shards:
            for row in range(0, shard.shape[1], rows):
                for column in range(0, shard.shape[2], width):
                    if first <= at < first + group:
                        w_s[number, ring.me, at] = shard[number, row : row + rows, column : column + width]
                    at += 1

    @pl.when(step == 0)
    def _():
        x_copy = pltpu.make_async_copy(x_ref.at[0], h_s, x_sem)
        x_copy.start()
        pack(0, 0)
        ring.meet()
        jobs[0, 0].begin()
        for key in list(jobs)[1:]:
            pack(key[0], key[1] * group)
        for number in range(1, ring.far + 1):
            if number < pieces // group:
                jobs[0, number].begin()
            jobs[0, 0].step(number)
        event("arrive", 0, (0, 0))
        x_copy.wait()

    @pl.when(within < blocks)
    def _():
        events(0, 0)
        here = pl.ds(pl.multiple_of(within * bq, bq), bq)
        wide = h_s[here, :].astype(F32)
        a = (wide * inverse_rms(wide)).astype(BF16)
        cos, sin = tables(table_ref, within * (bq // PLACES), bq // PLACES)
        for piece, (out_ref, kept) in enumerate(((q_ref, q_s), (k_ref, k_s), (v_ref, v_s))):
            y = dot(a, w_s[layer, :, piece].reshape(width, width)).astype(BF16)
            if piece < 2:
                turned = []
                for at in range(0, width, HEAD):
                    t = y[:, at : at + HEAD].astype(F32)
                    turned.append((t * cos + pltpu.roll(t, HEAD // 2, 1) * sin).astype(BF16))
                y = jnp.concatenate(turned, 1)
            out_ref[0] = y
            kept[here, :] = y

    @pl.when((within >= blocks) & (within < 2 * blocks))
    def _():
        b = within - blocks
        first = pl.multiple_of(b * bq, bq)
        top_s[:] = jnp.full_like(top_s, NEG)
        mix_s[:] = jnp.zeros_like(mix_s)

        def block(at, keys, strips, gap):
            here = pl.ds(at, keys)
            ones = jnp.ones((8, keys), BF16)
            work = [(m, a, w) for m in range(heads) for a, w in strips]
            scores = [dot_t(k_s[here, m * HEAD : (m + 1) * HEAD], q_s[pl.ds(first + a, w), m * HEAD : (m + 1) * HEAD]) for m, a, w in work]
            weights, keeps = [], []
            for (m, a, w), s in zip(work, scores):
                if gap == a:
                    s = jnp.where(lower(keys, w), s, HIDDEN)
                old = top_s[m : m + 1, a : a + w]
                top = jnp.maximum(old, s.max(axis=0, keepdims=True))
                top_s[m : m + 1, a : a + w] = top
                weights.append(jnp.exp2((s - top) * e).astype(BF16))
                keeps.append(jnp.exp2((old - top) * e))
            for (m, a, w), p, keep in zip(work, weights, keeps):
                values = jnp.concatenate([v_s[here, m * HEAD : (m + 1) * HEAD].T, ones])
                mix_s[m, :, a : a + w] = mix_s[m, :, a : a + w] * keep + dot(values, p)

        def before(j, _):
            events(1, j)
            block(pl.multiple_of(j * bq, bq), bq, [(0, bq)], None)

        lax.fori_loop(0, b, before, None)
        events(1, b)
        half = bq // 2
        block(first, half, [(0, half), (half, half)], 0)
        block(pl.multiple_of(first + half, half), half, [(half, half)], half)
        for m in range(heads):
            top, total = top_s[m : m + 1, :], mix_s[m, HEAD : HEAD + 1, :]
            o_ref[0, :, m * HEAD : (m + 1) * HEAD] = (mix_s[m, :HEAD, :] * (1 / total)).T.astype(BF16)
            lse_ref[0, m : m + 1, :] = top * e + jnp.log2(total)
        here = pl.ds(first, bq)
        h1 = h_s[here, :] + dot(o_ref[0], w_s[layer, :, 3].reshape(width, width)).astype(BF16)
        h_s[here, :] = h1
        h1_ref[0] = h1

    @pl.when(within >= 2 * blocks)
    def _():
        here = pl.ds(pl.multiple_of((within - 2 * blocks) * bq, bq), bq)
        wide = h_s[here, :].astype(F32)
        b = (wide * inverse_rms(wide)).astype(BF16)
        parts = (pieces - group) // 3
        owners = n // parts
        y = None
        for j in range(parts):
            events(2, j)
            gate = dot(b, w_s[layer, :, group + j].reshape(width, width))
            up = dot(b, w_s[layer, :, group + parts + j].reshape(width, width))
            act = (gate * sigmoid(gate) * up).astype(BF16)
            part = dot(act, w_s[layer, owners * j : owners * (j + 1), group + 2 * parts :].reshape(width, width))
            y = part if y is None else y + part
        h2 = h_s[here, :] + y.astype(BF16)
        h_s[here, :] = h2
        h2_ref[0] = h2

    @pl.when(step == plan.steps - 1)
    def _():
        for key, job in jobs.items():
            job.sent()
            put(key).wait()


def forward(x, shards, axis, n, pieces, number, bq=512):
    _, s, d = x.shape
    layers, rows = shards[0].shape[:2]
    heads, plan = d // HEAD, Forward(layers, s // bq)
    table = rotary_parts(s)
    block = lambda index: pl.BlockSpec((1, bq, d), lambda i: (*index(i), 0))
    out = jax.ShapeDtypeStruct((layers, s, d), BF16)
    weights = (layers, n, pieces, rows, d)
    return pl.pallas_call(
        functools.partial(_forward, plan=plan, scale=HEAD**-0.5, axis=axis),
        grid=(plan.steps,),
        in_specs=[pl.BlockSpec(memory_space=pl.ANY), held(table), *[held(a) for a in shards]],
        out_specs=[block(plan.block(0))] * 3 + [block(plan.block(1)), pl.BlockSpec((1, heads, bq), lambda i: (plan.block(1)(i)[0], 0, plan.block(1)(i)[1])),
                   block(plan.block(1)), block(plan.fed), pl.BlockSpec(memory_space=pl.ANY)],
        out_shape=[out] * 4 + [jax.ShapeDtypeStruct((layers, heads, s), F32), out, jax.ShapeDtypeStruct((layers - 1, s, d), BF16),
                   jax.ShapeDtypeStruct(weights, BF16)],
        scratch_shapes=[pltpu.VMEM(weights, BF16)] + [pltpu.VMEM((s, d), BF16)] * 4
        + [pltpu.VMEM((heads, bq), F32), pltpu.VMEM((heads, HEAD + 8, bq), F32), pltpu.SemaphoreType.DMA, pltpu.SemaphoreType.DMA((layers, pieces // 4)),
           pltpu.SemaphoreType.DMA((2, layers * (pieces // 4) * gather_copies(n)))],
        compiler_params=comm_params(number),
        cost_estimate=cost(layers * (2 * s * s * d + 32 * s * d * d), *[x] * 8, exps=layers * heads * s * s // 2),
        name="forward",
    )(x, table, *shards)


class Scatter:
    def __init__(self, axis, dw, out, own_s, core_s, come_s, go_s, own_sems, core_sems, hop_sems):
        ring = Ring(axis)
        far, pieces = ring.far, dw.shape[1]
        halves = (slice(0, pieces // 2), slice(pieces // 2, pieces))
        targets = [far] + [way * by for by in range(far - 1, 0, -1) for way in (1, -1)] + [0]
        slot = {by: at for at, by in enumerate(targets)} | {-far: 0}
        ways = lambda number, half: (1, -1) if number > 1 else (1 - 2 * half,)
        hops = [(number, half, way) for number in range(1, far + 1) for half in (0, 1) for way in ways(number, half)]
        index = {hop: at for at, hop in enumerate(hops)}

        def load(by):
            return pltpu.make_async_copy(dw.at[ring.own[by]], own_s.at[slot[by]], own_sems.at[slot[by]])

        def share(by):
            return ring.copy(dw.at[ring.other[by]], core_s.at[slot[by]], core_sems, slot[by], ring.other[0])

        def move(hop):
            return ring.copy(go_s.at[index[hop]], come_s.at[index[hop]], hop_sems, index[hop], ring.own[hop[2]])

        def total(dst, by, half, came):
            first = halves[half].start

            some = 3 if pieces % 3 == 0 else 2

            def add(i, _):
                for p in (i * some + at for at in range(some)):
                    terms = [own_s[slot[by], first + p], core_s[slot[by], first + p]] + [come_s[index[hop], p] for hop in came]
                    dst[p] = sum(x.astype(F32) for x in terms).astype(BF16)

            lax.fori_loop(0, pieces // 2 // some, add, None)

        def begin():
            for by in targets:
                load(by).start()
            ring.meet()
            for by in targets[:3]:
                share(by).start()

        def need(by):
            load(by).wait()
            share(by).wait_recv()

        def step(number, half):
            if half == 0:
                for by in sorted({slot[way * (far - number + 1)] for way in (1, -1)}):
                    need(targets[by])
            for way in ways(number, half):
                came = [hop for hop in [(number - 1, half, way)] if hop in index]
                for hop in came:
                    move(hop).wait_recv()
                total(go_s.at[index[number, half, way]], way * (far - number + 1), half, came)
            for way in ways(number, half):
                move((number, half, way)).start()
            if half == 1:
                for by in targets[2 * number + 1 : 2 * number + 3]:
                    share(by).start()

        def finish(half):
            if half == 0:
                need(0)
            came = [(far, half, way) for way in (1, -1)]
            for hop in came:
                move(hop).wait_recv()
            total(out.at[halves[half]], 0, half, came)

        def end():
            for hop in hops:
                move(hop).wait_send()
            for by in targets:
                share(by).wait_send()

        self.events = [begin] + [functools.partial(step, number, half) for number in range(1, far + 1) for half in (0, 1)]
        self.events += [functools.partial(finish, half) for half in (0, 1)] + [end]

    @staticmethod
    def scratch(n, pieces, rows, d):
        hops = 2 + 4 * (n // 4 - 1)
        whole, half = (pltpu.VMEM((count, share, rows, d), BF16) for count, share in ((n // 2, pieces), (hops, pieces // 2)))
        return [whole, whole, half, half, pltpu.SemaphoreType.DMA((n // 2,)), pltpu.SemaphoreType.DMA((2, n // 2)), pltpu.SemaphoreType.DMA((2, hops))]


def _scatter(dw_ref, out_ref, *scratch, axis):
    for event in Scatter(axis, dw_ref, out_ref, *scratch).events:
        event()


def scatter(dw, axis, number):
    out = jax.ShapeDtypeStruct(dw.shape[1:], BF16)
    return pl.pallas_call(
        functools.partial(_scatter, axis=axis),
        grid=(1,),
        in_specs=[ANYWHERE],
        out_specs=resident(out),
        out_shape=out,
        scratch_shapes=Scatter.scratch(*dw.shape),
        compiler_params=comm_params(number),
        name="scatter",
    )(dw)


def norm_back(wide, by_normed):
    r = inverse_rms(wide)
    normed = wide * r
    return r * (by_normed - normed * jnp.mean(normed * by_normed, -1, keepdims=True))


def _feed_back(h_ref, dh_ref, wg_ref, wu_ref, wd_ref, *rest, t, axis):
    rest = list(rest)
    timed = []
    blocks = wd_ref.shape[1]
    if axis:
        dwa_ref, ga_ref = rest.pop(0), rest.pop(2)
        points = [(step, place) for step in range(blocks) for place in range(3)]
        timed = [(*point, event) for point, event in zip(points, Scatter(axis, dwa_ref, ga_ref, *rest[11:]).events)]
    out_ref, dw_ref, b_s, bt_s, dht_s, act_s, dgate_s, dup_s, db_s, dw_s, sems = rest[:11]
    j = pl.program_id(0)
    s, d = h_ref.shape
    n, _, rows, _ = wg_ref.shape
    part = wd_ref.shape[0]
    wg, wu, wd = (r[:].reshape(d, d) for r in (wg_ref, wu_ref, wd_ref))
    strips = [slice(a, a + t) for a in range(0, s, t)]

    def stores(j):
        places = (dw_ref.at[:, j], dw_ref.at[:, blocks + j], dw_ref.at[pl.ds(j * part, part), 2 * blocks :])
        return [pltpu.make_async_copy(dw_s.at[i].reshape(p.shape), p, sems.at[i]) for i, p in enumerate(places)]

    due(timed, j, 0)

    @pl.when(j == 0)
    def _():
        for here in strips:
            wide = h_ref[here, :].astype(F32)
            b = (wide * inverse_rms(wide)).astype(BF16)
            b_s[here, :] = b
            bt_s[:, here] = b.T
            dht_s[:, here] = dh_ref[here, :].T
        db_s[:] = jnp.zeros_like(db_s)

    def products(here):
        b = b_s[here, :]
        return dot(b, wg), dot(b, wu), dot_t(dh_ref[here, :], wd).astype(BF16)

    def bends(here, gate, up, dact):
        dact = dact.astype(F32)
        sig = sigmoid(gate)
        silu = gate * sig
        act_s[here, :] = (silu * up).astype(BF16)
        dup_s[here, :] = (dact * silu).astype(BF16)
        dgate_s[here, :] = (dact * up * (sig + silu * (1 - sig))).astype(BF16)

    def sums(here):
        db_s[here, :] += dot_t(dgate_s[here, :], wg) + dot_t(dup_s[here, :], wu)

    made = {}
    for at in range(len(strips) + 2):
        if at == 3:
            due(timed, j, 1)
        if at < len(strips):
            made[at] = products(strips[at])
        if 1 <= at <= len(strips):
            bends(strips[at - 1], *made.pop(at - 1))
        if at >= 2:
            sums(strips[at - 2])

    @pl.when(j > 0)
    def _():
        for copy in stores(j - 1):
            copy.wait()

    due(timed, j, 2)
    for i, (a, b) in enumerate(((bt_s, dgate_s), (bt_s, dup_s), (dht_s, act_s))):
        g = dot(a[:], b[:])
        dw_s[i] = (g.T if i == 2 else g).astype(BF16).reshape(n, rows, d)
    for copy in stores(j):
        copy.start()

    @pl.when(j == blocks - 1)
    def _():
        for here in strips:
            grad = norm_back(h_ref[here, :].astype(F32), db_s[here, :].astype(BF16).astype(F32))
            out_ref[here, :] = (dh_ref[here, :].astype(F32) + grad).astype(BF16)
        for copy in stores(j):
            copy.wait()


def feed_back(h, dh, w, layer, blocks, dwa=None, axis=None, number=None, t=512):
    _, s, d = h.shape
    _, n, pieces, rows, _ = w.shape
    part, first = n // blocks, pieces - 3 * blocks
    extra = [] if dwa is None else [dwa]
    sums = [jax.ShapeDtypeStruct(a.shape[1:], BF16) for a in extra]
    column = lambda at: pl.BlockSpec((None, n, 1, rows, d), lambda j: (layer, 0, first + at + j, 0, 0))
    out = jax.ShapeDtypeStruct((s, d), BF16)
    state = pltpu.VMEM((s, d), BF16)
    flat = pltpu.VMEM((d, s), BF16)
    return pl.pallas_call(
        functools.partial(_feed_back, t=t, axis=axis),
        grid=(blocks,),
        in_specs=[layer_of(h, layer), held(out), column(0), column(blocks),
                  pl.BlockSpec((None, part, blocks, rows, d), lambda j: (layer, j, pieces // blocks - 1, 0, 0)), *[ANYWHERE for _ in extra]],
        out_specs=[resident(out), ANYWHERE, *map(resident, sums)],
        out_shape=[out, jax.ShapeDtypeStruct((n, 3 * blocks, rows, d), BF16), *sums],
        scratch_shapes=[state, flat, flat, state, state, state, pltpu.VMEM((s, d), F32), pltpu.VMEM((3, n, rows, d), BF16), pltpu.SemaphoreType.DMA((3,))]
        + [x for a in extra for x in Scatter.scratch(*a.shape)],
        compiler_params=comm_params(number),
        cost_estimate=cost(16 * s * d * d * blocks, *[out] * 7, exps=s * d * blocks),
        name="feed_back",
    )(h, dh, w, w, w, *extra)


def _attend_back(q_ref, k_ref, v_ref, o_ref, dh_ref, lse_ref, h_ref, wa_ref, table_ref, dwf_ref, *rest, scale, axis, by_input):
    out_ref, rest = (rest[0], rest[1:]) if by_input else (None, rest)
    dwa_ref, gf_ref, dq_s, dqs_s, dk_s, dv_s, do_s, delta_s, total_s, *scratch = rest
    i = pl.program_id(0)
    bq, width = q_ref.shape
    blocks = k_ref.shape[0] // bq
    heads = width // HEAD
    e = scale * LOG2E
    matrix = lambda piece: wa_ref[:, piece].reshape(width, width)
    cuts = [slice(n * HEAD, (n + 1) * HEAD) for n in range(heads)]
    points = [(step, place) for step in range(blocks) for place in range(step + 1)] + [(blocks + step, 0) for step in range(blocks)]
    timed = [(*point, event) for point, event in zip(points, Scatter(axis, dwf_ref, gf_ref, *scratch).events)]
    inside, after = ([t for t in timed if (t[0] < blocks) == first] for first in (True, False))

    @pl.when(i == 0)
    def _():
        dk_s[:] = jnp.zeros_like(dk_s)
        dv_s[:] = jnp.zeros_like(dv_s)
        total_s[:] = jnp.zeros_like(total_s)

    @pl.when(i < blocks)
    def _():
        first = pl.multiple_of(i * bq, bq)
        dq_s[:] = jnp.zeros_like(dq_s)
        do = dot_t(dh_ref[:], matrix(3)).astype(BF16)
        do_s[:] = do
        for n, cut in enumerate(cuts):
            delta_s[n : n + 1, :] = (do[:, cut].astype(F32) * o_ref[:, cut].astype(F32)).T.sum(axis=0, keepdims=True)

        def block(at, keys, pieces, gap):
            here = pl.ds(at, keys)
            work = [(cut, n, a, w) for n, cut in enumerate(cuts) for a, w in pieces]
            scores = [dot_t(k_ref[here, cut], q_ref[a : a + w, cut]) for cut, n, a, w in work]
            dps = [dot_t(v_ref[here, cut], do_s[a : a + w, cut]) for cut, n, a, w in work]
            for (cut, n, a, w), s, dp in zip(work, scores, dps):
                p = jnp.exp2(s * e - lse_ref[n : n + 1, a : a + w])
                if gap == a:
                    p = jnp.where(lower(keys, w), p, 0.0)
                ds = (p * (dp - delta_s[n : n + 1, a : a + w])).astype(BF16)
                dv_s[here, cut] += dot(p.astype(BF16), do_s[a : a + w, cut])
                dk_s[here, cut] += dot(ds, q_ref[a : a + w, cut])
                dq_s[n, :, a : a + w] += dot(k_ref[here, cut].T, ds)

        def before(j, _):
            due(inside, i, j)
            block(pl.multiple_of(j * bq, bq), bq, [(0, bq)], None)

        lax.fori_loop(0, i, before, None)
        due(inside, i, i)
        half = bq // 2
        block(first, half, [(0, half), (half, half)], 0)
        block(pl.multiple_of(first + half, half), half, [(half, half)], half)
        for n, cut in enumerate(cuts):
            dqs_s[pl.ds(first, bq), cut] = (dq_s[n] * scale).T.astype(BF16)

    @pl.when(i >= blocks)
    def _():
        b = i - blocks
        due(after, i, 0)
        here = pl.ds(pl.multiple_of(b * bq, bq), bq)
        wide = h_ref[:].astype(F32)
        a = (wide * inverse_rms(wide)).astype(BF16)
        cos, sin = tables(table_ref, b * (bq // PLACES), bq // PLACES)

        def back(x):
            parts = []
            for cut in cuts:
                t = x[:, cut].astype(F32)
                parts.append((t * cos - pltpu.roll(t, HEAD // 2, 1) * sin).astype(BF16))
            return jnp.concatenate(parts, axis=1)

        terms = [back(dqs_s[here, :]), back((dk_s[here, :] * scale).astype(BF16)), dv_s[here, :].astype(BF16)]
        at = a.T
        for p, x in enumerate(terms):
            total_s[p] += dot(at, x)
        total_s[3] += dot(o_ref[:].T, dh_ref[:])
        if by_input:
            by_a = sum(dot_t(x, matrix(p)) for p, x in enumerate(terms)).astype(BF16).astype(F32)
            out_ref[:] = (dh_ref[:].astype(F32) + norm_back(wide, by_a)).astype(BF16)

        @pl.when(i == 2 * blocks - 1)
        def _():
            for p in range(4):
                dwa_ref[:, p] = total_s[p].astype(BF16).reshape(dwa_ref.shape[0], dwa_ref.shape[2], width)


def attend_back(kept, dh, h, h_layer, w, dwf, layer, axis, number, bq=512):
    *_, s, d = h.shape
    _, n, pieces, rows, _ = w.shape
    heads, blocks, own = d // HEAD, s // bq, pieces - dwf.shape[1]
    table = rotary_parts(s)
    early, late, both = lambda i: jnp.minimum(i, blocks - 1), lambda i: jnp.maximum(i - blocks, 0), lambda i: lax.rem(i, blocks)
    row = lambda index, at: pl.BlockSpec((None, bq, d), lambda i: (at, index(i), 0))
    flat = lambda index: pl.BlockSpec((bq, d), lambda i: (index(i), 0))
    out = [jax.ShapeDtypeStruct((s, d), BF16)] * (layer > 0)
    sums = [jax.ShapeDtypeStruct(a, BF16) for a in ((n, own, rows, d), dwf.shape[1:])]
    state = pltpu.VMEM((s, d), F32)
    return pl.pallas_call(
        functools.partial(_attend_back, scale=HEAD**-0.5, axis=axis, by_input=layer > 0),
        grid=(2 * blocks,),
        in_specs=[row(early, layer), layer_of(kept[1], layer), layer_of(kept[2], layer), row(both, layer), flat(both),
                  pl.BlockSpec((None, heads, bq), lambda i: (layer, 0, early(i))), row(late, h_layer),
                  once((None, n, own, rows, d), fixed(layer, 0, 0, 0, 0)), held(table), ANYWHERE],
        out_specs=[flat(late) for _ in out] + [*map(resident, sums)],
        out_shape=out + sums,
        scratch_shapes=[pltpu.VMEM((heads, HEAD, bq), F32), pltpu.VMEM((s, d), BF16), state, state, pltpu.VMEM((bq, d), BF16),
                        pltpu.VMEM((heads, bq), F32), pltpu.VMEM((own, d, d), F32)] + Scatter.scratch(*dwf.shape),
        compiler_params=comm_params(number),
        cost_estimate=cost(5 * s * s * d + 16 * s * d * d, *[dh] * 9, exps=heads * s * s // 2),
        name="attend_back",
    )(*kept[:4], dh, kept[4], h, w, table, dwf)


def _adamw(*refs, layers):
    sums, refs = (refs[:layers], refs[layers : 2 * layers]), refs[2 * layers :]
    w_refs, m_refs, v_refs, outs = refs[:7], refs[7:14], refs[14:21], refs[21:]
    layer, first, every = pl.program_id(0), 0, slice(None)
    for i, (w_ref, m_ref, v_ref) in enumerate(zip(w_refs, m_refs, v_refs)):
        which, first = sums[i >= 4], 0 if i == 4 else first
        rows, d = which[0].shape[1:]
        pieces = w_ref.shape[1] * w_ref.shape[2] // (rows * d)
        for p in range(pieces):
            cut = lambda size: slice(p * size, p * size + size)
            at = (0, every, cut(d)) if w_ref.shape[2] > d else (0, cut(rows), every)
            g = which[-1][first + p]
            for number in range(layers - 1):
                g = jnp.where(layer == number, which[number][first + p], g)
            g = g.astype(F32)
            m = 0.9 * m_ref[at] + 0.1 * g
            v = 0.95 * v_ref[at] + 0.05 * g * g
            w = w_ref[at].astype(F32)
            outs[i][at] = (w - 0.02 * (m * lax.rsqrt(v + 1e-8) + 0.1 * w)).astype(BF16)
            outs[7 + i][at] = m
            outs[14 + i][at] = v
        first += pieces


def adamw(sums_a, sums_f, weights, ms, vs):
    layers = len(sums_a)
    spec = lambda a: pl.BlockSpec((1, *a.shape[1:]), lambda l: (l, 0, 0))
    sums = [held(a) for a in (*sums_a, *sums_f)]
    state = (*weights, *ms, *vs)
    return pl.pallas_call(
        functools.partial(_adamw, layers=layers),
        grid=(layers,),
        in_specs=sums + [spec(a) for a in state],
        out_specs=[spec(a) for a in state],
        out_shape=[jax.ShapeDtypeStruct(a.shape, a.dtype) for a in state],
        compiler_params=comm_params(None),
        cost_estimate=cost(20 * sum(a.size for a in weights), *state, *state),
        name="adamw",
    )(*sums_a, *sums_f, *state)


def solution(mesh):
    axis, n = "dp", mesh.shape["dp"]

    def step(x, dy, *arrays):
        weights, ms, vs = (arrays[i : i + 7] for i in (0, 7, 14))
        layers, d, ff = weights[0].shape[0], x.shape[2], weights[4].shape[2]
        blocks = ff // d
        *kept, h1, h2, w = forward(x, weights, axis, n, 4 + 3 * blocks, 0)
        by_h, dwa, sums_a, sums_f = dy[0], None, [None] * layers, [None] * layers
        for layer in reversed(range(layers)):
            if dwa is None:
                by_h, dwf = feed_back(h1, by_h, w, layer, blocks)
            else:
                by_h, dwf, sums_a[layer + 1] = feed_back(h1, by_h, w, layer, blocks, dwa, axis, 1)
            *by_x, dwa, sums_f[layer] = attend_back(kept, by_h, h2 if layer else x, max(layer - 1, 0), w, dwf, layer, axis, 2 + (layer > 0))
            by_h = by_x[0] if by_x else None
        sums_a[0] = scatter(dwa, axis, 4)
        return tuple(adamw(sums_a, sums_f, weights, ms, vs))

    states, cut = P(("rep", "dp"), None, None), P(None, "dp", None)
    return jax.shard_map(
        step,
        mesh=mesh,
        in_specs=(states, states) + (cut,) * 21,
        out_specs=(P("rep", "dp", None),) * 21,
        check_vma=False,
    )
```

```python
import functools

import jax
import jax.numpy as jnp
import numpy as np
from jax import lax
from jax.experimental import pallas as pl
from jax.experimental.pallas import tpu as pltpu
from jax.sharding import PartitionSpec as P

F32, BF16 = jnp.float32, jnp.bfloat16
HEAD = 128
THETA = 10000
NEG = -1e30
HIDDEN = 2 * NEG
LOG2E = 1.4426950408889634
VMEM = 62 * 2**20


def contract(a, b, ca, cb):
    return lax.dot_general(a, b, (((ca,), (cb,)), ((), ())), preferred_element_type=F32)


def dot(a, b):
    return contract(a, b, 1, 0)


def dot_t(a, b):
    return contract(a, b, 1, 1)


def comm_params(number):
    return pltpu.CompilerParams(dimension_semantics=("arbitrary",), vmem_limit_bytes=VMEM, collective_id=number, has_side_effects=number is not None)


def cost(flops, *arrays, exps=0):
    return pl.CostEstimate(flops=flops, transcendentals=exps, bytes_accessed=sum(a.size * a.dtype.itemsize for a in arrays))


def once(shape, index):
    return pl.BlockSpec(shape, index, pipeline_mode=pl.Buffered(1))


def fixed(*index):
    return lambda i: index


def held(a):
    return once(a.shape, fixed(*[0] * a.ndim))


def resident(a):
    return pl.BlockSpec(a.shape, fixed(*[0] * len(a.shape)))


ANYWHERE = pl.BlockSpec(memory_space=pl.ANY)


def inverse_rms(wide):
    return lax.rsqrt(jnp.mean(wide * wide, -1, keepdims=True) + 1e-6)


def sigmoid(x):
    return 1 / (1 + jnp.exp(-x))


def lower(keys, queries):
    place = lambda dim: lax.broadcasted_iota(jnp.int32, (keys, queries), dim)
    return place(1) >= place(0)


def due(timed, step, place):
    for at in sorted({t[0] for t in timed}):

        @pl.when(step == at)
        def _():
            for first, second, run in timed:
                if first == at and not isinstance(place, int):
                    pl.when(place == second)(run)
                elif first == at and place == second:
                    run()


class Ring:
    def __init__(self, axis):
        n, me = lax.axis_size(axis), lax.axis_index(axis)
        chip, core = lax.div(me, 2), lax.rem(me, 2)
        self.axis, self.me, self.far = axis, me, n // 4
        steps = range(-self.far, self.far + 1)
        chips = [2 * lax.rem(chip + by + n // 2, n // 2) for by in steps]
        self.own = {by: at + core for by, at in zip(steps, chips)}
        self.other = {by: at + 1 - core for by, at in zip(steps, chips)}

    def meet(self):
        barrier = pltpu.get_barrier_semaphore()
        for to in (self.own[1], self.own[-1], self.other[0]):
            pl.semaphore_signal(barrier, inc=1, device_id={self.axis: to}, device_id_type=pl.DeviceIdType.MESH)
        pl.semaphore_wait(barrier, 3)

    def copy(self, src, dst, sems, at, to):
        return pltpu.make_async_remote_copy(src, dst, sems.at[0, at], sems.at[1, at], device_id={self.axis: to}, device_id_type=pl.DeviceIdType.MESH)


class Gather:
    def __init__(self, ring, w_ref, first, pieces, sems, base):
        far, half = ring.far, pieces // 2
        every = slice(first, first + pieces)
        part = lambda number, way: every if number < far else slice(first, first + half) if way == 1 else slice(first + half, first + pieces)
        self.hops = [(number, way) for number in range(1, far + 1) for way in (1, -1)]
        self.table = {hop: (ring.own[hop[1]], ring.own[(1 - hop[0]) * hop[1]], ring.own[-hop[0] * hop[1]], part(*hop)) for hop in self.hops}
        for number, way in [(0, 1), *self.hops]:
            at = -number * way
            self.table["core", number, way] = ring.other[0], ring.own[at], ring.other[at], part(number, way)
        self.index = {key: base + at for at, key in enumerate(self.table)}
        self.ring, self.w_ref, self.sems = ring, w_ref, sems

    def copy(self, key, comes=False):
        to, sent, arriving, part = self.table[key]
        dst = self.w_ref.at[arriving if comes else sent, part]
        return self.ring.copy(dst, dst, self.sems, self.index[key], to)

    def begin(self):
        for way in (1, -1):
            self.copy((1, way)).start()
        self.copy(("core", 0, 1)).start()

    def step(self, number):
        for way in (1, -1):
            self.copy((number, way), True).wait_recv()
            if number < self.ring.far:
                self.copy((number + 1, way)).start()
            self.copy(("core", number, way)).start()

    def arrive(self):
        for key in self.table:
            if key[0] == "core":
                self.copy(key, True).wait_recv()

    def sent(self):
        for key in self.table:
            self.copy(key).wait_send()


def gather_copies(n):
    return 2 * 2 * (n // 4) + 1


PLACES = 64


def rotary_parts(tokens):
    half = HEAD // 2
    place = np.concatenate([np.arange(PLACES), np.arange(0, tokens, PLACES)]).astype(np.float32)
    angle = place[:, None] * np.float32(THETA) ** (-np.arange(half, dtype=np.float32) / half)
    return np.stack([np.concatenate([f(angle.astype(np.float64))] * 2, axis=1) for f in (np.cos, np.sin)]).astype(np.float32)


def tables(table_ref, first, count):
    near_cos, near_sin = table_ref[0, :PLACES], table_ref[1, :PLACES]
    sign = jnp.where(lax.broadcasted_iota(jnp.int32, (1, HEAD), 1) < HEAD // 2, -1.0, 1.0)
    cos, sin = [], []
    for i in range(count):
        far_cos, far_sin = (table_ref[f, pl.ds(PLACES + first + i, 1)] for f in range(2))
        cos.append(near_cos * far_cos - near_sin * far_sin)
        sin.append((near_sin * far_cos + near_cos * far_sin) * sign)
    return jnp.concatenate(cos), jnp.concatenate(sin)


class Forward:
    def __init__(self, layers, blocks):
        self.layers, self.blocks = layers, blocks
        self.steps = (3 * layers - 1) * blocks

    def at(self, step):
        layer = lax.div(step, 3 * self.blocks)
        return layer, step - 3 * self.blocks * layer

    def block(self, phase):
        return lambda step: (self.at(step)[0], jnp.clip(self.at(step)[1] - phase * self.blocks, 0, self.blocks - 1))


    def points(self):
        durations = {0: 1.6, 1: 1.75, 2: 1.15}
        time, out = 0.0, []
        for step in range(self.steps):
            phase, block = divmod(step % (3 * self.blocks), self.blocks)
            for place in range((1, block + 1, self.blocks)[phase]):
                out.append((time, step, place))
                time += durations[phase]
        return out

    def timed(self, rounds, far):
        hop, delay = 2.8, 2.2
        points, out, link, place = self.points(), [], 0.0, 0

        first_use = lambda job: 3 * self.blocks * job[0] + (2 * self.blocks if job[1] else 0)
        missing = [job for jobs in rounds for job in jobs]

        def add(time, kind, number, job):
            nonlocal place
            limit = min(map(first_use, missing))
            while place < len(points) - 1 and points[place][0] < time and points[place + 1][1:] <= (limit, 0):
                place += 1
            if kind == "arrive":
                missing.remove(job)
            out.append((*points[place][1:], kind, number, job))
            return max(time, points[place][0])

        def send(time, length):
            nonlocal link
            link = max(link, time) + length
            return link + delay

        came = {job: 0.0 for job in rounds[0]}
        for jobs, later in zip(rounds, rounds[1:] + [[]]):
            for number in range(1, far + 1):
                for job in jobs:
                    time = add(came[job], "step", number, job)
                    if number < far:
                        came[job] = send(time, hop if number + 1 < far else hop / 2)
                if number == far - 1:
                    for job in later:
                        came[job] = send(add(link - hop, "begin", 0, job), hop)
            for job in jobs:
                add(came[job] + 1, "arrive", 0, job)
        return out


def _forward(x_ref, table_ref, *rest, plan, scale, axis):
    shards, rest = rest[:7], rest[7:]
    q_ref, k_ref, v_ref, o_ref, lse_ref, h1_ref, hs_ref, w_ref = rest[:8]
    w_s, h_s, q_s, k_s, v_s, top_s, mix_s, x_sem, w_sems, ring_sems = rest[8:]
    step = pl.program_id(0)
    blocks = plan.blocks
    layer, within = plan.at(step)
    bq, width = q_ref.shape[1:]
    n, pieces, rows, _ = w_s.shape[1:]
    group = 4
    heads = width // HEAD
    e = scale * LOG2E
    ring = Ring(axis)
    jobs = {}
    for number in range(plan.layers):
        for first in range(0, pieces, group):
            jobs[number, first // group] = Gather(ring, w_s.at[number], first, group, ring_sems, gather_copies(n) * len(jobs))

    def put(key):
        number, first = key[0], key[1] * group
        cut = lambda ref: ref.at[number, :, first : first + group]
        return pltpu.make_async_copy(cut(w_s), cut(w_ref), w_sems.at[number, key[1]])

    def event(kind, number, key):
        job = jobs[key]
        if kind == "begin":
            job.begin()
        elif kind == "step":
            job.step(number)
        else:
            job.arrive()
            put(key).start()

    groups = pieces // group
    rounds = [[(0, at) for at in range(1, groups)]]
    for number in range(1, plan.layers):
        rounds += [[(number, at), (number, at + 1)] for at in range(0, groups, 2)]
    timed = [(*t[:2], functools.partial(event, *t[2:])) for t in plan.timed(rounds, ring.far)]

    def events(phase, place):
        due([t for t in timed if t[0] % (3 * blocks) // blocks == phase], step, place)

    def pack(number, first):
        at = 0
        for shard in shards:
            for row in range(0, shard.shape[1], rows):
                for column in range(0, shard.shape[2], width):
                    if first <= at < first + group:
                        w_s[number, ring.me, at] = shard[number, row : row + rows, column : column + width]
                    at += 1

    @pl.when(step == 0)
    def _():
        x_copy = pltpu.make_async_copy(x_ref.at[0], h_s, x_sem)
        x_copy.start()
        pack(0, 0)
        ring.meet()
        jobs[0, 0].begin()
        for key in list(jobs)[1:]:
            pack(key[0], key[1] * group)
        for number in range(1, ring.far + 1):
            if number < pieces // group:
                jobs[0, number].begin()
            jobs[0, 0].step(number)
        event("arrive", 0, (0, 0))
        x_copy.wait()

    @pl.when(within < blocks)
    def _():
        events(0, 0)
        here = pl.ds(pl.multiple_of(within * bq, bq), bq)
        hs_ref[0] = h_s[here, :]
        wide = h_s[here, :].astype(F32)
        a = (wide * inverse_rms(wide)).astype(BF16)
        cos, sin = tables(table_ref, within * (bq // PLACES), bq // PLACES)
        for piece, (out_ref, kept) in enumerate(((q_ref, q_s), (k_ref, k_s), (v_ref, v_s))):
            y = dot(a, w_s[layer, :, piece].reshape(width, width)).astype(BF16)
            if piece < 2:
                turned = []
                for at in range(0, width, HEAD):
                    t = y[:, at : at + HEAD].astype(F32)
                    turned.append((t * cos + pltpu.roll(t, HEAD // 2, 1) * sin).astype(BF16))
                y = jnp.concatenate(turned, 1)
            out_ref[0] = y
            kept[here, :] = y

    @pl.when((within >= blocks) & (within < 2 * blocks))
    def _():
        b = within - blocks
        first = pl.multiple_of(b * bq, bq)
        top_s[:] = jnp.full_like(top_s, NEG)
        mix_s[:] = jnp.zeros_like(mix_s)

        def block(at, keys, strips, gap):
            here = pl.ds(at, keys)
            ones = jnp.ones((8, keys), BF16)
            work = [(m, a, w) for m in range(heads) for a, w in strips]
            scores = [dot_t(k_s[here, m * HEAD : (m + 1) * HEAD], q_s[pl.ds(first + a, w), m * HEAD : (m + 1) * HEAD]) for m, a, w in work]
            weights, keeps = [], []
            for (m, a, w), s in zip(work, scores):
                if gap == a:
                    s = jnp.where(lower(keys, w), s, HIDDEN)
                old = top_s[m : m + 1, a : a + w]
                top = jnp.maximum(old, s.max(axis=0, keepdims=True))
                top_s[m : m + 1, a : a + w] = top
                weights.append(jnp.exp2((s - top) * e).astype(BF16))
                keeps.append(jnp.exp2((old - top) * e))
            for (m, a, w), p, keep in zip(work, weights, keeps):
                values = jnp.concatenate([v_s[here, m * HEAD : (m + 1) * HEAD].T, ones])
                mix_s[m, :, a : a + w] = mix_s[m, :, a : a + w] * keep + dot(values, p)

        def before(j, _):
            events(1, j)
            block(pl.multiple_of(j * bq, bq), bq, [(0, bq)], None)

        lax.fori_loop(0, b, before, None)
        events(1, b)
        half = bq // 2
        block(first, half, [(0, half), (half, half)], 0)
        block(pl.multiple_of(first + half, half), half, [(half, half)], half)
        for m in range(heads):
            top, total = top_s[m : m + 1, :], mix_s[m, HEAD : HEAD + 1, :]
            o_ref[0, :, m * HEAD : (m + 1) * HEAD] = (mix_s[m, :HEAD, :] * (1 / total)).T.astype(BF16)
            lse_ref[0, m : m + 1, :] = top * e + jnp.log2(total)
        here = pl.ds(first, bq)
        h1 = h_s[here, :] + dot(o_ref[0], w_s[layer, :, 3].reshape(width, width)).astype(BF16)
        h_s[here, :] = h1
        h1_ref[0] = h1

    @pl.when(within >= 2 * blocks)
    def _():
        here = pl.ds(pl.multiple_of((within - 2 * blocks) * bq, bq), bq)
        wide = h_s[here, :].astype(F32)
        b = (wide * inverse_rms(wide)).astype(BF16)
        parts = (pieces - group) // 3
        owners = n // parts
        y = None
        for j in range(parts):
            events(2, j)
            gate = dot(b, w_s[layer, :, group + j].reshape(width, width))
            up = dot(b, w_s[layer, :, group + parts + j].reshape(width, width))
            act = (gate * sigmoid(gate) * up).astype(BF16)
            part = dot(act, w_s[layer, owners * j : owners * (j + 1), group + 2 * parts :].reshape(width, width))
            y = part if y is None else y + part
        h_s[here, :] += y.astype(BF16)

    @pl.when(step == plan.steps - 1)
    def _():
        for key, job in jobs.items():
            job.sent()
            put(key).wait()


def forward(x, shards, axis, n, pieces, number, bq=512):
    _, s, d = x.shape
    layers, rows = shards[0].shape[:2]
    heads, plan = d // HEAD, Forward(layers, s // bq)
    table = rotary_parts(s)
    block = lambda index: pl.BlockSpec((1, bq, d), lambda i: (*index(i), 0))
    out = jax.ShapeDtypeStruct((layers, s, d), BF16)
    weights = (layers, n, pieces, rows, d)
    return pl.pallas_call(
        functools.partial(_forward, plan=plan, scale=HEAD**-0.5, axis=axis),
        grid=(plan.steps,),
        in_specs=[ANYWHERE, held(table), *[held(a) for a in shards]],
        out_specs=[block(plan.block(0))] * 3 + [block(plan.block(1)), pl.BlockSpec((1, heads, bq), lambda i: (plan.block(1)(i)[0], 0, plan.block(1)(i)[1])),
                   block(plan.block(1)), block(plan.block(0)), ANYWHERE],
        out_shape=[out] * 4 + [jax.ShapeDtypeStruct((layers, heads, s), F32), out, out, jax.ShapeDtypeStruct(weights, BF16)],
        scratch_shapes=[pltpu.VMEM(weights, BF16)] + [pltpu.VMEM((s, d), BF16)] * 4
        + [pltpu.VMEM((heads, bq), F32), pltpu.VMEM((heads, HEAD + 8, bq), F32), pltpu.SemaphoreType.DMA, pltpu.SemaphoreType.DMA((layers, pieces // 4)),
           pltpu.SemaphoreType.DMA((2, layers * (pieces // 4) * gather_copies(n)))],
        compiler_params=comm_params(number),
        cost_estimate=cost(layers * (2 * s * s * d + 32 * s * d * d), *[x] * 8, exps=layers * heads * s * s // 2),
        name="forward",
    )(x, table, *shards)


class Scatter:
    def __init__(self, ring, dw, out, core_s, come_s, core_sems, hop_sems):
        far, pieces = ring.far, dw.shape[1]
        halves = (slice(0, pieces // 2), slice(pieces // 2, pieces))
        targets = [far] + [way * by for by in range(far - 1, 0, -1) for way in (1, -1)] + [0]
        slot = {by: at for at, by in enumerate(targets)} | {-far: 0}
        ways = lambda number, half: (1, -1) if number > 1 else (1 - 2 * half,)
        hops = [(number, half, way) for number in range(1, far + 1) for half in (0, 1) for way in ways(number, half)]
        index = {hop: at for at, hop in enumerate(hops)}

        def share(by):
            return ring.copy(dw.at[ring.other[by]], core_s.at[slot[by]], core_sems, slot[by], ring.other[0])

        def going(hop):
            number, half, way = hop
            return dw.at[ring.own[way * (far - number + 1)], halves[half]]

        def move(hop):
            return ring.copy(going(hop), come_s.at[index[hop]], hop_sems, index[hop], ring.own[hop[2]])

        def total(dst, by, half, came):
            first = halves[half].start
            some = 3 if pieces % 3 == 0 else 2

            def add(i, _):
                for p in (i * some + at for at in range(some)):
                    terms = [dw[ring.own[by], first + p], core_s[slot[by], first + p]] + [come_s[index[hop], p] for hop in came]
                    dst[p] = sum(x.astype(F32) for x in terms).astype(BF16)

            lax.fori_loop(0, pieces // 2 // some, add, None)

        def begin():
            for by in targets[:3]:
                share(by).start()

        def step(number, half):
            if half == 0:
                for at in sorted({slot[way * (far - number + 1)] for way in (1, -1)}):
                    share(targets[at]).wait_recv()
            for way in ways(number, half):
                came = [hop for hop in [(number - 1, half, way)] if hop in index]
                for hop in came:
                    move(hop).wait_recv()
                total(going((number, half, way)), way * (far - number + 1), half, came)
            for way in ways(number, half):
                move((number, half, way)).start()
            if half == 1:
                for by in targets[2 * number + 1 : 2 * number + 3]:
                    share(by).start()

        def finish(half):
            if half == 0:
                share(0).wait_recv()
            came = [(far, half, way) for way in (1, -1)]
            for hop in came:
                move(hop).wait_recv()
            total(out.at[halves[half]], 0, half, came)

        def end():
            for hop in hops:
                move(hop).wait_send()
            for by in targets:
                share(by).wait_send()

        self.events = [begin] + [functools.partial(step, number, half) for number in range(1, far + 1) for half in (0, 1)]
        self.events += [functools.partial(finish, half) for half in (0, 1)] + [end]

    @staticmethod
    def scratch(n, pieces, rows, d):
        hops = 2 + 4 * (n // 4 - 1)
        whole, half = (pltpu.VMEM((count, share, rows, d), BF16) for count, share in ((n // 2, pieces), (hops, pieces // 2)))
        return [whole, half, pltpu.SemaphoreType.DMA((2, n // 2)), pltpu.SemaphoreType.DMA((2, hops))]


def norm_back(wide, by_normed):
    r = inverse_rms(wide)
    normed = wide * r
    return r * (by_normed - normed * jnp.mean(normed * by_normed, -1, keepdims=True))


class Backward:
    def __init__(self, layers, hidden, blocks):
        self.layers, self.hidden, self.blocks = layers, hidden, blocks
        self.per = hidden + 2 * blocks

    def at(self, step):
        turn = lax.div(step, self.per)
        return self.layers - 1 - turn, step - self.per * turn

    def block(self, *firsts):
        def index(step):
            layer, within = self.at(step)
            out = jnp.int32(0)
            for first in firsts:
                out = jnp.where(within >= first, jnp.clip(within - first, 0, self.blocks - 1), out)
            return layer, out

        return index

    def weights(self, step):
        layer, within = self.at(step)
        return jnp.where(within < self.hidden, layer, jnp.maximum(layer - 1, 0)), jnp.where(within < self.hidden, within, 0)


def _backward(dy_ref, h1_ref, wg_ref, wu_ref, wd_ref, q_ref, k_ref, v_ref, o_ref, lse_ref, h_ref, wa_ref, table_ref, ga_ref, gf_ref,
              dh_s, lhs_s, rhs_s, sum_s, dv_s, dq_s, do_s, delta_s, dwa_s, dwf_s, load_sems, *scratch, plan, scale, axis):
    step = pl.program_id(0)
    layer, within = plan.at(step)
    hidden, blocks = plan.hidden, plan.blocks
    s, d = h1_ref.shape
    t = bq = s // blocks
    n, _, rows, _ = dwa_s.shape
    heads = d // HEAD
    e = scale * LOG2E
    cuts = [slice(m * HEAD, (m + 1) * HEAD) for m in range(heads)]
    flat = lambda w: w.reshape(d, d)
    rows_of = lambda block: slice(block * t, block * t + t) if isinstance(block, int) else pl.ds(pl.multiple_of(block * t, t), t)
    first_lhs, second_lhs = lhs_s.at[0], lhs_s.at[1]
    b_s, act_s, dup_s, dgate_s = (rhs_s.at[i] for i in range(4))
    dqs_s, k_s, v_s, was_s = b_s, act_s, dup_s, dgate_s

    ring = Ring(axis)
    half = len(scratch) // 2
    inside = [(hidden + b, place) for b in range(blocks) for place in range(b + 1)]
    after = [(hidden + blocks + b, 0) for b in range(blocks)]
    turns = (0, 1, 1, 4, 4, 7, 9, 10, 11, 12, 13, 13)
    before = [(j, place) for j in range(hidden) for place in range(3)]
    sum_f = Scatter(ring, dwf_s, gf_ref.at[layer], *scratch[half:]).events
    sum_a = lambda layer: Scatter(ring, dwa_s, ga_ref.at[layer], *scratch[:half]).events
    timed_f = [(*(inside + after)[turn], event) for turn, event in zip(turns, sum_f)]
    timed_a = [(*point, event) for point, event in zip(before, sum_a(jnp.minimum(layer + 1, plan.layers - 1)))]
    due_inside = lambda place: due([x for x in timed_f if x[:2] in inside], within, place)

    def due_before(place):
        @pl.when(layer < plan.layers - 1)
        def _():
            due(timed_a, within, place)

    def load(src, dst, at):
        return pltpu.make_async_copy(src, dst, load_sems.at[at])

    @pl.when(step == 0)
    def _():
        copy = load(dy_ref.at[0], dh_s, 0)
        copy.start()
        ring.meet()
        copy.wait()

    @pl.when(within < hidden)
    def _():
        j = within
        due_before(0)
        wg, wu, wd = (flat(r[:]) for r in (wg_ref, wu_ref, wd_ref))

        @pl.when(j == 0)
        def _():
            def strip(i, _):
                here = rows_of(i)
                wide = h1_ref[here, :].astype(F32)
                b = (wide * inverse_rms(wide)).astype(BF16)
                b_s[here, :] = b
                first_lhs[:, here] = b.T
                second_lhs[:, here] = dh_s[here, :].T
                sum_s[here, :] = jnp.zeros((t, d), F32)

            lax.fori_loop(0, blocks, strip, None)

        def products(here):
            b = b_s[here, :]
            return dot(b, wg), dot(b, wu), dot_t(dh_s[here, :], wd).astype(BF16)

        def bends(here, gate, up, dact):
            dact = dact.astype(F32)
            sig = sigmoid(gate)
            silu = gate * sig
            act_s[here, :] = (silu * up).astype(BF16)
            dup_s[here, :] = (dact * silu).astype(BF16)
            dgate_s[here, :] = (dact * up * (sig + silu * (1 - sig))).astype(BF16)

        def sums(here):
            sum_s[here, :] += dot_t(dgate_s[here, :], wg) + dot_t(dup_s[here, :], wu)

        made = {}
        for at in range(blocks + 2):
            if at == 3:
                due_before(1)
            if at < blocks:
                made[at] = products(rows_of(at))
            if 1 <= at <= blocks:
                bends(rows_of(at - 1), *made.pop(at - 1))
            if at >= 2:
                sums(rows_of(at - 2))
        due_before(2)

        def gradients(i, _):
            dwf_s[:, i * hidden + j] = dot(first_lhs[:], rhs_s[3 - i]).astype(BF16).reshape(n, rows, d)

        lax.fori_loop(0, 2, gradients, None)
        part = n // hidden
        dwf_s[pl.ds(j * part, part), 2 * hidden :] = dot(second_lhs[:], act_s[:]).T.astype(BF16).reshape(part, hidden, rows, d)

        @pl.when(j == hidden - 1)
        def _():
            for at, (src, dst) in enumerate(((k_ref, k_s), (v_ref, v_s))):
                load(src.at[layer], dst, at).start()

            def strip(i, _):
                here = rows_of(i)
                grad = norm_back(h1_ref[here, :].astype(F32), sum_s[here, :].astype(BF16).astype(F32))
                dh_s[here, :] = (dh_s[here, :].astype(F32) + grad).astype(BF16)

            lax.fori_loop(0, blocks, strip, None)
            for at, (src, dst) in enumerate(((k_ref, k_s), (v_ref, v_s))):
                load(src.at[layer], dst, at).wait()

    @pl.when((within >= hidden) & (within < hidden + blocks))
    def _():
        i = within - hidden
        first = pl.multiple_of(i * bq, bq)
        mine = pl.ds(first, bq)
        dq_s[:] = jnp.zeros_like(dq_s)
        do = dot_t(dh_s[mine, :], flat(wa_ref[:, 3])).astype(BF16)
        do_s[:] = do
        for m, cut in enumerate(cuts):
            delta_s[m : m + 1, :] = (do[:, cut].astype(F32) * o_ref[:, cut].astype(F32)).T.sum(axis=0, keepdims=True)

        def block(at, keys, strips, gap):
            here = pl.ds(at, keys)
            work = [(cut, m, a, w) for m, cut in enumerate(cuts) for a, w in strips]
            scores = [dot_t(k_s[here, cut], q_ref[a : a + w, cut]) for cut, m, a, w in work]
            dps = [dot_t(v_s[here, cut], do_s[a : a + w, cut]) for cut, m, a, w in work]
            for (cut, m, a, w), score, dp in zip(work, scores, dps):
                p = jnp.exp2(score * e - lse_ref[m : m + 1, a : a + w])
                if gap == a:
                    p = jnp.where(lower(keys, w), p, 0.0)
                ds = (p * (dp - delta_s[m : m + 1, a : a + w])).astype(BF16)
                by_v, by_k = dot(p.astype(BF16), do_s[a : a + w, cut]), dot(ds, q_ref[a : a + w, cut])
                if gap == a:
                    dv_s[here, cut] = by_v
                    sum_s[here, cut] = by_k
                else:
                    dv_s[here, cut] += by_v
                    sum_s[here, cut] += by_k
                dq_s[m, :, a : a + w] += dot(k_s[here, cut].T, ds)

        def earlier(j, _):
            due_inside(j)
            block(pl.multiple_of(j * bq, bq), bq, [(0, bq)], None)

        lax.fori_loop(0, i, earlier, None)
        due_inside(i)
        half = bq // 2
        block(first, half, [(0, half), (half, half)], 0)
        block(pl.multiple_of(first + half, half), half, [(half, half)], half)
        for m, cut in enumerate(cuts):
            dqs_s[mine, cut] = (dq_s[m] * scale).T.astype(BF16)

    @pl.when(within >= hidden + blocks)
    def _():
        b = within - hidden - blocks
        due([x for x in timed_f if x[:2] in after], within, 0)
        here = rows_of(b)
        wide = h_ref[:].astype(F32)
        first_lhs[:, here] = (wide * inverse_rms(wide)).astype(BF16).T
        second_lhs[:, here] = o_ref[:].T
        cos, sin = tables(table_ref, b * (bq // PLACES), bq // PLACES)

        def back(x):
            parts = []
            for cut in cuts:
                part = x[:, cut].astype(F32)
                parts.append((part * cos - pltpu.roll(part, HEAD // 2, 1) * sin).astype(BF16))
            return jnp.concatenate(parts, axis=1)

        terms = [back(dqs_s[here, :]), back((sum_s[here, :] * scale).astype(BF16)), dv_s[here, :].astype(BF16)]
        for p, x in enumerate(terms):
            rhs_s[p, here, :] = x
        was = dh_s[here, :]
        was_s[here, :] = was

        @pl.when(layer > 0)
        def _():
            by_a = sum(dot_t(rhs_s[p, here, :], flat(wa_ref[:, p])) for p in range(3)).astype(BF16).astype(F32)
            dh_s[here, :] = (was.astype(F32) + norm_back(wide, by_a)).astype(BF16)

        @pl.when(b == blocks - 1)
        def _():
            def gradients(p, _):
                dwa_s[:, p] = dot(lhs_s[lax.div(p, 3)], rhs_s[p]).astype(BF16).reshape(n, rows, d)

            lax.fori_loop(0, 4, gradients, None)

    @pl.when(step == plan.layers * plan.per - 1)
    def _():
        for event in sum_a(0):
            event()


def backward(dy, hs, kept, h1, w, axis, number, bq=512):
    layers, s, d = hs.shape
    _, n, pieces, rows, _ = w.shape
    own = 4
    heads, hidden, blocks = d // HEAD, (pieces - own) // 3, s // bq
    part = n // hidden
    plan = Backward(layers, hidden, blocks)
    table = rotary_parts(s)
    whole = lambda shape: once((None, *shape), lambda i: (plan.at(i)[0], *[0] * len(shape)))
    row = lambda *firsts: pl.BlockSpec((None, bq, d), lambda i: (*plan.block(*firsts)(i), 0))
    column = lambda first: pl.BlockSpec((None, n, 1, rows, d), lambda i: (plan.weights(i)[0], 0, first + plan.weights(i)[1], 0, 0))
    lse = lambda i: (plan.block(hidden)(i)[0], 0, plan.block(hidden)(i)[1])
    sums = [jax.ShapeDtypeStruct((layers, count, rows, d), BF16) for count in (own, pieces - own)]
    state, terms = pltpu.VMEM((s, d), F32), [(n, count, rows, d) for count in (own, pieces - own)]
    return pl.pallas_call(
        functools.partial(_backward, plan=plan, scale=HEAD**-0.5, axis=axis),
        grid=(layers * plan.per,),
        in_specs=[ANYWHERE, whole((s, d)), column(own), column(own + hidden),
                  pl.BlockSpec((None, part, hidden, rows, d), lambda i: (plan.weights(i)[0], plan.weights(i)[1], pieces // hidden - 1, 0, 0)),
                  row(hidden), ANYWHERE, ANYWHERE, row(hidden, hidden + blocks), pl.BlockSpec((None, heads, bq), lse), row(hidden + blocks),
                  whole((n, own, rows, d)), held(table)],
        out_specs=[*map(resident, sums)],
        out_shape=sums,
        scratch_shapes=[pltpu.VMEM((s, d), BF16), pltpu.VMEM((2, d, s), BF16), pltpu.VMEM((4, s, d), BF16), state, state,
                        pltpu.VMEM((heads, HEAD, bq), F32), pltpu.VMEM((bq, d), BF16), pltpu.VMEM((heads, bq), F32)]
        + [pltpu.VMEM(shape, BF16) for shape in terms] + [pltpu.SemaphoreType.DMA((2,))] + [x for shape in terms for x in Scatter.scratch(*shape)],
        compiler_params=comm_params(number),
        cost_estimate=cost(layers * (5 * s * s * d + 80 * s * d * d), *[dy] * 16, exps=layers * heads * s * s),
        name="backward",
    )(dy, h1, w, w, w, kept[0], kept[1], kept[2], kept[3], kept[4], hs, w, table)


def _adamw(*refs):
    sums, w_refs, m_refs, v_refs, outs = refs[:2], refs[2:9], refs[9:16], refs[16:23], refs[23:]
    first, every = 0, slice(None)
    for i, (w_ref, m_ref, v_ref) in enumerate(zip(w_refs, m_refs, v_refs)):
        g_ref, first = sums[i >= 4], 0 if i == 4 else first
        rows, d = g_ref.shape[2:]
        pieces = w_ref.shape[1] * w_ref.shape[2] // (rows * d)
        for p in range(pieces):
            cut = lambda size: slice(p * size, p * size + size)
            at = (0, every, cut(d)) if w_ref.shape[2] > d else (0, cut(rows), every)
            g = g_ref[0, first + p].astype(F32)
            m = 0.9 * m_ref[at] + 0.1 * g
            v = 0.95 * v_ref[at] + 0.05 * g * g
            w = w_ref[at].astype(F32)
            outs[i][at] = (w - 0.02 * (m * lax.rsqrt(v + 1e-8) + 0.1 * w)).astype(BF16)
            outs[7 + i][at] = m
            outs[14 + i][at] = v
        first += pieces


def adamw(sums, weights, ms, vs):
    spec = lambda a: pl.BlockSpec((1, *a.shape[1:]), lambda i: (i, *[0] * (a.ndim - 1)))
    state = (*weights, *ms, *vs)
    return pl.pallas_call(
        _adamw,
        grid=(weights[0].shape[0],),
        in_specs=[spec(a) for a in (*sums, *state)],
        out_specs=[spec(a) for a in state],
        out_shape=[jax.ShapeDtypeStruct(a.shape, a.dtype) for a in state],
        compiler_params=comm_params(None),
        cost_estimate=cost(20 * sum(a.size for a in weights), *state, *state),
        name="adamw",
    )(*sums, *state)


def solution(mesh):
    axis, n = "dp", mesh.shape["dp"]

    def step(x, dy, *arrays):
        weights, ms, vs = (arrays[i : i + 7] for i in (0, 7, 14))
        d, ff = x.shape[2], weights[4].shape[2]
        *kept, h1, hs, w = forward(x, weights, axis, n, 4 + 3 * ff // d, 0)
        return tuple(adamw(backward(dy, hs, kept, h1, w, axis, 1), weights, ms, vs))

    states, cut = P(("rep", "dp"), None, None), P(None, "dp", None)
    return jax.shard_map(
        step,
        mesh=mesh,
        in_specs=(states, states) + (cut,) * 21,
        out_specs=(P("rep", "dp", None),) * 21,
        check_vma=False,
    )
```

```python
import functools
import itertools

import jax
import jax.numpy as jnp
import numpy as np
from jax import lax
from jax.experimental import pallas as pl
from jax.experimental.pallas import tpu as pltpu
from jax.sharding import PartitionSpec as P

F32, BF16 = jnp.float32, jnp.bfloat16
HEAD = 128
THETA = 10000
NEG = -1e30
HIDDEN = 2 * NEG
LOG2E = 1.4426950408889634
VMEM = 62 * 2**20


def contract(a, b, ca, cb):
    return lax.dot_general(a, b, (((ca,), (cb,)), ((), ())), preferred_element_type=F32)


def dot(a, b):
    return contract(a, b, 1, 0)


def dot_t(a, b):
    return contract(a, b, 1, 1)


def comm_params(number):
    return pltpu.CompilerParams(dimension_semantics=("arbitrary",), vmem_limit_bytes=VMEM, collective_id=number, has_side_effects=number is not None)


def cost(flops, *arrays, exps=0):
    return pl.CostEstimate(flops=flops, transcendentals=exps, bytes_accessed=sum(a.size * a.dtype.itemsize for a in arrays))


def once(shape, index):
    return pl.BlockSpec(shape, index, pipeline_mode=pl.Buffered(1))


def fixed(*index):
    return lambda i: index


def held(a):
    return once(a.shape, fixed(*[0] * a.ndim))


def resident(a):
    return pl.BlockSpec(a.shape, fixed(*[0] * len(a.shape)))


ANYWHERE = pl.BlockSpec(memory_space=pl.ANY)


def inverse_rms(wide):
    return lax.rsqrt(jnp.mean(wide * wide, -1, keepdims=True) + 1e-6)


def sigmoid(x):
    return 1 / (1 + jnp.exp(-x))


def lower(keys, queries):
    place = lambda dim: lax.broadcasted_iota(jnp.int32, (keys, queries), dim)
    return place(1) >= place(0)


def due(timed, step, place):
    for at in sorted({t[0] for t in timed}):

        @pl.when(step == at)
        def _():
            for first, second, run in timed:
                if first == at and not isinstance(place, int):
                    pl.when(place == second)(run)
                elif first == at and place == second:
                    run()


class Ring:
    def __init__(self, axis):
        n, me = lax.axis_size(axis), lax.axis_index(axis)
        chip, core = lax.div(me, 2), lax.rem(me, 2)
        self.axis, self.me, self.far = axis, me, n // 4
        steps = range(-self.far, self.far + 1)
        chips = [2 * lax.rem(chip + by + n // 2, n // 2) for by in steps]
        self.own = {by: at + core for by, at in zip(steps, chips)}
        self.other = {by: at + 1 - core for by, at in zip(steps, chips)}

    def meet(self):
        barrier = pltpu.get_barrier_semaphore()
        for to in (self.own[1], self.own[-1], self.other[0]):
            pl.semaphore_signal(barrier, inc=1, device_id={self.axis: to}, device_id_type=pl.DeviceIdType.MESH)
        pl.semaphore_wait(barrier, 3)

    def copy(self, src, dst, sems, at, to):
        return pltpu.make_async_remote_copy(src, dst, sems.at[0, at], sems.at[1, at], device_id={self.axis: to}, device_id_type=pl.DeviceIdType.MESH)


class Gather:
    def __init__(self, ring, w_ref, first, pieces, sems, base):
        far, half = ring.far, pieces // 2
        every = slice(first, first + pieces)
        part = lambda number, way: every if number < far else slice(first, first + half) if way == 1 else slice(first + half, first + pieces)
        self.hops = [(number, way) for number in range(1, far + 1) for way in (1, -1)]
        self.table = {hop: (ring.own[hop[1]], ring.own[(1 - hop[0]) * hop[1]], ring.own[-hop[0] * hop[1]], part(*hop)) for hop in self.hops}
        for number, way in [(0, 1), *self.hops]:
            at = -number * way
            self.table["core", number, way] = ring.other[0], ring.own[at], ring.other[at], part(number, way)
        self.index = {key: base + at for at, key in enumerate(self.table)}
        self.ring, self.w_ref, self.sems = ring, w_ref, sems

    def copy(self, key, comes=False):
        to, sent, arriving, part = self.table[key]
        dst = self.w_ref.at[arriving if comes else sent, part]
        return self.ring.copy(dst, dst, self.sems, self.index[key], to)

    def begin(self):
        for way in (1, -1):
            self.copy((1, way)).start()
        self.copy(("core", 0, 1)).start()

    def step(self, number):
        for way in (1, -1):
            self.copy((number, way), True).wait_recv()
            if number < self.ring.far:
                self.copy((number + 1, way)).start()
            self.copy(("core", number, way)).start()

    def arrive(self):
        for key in self.table:
            if key[0] == "core":
                self.copy(key, True).wait_recv()

    def sent(self):
        for key in self.table:
            self.copy(key).wait_send()


def gather_copies(n):
    return 2 * 2 * (n // 4) + 1


PLACES = 64


def rotary_parts(tokens):
    half = HEAD // 2
    place = np.concatenate([np.arange(PLACES), np.arange(0, tokens, PLACES)]).astype(np.float32)
    angle = place[:, None] * np.float32(THETA) ** (-np.arange(half, dtype=np.float32) / half)
    return np.stack([np.concatenate([f(angle.astype(np.float64))] * 2, axis=1) for f in (np.cos, np.sin)]).astype(np.float32)


def tables(table_ref, first, count):
    near_cos, near_sin = table_ref[0, :PLACES], table_ref[1, :PLACES]
    sign = jnp.where(lax.broadcasted_iota(jnp.int32, (1, HEAD), 1) < HEAD // 2, -1.0, 1.0)
    cos, sin = [], []
    for i in range(count):
        far_cos, far_sin = (table_ref[f, pl.ds(PLACES + first + i, 1)] for f in range(2))
        cos.append(near_cos * far_cos - near_sin * far_sin)
        sin.append((near_sin * far_cos + near_cos * far_sin) * sign)
    return jnp.concatenate(cos), jnp.concatenate(sin)


class Forward:
    def __init__(self, layers, blocks):
        self.layers, self.blocks = layers, blocks
        self.steps = (3 * layers - 1) * blocks

    def at(self, step):
        layer = lax.div(step, 3 * self.blocks)
        return layer, step - 3 * self.blocks * layer

    def block(self, phase):
        return lambda step: (self.at(step)[0], jnp.clip(self.at(step)[1] - phase * self.blocks, 0, self.blocks - 1))


    def points(self):
        durations = {0: 1.6, 1: 1.75, 2: 1.15}
        time, out = 0.0, []
        for step in range(self.steps):
            phase, block = divmod(step % (3 * self.blocks), self.blocks)
            for place in range((1, block + 1, self.blocks)[phase]):
                out.append((time, step, place))
                time += durations[phase]
        return out

    def timed(self, rounds, far):
        hop, delay = 2.8, 2.2
        points, out, link, place = self.points(), [], 0.0, 0

        first_use = lambda job: 3 * self.blocks * job[0] + (2 * self.blocks if job[1] else 0)
        missing = [job for jobs in rounds for job in jobs]

        def add(time, kind, number, job):
            nonlocal place
            limit = min(map(first_use, missing))
            while place < len(points) - 1 and points[place][0] < time and points[place + 1][1:] <= (limit, 0):
                place += 1
            if kind == "arrive":
                missing.remove(job)
            out.append((*points[place][1:], kind, number, job))
            return max(time, points[place][0])

        def send(time, length):
            nonlocal link
            link = max(link, time) + length
            return link + delay

        came = {job: 0.0 for job in rounds[0]}
        for jobs, later in zip(rounds, rounds[1:] + [[]]):
            for number in range(1, far + 1):
                for job in jobs:
                    time = add(came[job], "step", number, job)
                    if number < far:
                        came[job] = send(time, hop if number + 1 < far else hop / 2)
                if number == far - 1:
                    for job in later:
                        came[job] = send(add(link - hop, "begin", 0, job), hop)
            for job in jobs:
                add(came[job] + 1, "arrive", 0, job)
        return out


def _forward(x_ref, table_ref, *rest, plan, scale, axis):
    shards, rest = rest[:7], rest[7:]
    q_ref, k_ref, v_ref, o_ref, lse_ref, at_ref, ot_ref, h1_ref, hs_ref, w_ref = rest[:10]
    w_s, h_s, q_s, k_s, v_s, top_s, mix_s, x_sem, w_sems, ring_sems = rest[10:]
    step = pl.program_id(0)
    blocks = plan.blocks
    layer, within = plan.at(step)
    bq, width = q_ref.shape[1:]
    n, pieces, rows, _ = w_s.shape[1:]
    group = 4
    heads = width // HEAD
    e = scale * LOG2E
    ring = Ring(axis)
    jobs = {}
    for number in range(plan.layers):
        for first in range(0, pieces, group):
            jobs[number, first // group] = Gather(ring, w_s.at[number], first, group, ring_sems, gather_copies(n) * len(jobs))

    def put(key):
        number, first = key[0], key[1] * group
        cut = lambda ref: ref.at[number, :, first : first + group]
        return pltpu.make_async_copy(cut(w_s), cut(w_ref), w_sems.at[number, key[1]])

    def event(kind, number, key):
        job = jobs[key]
        if kind == "begin":
            job.begin()
        elif kind == "step":
            job.step(number)
        else:
            job.arrive()
            put(key).start()

    groups = pieces // group
    rounds = [[(0, at) for at in range(1, groups)]]
    for number in range(1, plan.layers):
        rounds += [[(number, at), (number, at + 1)] for at in range(0, groups, 2)]
    timed = [(*t[:2], functools.partial(event, *t[2:])) for t in plan.timed(rounds, ring.far)]

    def events(phase, place):
        due([t for t in timed if t[0] % (3 * blocks) // blocks == phase], step, place)

    def pack(number, first):
        at = 0
        for shard in shards:
            for row in range(0, shard.shape[1], rows):
                for column in range(0, shard.shape[2], width):
                    if first <= at < first + group:
                        w_s[number, ring.me, at] = shard[number, row : row + rows, column : column + width]
                    at += 1

    @pl.when(step == 0)
    def _():
        x_copy = pltpu.make_async_copy(x_ref.at[0], h_s, x_sem)
        x_copy.start()
        pack(0, 0)
        ring.meet()
        jobs[0, 0].begin()
        for key in list(jobs)[1:]:
            pack(key[0], key[1] * group)
        for number in range(1, ring.far + 1):
            if number < pieces // group:
                jobs[0, number].begin()
            jobs[0, 0].step(number)
        event("arrive", 0, (0, 0))
        x_copy.wait()

    @pl.when(within < blocks)
    def _():
        events(0, 0)
        here = pl.ds(pl.multiple_of(within * bq, bq), bq)
        hs_ref[0] = h_s[here, :]
        wide = h_s[here, :].astype(F32)
        a = (wide * inverse_rms(wide)).astype(BF16)
        at_ref[0] = a.T
        cos, sin = tables(table_ref, within * (bq // PLACES), bq // PLACES)
        for piece, (out_ref, kept) in enumerate(((q_ref, q_s), (k_ref, k_s), (v_ref, v_s))):
            y = dot(a, w_s[layer, :, piece].reshape(width, width)).astype(BF16)
            if piece < 2:
                turned = []
                for at in range(0, width, HEAD):
                    t = y[:, at : at + HEAD].astype(F32)
                    turned.append((t * cos + pltpu.roll(t, HEAD // 2, 1) * sin).astype(BF16))
                y = jnp.concatenate(turned, 1)
            out_ref[0] = y
            kept[here, :] = y

    @pl.when((within >= blocks) & (within < 2 * blocks))
    def _():
        b = within - blocks
        first = pl.multiple_of(b * bq, bq)
        top_s[:] = jnp.full_like(top_s, NEG)
        mix_s[:] = jnp.zeros_like(mix_s)

        def block(at, keys, strips, gap):
            here = pl.ds(at, keys)
            ones = jnp.ones((8, keys), BF16)
            work = [(m, a, w) for m in range(heads) for a, w in strips]
            scores = [dot_t(k_s[here, m * HEAD : (m + 1) * HEAD], q_s[pl.ds(first + a, w), m * HEAD : (m + 1) * HEAD]) for m, a, w in work]
            weights, keeps = [], []
            for (m, a, w), s in zip(work, scores):
                if gap == a:
                    s = jnp.where(lower(keys, w), s, HIDDEN)
                old = top_s[m : m + 1, a : a + w]
                top = jnp.maximum(old, s.max(axis=0, keepdims=True))
                top_s[m : m + 1, a : a + w] = top
                weights.append(jnp.exp2((s - top) * e).astype(BF16))
                keeps.append(jnp.exp2((old - top) * e))
            for (m, a, w), p, keep in zip(work, weights, keeps):
                values = jnp.concatenate([v_s[here, m * HEAD : (m + 1) * HEAD].T, ones])
                mix_s[m, :, a : a + w] = mix_s[m, :, a : a + w] * keep + dot(values, p)

        def before(j, _):
            events(1, j)
            block(pl.multiple_of(j * bq, bq), bq, [(0, bq)], None)

        lax.fori_loop(0, b, before, None)
        events(1, b)
        half = bq // 2
        block(first, half, [(0, half), (half, half)], 0)
        block(pl.multiple_of(first + half, half), half, [(half, half)], half)
        for m in range(heads):
            top, total = top_s[m : m + 1, :], mix_s[m, HEAD : HEAD + 1, :]
            part = (mix_s[m, :HEAD, :] * (1 / total)).astype(BF16)
            ot_ref[0, m * HEAD : (m + 1) * HEAD, :] = part
            o_ref[0, :, m * HEAD : (m + 1) * HEAD] = part.T
            lse_ref[0, m : m + 1, :] = top * e + jnp.log2(total)
        here = pl.ds(first, bq)
        h1 = h_s[here, :] + dot(o_ref[0], w_s[layer, :, 3].reshape(width, width)).astype(BF16)
        h_s[here, :] = h1
        h1_ref[0] = h1

    @pl.when(within >= 2 * blocks)
    def _():
        here = pl.ds(pl.multiple_of((within - 2 * blocks) * bq, bq), bq)
        wide = h_s[here, :].astype(F32)
        b = (wide * inverse_rms(wide)).astype(BF16)
        parts = (pieces - group) // 3
        owners = n // parts
        y = None
        for j in range(parts):
            events(2, j)
            gate = dot(b, w_s[layer, :, group + j].reshape(width, width))
            up = dot(b, w_s[layer, :, group + parts + j].reshape(width, width))
            act = (gate * sigmoid(gate) * up).astype(BF16)
            part = dot(act, w_s[layer, owners * j : owners * (j + 1), group + 2 * parts :].reshape(width, width))
            y = part if y is None else y + part
        h_s[here, :] += y.astype(BF16)

    @pl.when(step == plan.steps - 1)
    def _():
        for key, job in jobs.items():
            job.sent()
            put(key).wait()


def forward(x, shards, axis, n, pieces, number, bq=512):
    _, s, d = x.shape
    layers, rows = shards[0].shape[:2]
    heads, plan = d // HEAD, Forward(layers, s // bq)
    table = rotary_parts(s)
    block = lambda index: pl.BlockSpec((1, bq, d), lambda i: (*index(i), 0))
    across = lambda height, index: pl.BlockSpec((1, height, bq), lambda i: (index(i)[0], 0, index(i)[1]))
    flat = jax.ShapeDtypeStruct((layers, d, s), BF16)
    out = jax.ShapeDtypeStruct((layers, s, d), BF16)
    weights = (layers, n, pieces, rows, d)
    return pl.pallas_call(
        functools.partial(_forward, plan=plan, scale=HEAD**-0.5, axis=axis),
        grid=(plan.steps,),
        in_specs=[ANYWHERE, held(table), *[held(a) for a in shards]],
        out_specs=[block(plan.block(0))] * 3 + [block(plan.block(1)), across(heads, plan.block(1)), across(d, plan.block(0)), across(d, plan.block(1)),
                   block(plan.block(1)), block(plan.block(0)), ANYWHERE],
        out_shape=[out] * 4 + [jax.ShapeDtypeStruct((layers, heads, s), F32), flat, flat, out, out, jax.ShapeDtypeStruct(weights, BF16)],
        scratch_shapes=[pltpu.VMEM(weights, BF16)] + [pltpu.VMEM((s, d), BF16)] * 4
        + [pltpu.VMEM((heads, bq), F32), pltpu.VMEM((heads, HEAD + 8, bq), F32), pltpu.SemaphoreType.DMA, pltpu.SemaphoreType.DMA((layers, pieces // 4)),
           pltpu.SemaphoreType.DMA((2, layers * (pieces // 4) * gather_copies(n)))],
        compiler_params=comm_params(number),
        cost_estimate=cost(layers * (2 * s * s * d + 32 * s * d * d), *[x] * 8, exps=layers * heads * s * s // 2),
        name="forward",
    )(x, table, *shards)


class Scatter:
    def __init__(self, ring, dw, out, core_s, come_s, core_sems, hop_sems):
        far, pieces = ring.far, dw.shape[1]
        halves = (slice(0, pieces // 2), slice(pieces // 2, pieces))
        targets = [far] + [way * by for by in range(far - 1, 0, -1) for way in (1, -1)] + [0]
        slot = {by: at for at, by in enumerate(targets)} | {-far: 0}
        ways = lambda number, half: (1, -1) if number > 1 else (1 - 2 * half,)
        hops = [(number, half, way) for number in range(1, far + 1) for half in (0, 1) for way in ways(number, half)]
        index = {hop: at for at, hop in enumerate(hops)}

        def share(by):
            return ring.copy(dw.at[ring.other[by]], core_s.at[slot[by]], core_sems, slot[by], ring.other[0])

        def going(hop):
            number, half, way = hop
            return dw.at[ring.own[way * (far - number + 1)], halves[half]]

        def move(hop):
            return ring.copy(going(hop), come_s.at[index[hop]], hop_sems, index[hop], ring.own[hop[2]])

        def total(dst, by, half, came):
            first = halves[half].start
            some = next(k for k in (3, 2, 1) if pieces // 2 % k == 0)

            def add(i, _):
                for p in (i * some + at for at in range(some)):
                    terms = [dw[ring.own[by], first + p], core_s[slot[by], first + p]] + [come_s[index[hop], p] for hop in came]
                    dst[p] = sum(x.astype(F32) for x in terms).astype(BF16)

            lax.fori_loop(0, pieces // 2 // some, add, None)

        def begin():
            for by in targets[:3]:
                share(by).start()

        def step(number, half):
            if half == 0:
                for at in sorted({slot[way * (far - number + 1)] for way in (1, -1)}):
                    share(targets[at]).wait_recv()
            for way in ways(number, half):
                came = [hop for hop in [(number - 1, half, way)] if hop in index]
                for hop in came:
                    move(hop).wait_recv()
                total(going((number, half, way)), way * (far - number + 1), half, came)
            for way in ways(number, half):
                move((number, half, way)).start()
            if half == 1:
                for by in targets[2 * number + 1 : 2 * number + 3]:
                    share(by).start()

        def finish(half):
            if half == 0:
                share(0).wait_recv()
            came = [(far, half, way) for way in (1, -1)]
            for hop in came:
                move(hop).wait_recv()
            total(out.at[halves[half]], 0, half, came)

        def end():
            for hop in hops:
                move(hop).wait_send()
            for by in targets:
                share(by).wait_send()

        self.events = [begin] + [functools.partial(step, number, half) for number in range(1, far + 1) for half in (0, 1)]
        self.events += [functools.partial(finish, half) for half in (0, 1)] + [end]

    @staticmethod
    def scratch(n, pieces, rows, d):
        hops = 2 + 4 * (n // 4 - 1)
        whole, half = (pltpu.VMEM((count, share, rows, d), BF16) for count, share in ((n // 2, pieces), (hops, pieces // 2)))
        return [whole, half, pltpu.SemaphoreType.DMA((2, n // 2)), pltpu.SemaphoreType.DMA((2, hops))]


def norm_back(wide, by_normed):
    r = inverse_rms(wide)
    normed = wide * r
    return r * (by_normed - normed * jnp.mean(normed * by_normed, -1, keepdims=True))


class Backward:
    def __init__(self, layers, hidden, blocks):
        self.layers, self.hidden, self.blocks = layers, hidden, blocks
        self.per = hidden + 2 * blocks

    def at(self, step):
        turn = lax.div(step, self.per)
        return self.layers - 1 - turn, step - self.per * turn

    def block(self, first):
        return lambda step: (self.at(step)[0], jnp.clip(self.at(step)[1] - first, 0, self.blocks - 1))

    def weights(self, step):
        layer, within = self.at(step)
        return jnp.where(within < self.hidden, layer, jnp.maximum(layer - 1, 0)), jnp.where(within < self.hidden, within, 0)


def _backward(dy_ref, h1_ref, wg_ref, wu_ref, wd_ref, q_ref, k_ref, v_ref, o_ref, lse_ref, at_ref, ot_ref, h_ref, wa_ref, table_ref, ga_ref, gf_ref,
              dh_s, lhs_s, rhs_s, sum_s, dv_s, dq_s, do_s, delta_s, dwa_s, dwf_s, load_sems, *scratch, plan, scale, axis):
    step = pl.program_id(0)
    layer, within = plan.at(step)
    hidden, blocks = plan.hidden, plan.blocks
    s, d = h1_ref.shape
    t = bq = s // blocks
    n, _, rows, _ = dwa_s.shape
    heads = d // HEAD
    e = scale * LOG2E
    cuts = [slice(m * HEAD, (m + 1) * HEAD) for m in range(heads)]
    flat = lambda w: w.reshape(d, d)
    rows_of = lambda block: slice(block * t, block * t + t) if isinstance(block, int) else pl.ds(pl.multiple_of(block * t, t), t)
    first_lhs, second_lhs = lhs_s.at[0], lhs_s.at[1]
    b_s, act_s, dup_s, dgate_s = (rhs_s.at[i] for i in range(4))
    dqs_s, k_s, v_s, was_s = b_s, act_s, dup_s, dgate_s

    ring = Ring(axis)
    third = len(scratch) // 3
    inside = [(hidden + b, place) for b in range(blocks) for place in range(b + 1)]
    after = [(hidden + blocks + b, 0) for b in range(blocks)]
    before = [(j, place) for j in range(hidden) for place in range(3)]

    def sums(layer):
        parts = ((dwa_s.at[:, :2], ga_ref.at[layer, :2]), (dwa_s.at[:, 2:], ga_ref.at[layer, 2:]), (dwf_s, gf_ref.at[layer]))
        return [Scatter(ring, *part, *scratch[third * i : third * (i + 1)]).events for i, part in enumerate(parts)]

    _, of_vo, of_f = sums(layer)
    soon_f, soon_vo = range(9), range(7)
    timed_f = [(*(inside + after)[max(i > 0, (3 * i - 3) // 2)], of_f[i]) for i in soon_f] + [(*after[1 + (i + 1) // 3], of_vo[i]) for i in soon_vo]

    def later(layer):
        of_qk, of_vo, of_f = sums(layer)
        return itertools.zip_longest(of_qk, of_f[len(soon_f) :] + of_vo[len(soon_vo) :], fillvalue=lambda: None)

    timed_a = [(*point, event) for point, pair in zip(before, later(jnp.minimum(layer + 1, plan.layers - 1))) for event in pair]
    due_inside = lambda place: due([x for x in timed_f if x[:2] in inside], within, place)

    def due_before(place):
        @pl.when(layer < plan.layers - 1)
        def _():
            due(timed_a, within, place)

    def load(src, dst, at):
        return pltpu.make_async_copy(src, dst, load_sems.at[at])

    def loads():
        pairs = ((k_ref, k_s), (v_ref, v_s), (at_ref, first_lhs), (ot_ref, second_lhs))
        return [load(src.at[layer], dst, at) for at, (src, dst) in enumerate(pairs)]

    @pl.when(step == 0)
    def _():
        copy = load(dy_ref.at[0], dh_s, 0)
        copy.start()
        ring.meet()
        copy.wait()

    @pl.when(within < hidden)
    def _():
        j = within
        due_before(0)
        wg, wu, wd = (flat(r[:]) for r in (wg_ref, wu_ref, wd_ref))

        @pl.when(j == 0)
        def _():
            def strip(i, _):
                here = rows_of(i)
                wide = h1_ref[here, :].astype(F32)
                b = (wide * inverse_rms(wide)).astype(BF16)
                b_s[here, :] = b
                first_lhs[:, here] = b.T
                second_lhs[:, here] = dh_s[here, :].T
                sum_s[here, :] = jnp.zeros((t, d), F32)

            lax.fori_loop(0, blocks, strip, None)

        def products(here):
            b = b_s[here, :]
            return dot(b, wg), dot(b, wu), dot_t(dh_s[here, :], wd).astype(BF16)

        def bends(here, gate, up, dact):
            dact = dact.astype(F32)
            sig = sigmoid(gate)
            silu = gate * sig
            act_s[here, :] = (silu * up).astype(BF16)
            dup_s[here, :] = (dact * silu).astype(BF16)
            dgate_s[here, :] = (dact * up * (sig + silu * (1 - sig))).astype(BF16)

        def pass_on(here):
            sum_s[here, :] += dot_t(dgate_s[here, :], wg) + dot_t(dup_s[here, :], wu)

        made = {}
        for at in range(blocks + 2):
            if at == 3:
                due_before(1)
            if at < blocks:
                made[at] = products(rows_of(at))
            if 1 <= at <= blocks:
                bends(rows_of(at - 1), *made.pop(at - 1))
            if at >= 2:
                pass_on(rows_of(at - 2))
        due_before(2)

        def gradients(i, _):
            dwf_s[:, i * hidden + j] = dot(first_lhs[:], rhs_s[3 - i]).astype(BF16).reshape(n, rows, d)

        lax.fori_loop(0, 2, gradients, None)
        part = n // hidden
        dwf_s[pl.ds(j * part, part), 2 * hidden :] = dot(second_lhs[:], act_s[:]).T.astype(BF16).reshape(part, hidden, rows, d)

        @pl.when(j == hidden - 1)
        def _():
            for copy in loads():
                copy.start()

            def strip(i, _):
                here = rows_of(i)
                grad = norm_back(h1_ref[here, :].astype(F32), sum_s[here, :].astype(BF16).astype(F32))
                dh_s[here, :] = (dh_s[here, :].astype(F32) + grad).astype(BF16)

            lax.fori_loop(0, blocks, strip, None)
            for copy in loads()[:2]:
                copy.wait()

    @pl.when((within >= hidden) & (within < hidden + blocks))
    def _():
        i = within - hidden
        first = pl.multiple_of(i * bq, bq)
        mine = pl.ds(first, bq)
        dq_s[:] = jnp.zeros_like(dq_s)
        do = dot_t(dh_s[mine, :], flat(wa_ref[:, 3])).astype(BF16)
        do_s[:] = do
        for m, cut in enumerate(cuts):
            delta_s[m : m + 1, :] = (do[:, cut].astype(F32) * o_ref[:, cut].astype(F32)).T.sum(axis=0, keepdims=True)

        def block(at, keys, strips, gap):
            here = pl.ds(at, keys)
            work = [(cut, m, a, w) for m, cut in enumerate(cuts) for a, w in strips]
            scores = [dot_t(k_s[here, cut], q_ref[a : a + w, cut]) for cut, m, a, w in work]
            dps = [dot_t(v_s[here, cut], do_s[a : a + w, cut]) for cut, m, a, w in work]
            for (cut, m, a, w), score, dp in zip(work, scores, dps):
                p = jnp.exp2(score * e - lse_ref[m : m + 1, a : a + w])
                if gap == a:
                    p = jnp.where(lower(keys, w), p, 0.0)
                ds = (p * (dp - delta_s[m : m + 1, a : a + w])).astype(BF16)
                by_v, by_k = dot(p.astype(BF16), do_s[a : a + w, cut]), dot(ds, q_ref[a : a + w, cut])
                if gap == a:
                    dv_s[here, cut] = by_v
                    sum_s[here, cut] = by_k
                else:
                    dv_s[here, cut] += by_v
                    sum_s[here, cut] += by_k
                dq_s[m, :, a : a + w] += dot(k_s[here, cut].T, ds)

        def earlier(j, _):
            due_inside(j)
            block(pl.multiple_of(j * bq, bq), bq, [(0, bq)], None)

        lax.fori_loop(0, i, earlier, None)
        due_inside(i)
        half = bq // 2
        block(first, half, [(0, half), (half, half)], 0)
        block(pl.multiple_of(first + half, half), half, [(half, half)], half)
        for m, cut in enumerate(cuts):
            dqs_s[mine, cut] = (dq_s[m] * scale).T.astype(BF16)

    @pl.when(within >= hidden + blocks)
    def _():
        b = within - hidden - blocks
        due([x for x in timed_f if x[:2] in after], within, 0)
        here = rows_of(b)

        @pl.when(b == 0)
        def _():
            for copy in loads()[2:]:
                copy.wait()

            def strip(i, _):
                rhs_s[2, rows_of(i), :] = dv_s[rows_of(i), :].astype(BF16)
                was_s[rows_of(i), :] = dh_s[rows_of(i), :]

            lax.fori_loop(0, blocks, strip, None)

            def gradients(i, _):
                dwa_s[:, 2 + i] = dot(lhs_s[i], rhs_s[2 + i]).astype(BF16).reshape(n, rows, d)

            lax.fori_loop(0, 2, gradients, None)

        cos, sin = tables(table_ref, b * (bq // PLACES), bq // PLACES)
        for p, x in enumerate((dqs_s[here, :], (sum_s[here, :] * scale).astype(BF16))):
            for cut in cuts:
                part = x[:, cut].astype(F32)
                rhs_s[p, here, cut] = (part * cos - pltpu.roll(part, HEAD // 2, 1) * sin).astype(BF16)

        @pl.when(layer > 0)
        def _():
            by_a = sum(dot_t(rhs_s[p, here, :], flat(wa_ref[:, p])) for p in range(3)).astype(BF16).astype(F32)
            dh_s[here, :] = (dh_s[here, :].astype(F32) + norm_back(h_ref[:].astype(F32), by_a)).astype(BF16)

        @pl.when(b == blocks - 1)
        def _():
            def gradients(p, _):
                dwa_s[:, p] = dot(first_lhs[:], rhs_s[p]).astype(BF16).reshape(n, rows, d)

            lax.fori_loop(0, 2, gradients, None)

    @pl.when(step == plan.layers * plan.per - 1)
    def _():
        for event in itertools.chain(*later(0)):
            event()


def backward(dy, kept, h1, hs, w, axis, number, bq=512):
    layers, s, d = hs.shape
    _, n, pieces, rows, _ = w.shape
    own = 4
    heads, hidden, blocks = d // HEAD, (pieces - own) // 3, s // bq
    part = n // hidden
    plan = Backward(layers, hidden, blocks)
    table = rotary_parts(s)
    whole = lambda shape: once((None, *shape), lambda i: (plan.at(i)[0], *[0] * len(shape)))
    row = lambda first: pl.BlockSpec((None, bq, d), lambda i: (*plan.block(first)(i), 0))
    column = lambda first: pl.BlockSpec((None, n, 1, rows, d), lambda i: (plan.weights(i)[0], 0, first + plan.weights(i)[1], 0, 0))
    lse = lambda i: (plan.block(hidden)(i)[0], 0, plan.block(hidden)(i)[1])
    sums = [jax.ShapeDtypeStruct((layers, count, rows, d), BF16) for count in (own, pieces - own)]
    state, terms = pltpu.VMEM((s, d), F32), [(n, count, rows, d) for count in (own, pieces - own)]
    return pl.pallas_call(
        functools.partial(_backward, plan=plan, scale=HEAD**-0.5, axis=axis),
        grid=(layers * plan.per,),
        in_specs=[ANYWHERE, whole((s, d)), column(own), column(own + hidden),
                  pl.BlockSpec((None, part, hidden, rows, d), lambda i: (plan.weights(i)[0], plan.weights(i)[1], pieces // hidden - 1, 0, 0)),
                  row(hidden), ANYWHERE, ANYWHERE, row(hidden), pl.BlockSpec((None, heads, bq), lse), ANYWHERE, ANYWHERE, row(hidden + blocks),
                  whole((n, own, rows, d)), held(table)],
        out_specs=[*map(resident, sums)],
        out_shape=sums,
        scratch_shapes=[pltpu.VMEM((s, d), BF16), pltpu.VMEM((2, d, s), BF16), pltpu.VMEM((4, s, d), BF16), state, state,
                        pltpu.VMEM((heads, HEAD, bq), F32), pltpu.VMEM((bq, d), BF16), pltpu.VMEM((heads, bq), F32)]
        + [pltpu.VMEM(shape, BF16) for shape in terms] + [pltpu.SemaphoreType.DMA((4,))]
        + [x for count in (2, own - 2, pieces - own) for x in Scatter.scratch(n, count, rows, d)],
        compiler_params=comm_params(number),
        cost_estimate=cost(layers * (5 * s * s * d + 80 * s * d * d), *[dy] * 16, exps=layers * heads * s * s),
        name="backward",
    )(dy, h1, w, w, w, *kept, hs, w, table)


def _adamw(*refs):
    sums, w_refs, m_refs, v_refs, outs = refs[:2], refs[2:9], refs[9:16], refs[16:23], refs[23:]
    first, every = 0, slice(None)
    for i, (w_ref, m_ref, v_ref) in enumerate(zip(w_refs, m_refs, v_refs)):
        g_ref, first = sums[i >= 4], 0 if i == 4 else first
        rows, d = g_ref.shape[2:]
        pieces = w_ref.shape[1] * w_ref.shape[2] // (rows * d)
        for p in range(pieces):
            cut = lambda size: slice(p * size, p * size + size)
            at = (0, every, cut(d)) if w_ref.shape[2] > d else (0, cut(rows), every)
            g = g_ref[0, first + p].astype(F32)
            m = 0.9 * m_ref[at] + 0.1 * g
            v = 0.95 * v_ref[at] + 0.05 * g * g
            w = w_ref[at].astype(F32)
            outs[i][at] = (w - 0.02 * (m * lax.rsqrt(v + 1e-8) + 0.1 * w)).astype(BF16)
            outs[7 + i][at] = m
            outs[14 + i][at] = v
        first += pieces


def adamw(sums, weights, ms, vs):
    spec = lambda a: pl.BlockSpec((1, *a.shape[1:]), lambda i: (i, *[0] * (a.ndim - 1)))
    state = (*weights, *ms, *vs)
    return pl.pallas_call(
        _adamw,
        grid=(weights[0].shape[0],),
        in_specs=[spec(a) for a in (*sums, *state)],
        out_specs=[spec(a) for a in state],
        out_shape=[jax.ShapeDtypeStruct(a.shape, a.dtype) for a in state],
        compiler_params=comm_params(None),
        cost_estimate=cost(20 * sum(a.size for a in weights), *state, *state),
        name="adamw",
    )(*sums, *state)


def solution(mesh):
    axis, n = "dp", mesh.shape["dp"]

    def step(x, dy, *arrays):
        weights, ms, vs = (arrays[i : i + 7] for i in (0, 7, 14))
        d, ff = x.shape[2], weights[4].shape[2]
        *kept, h1, hs, w = forward(x, weights, axis, n, 4 + 3 * ff // d, 0)
        return tuple(adamw(backward(dy, kept, h1, hs, w, axis, 1), weights, ms, vs))

    states, cut = P(("rep", "dp"), None, None), P(None, "dp", None)
    return jax.shard_map(
        step,
        mesh=mesh,
        in_specs=(states, states) + (cut,) * 21,
        out_specs=(P("rep", "dp", None),) * 21,
        check_vma=False,
    )
```

```python
import functools
import itertools

import jax
import jax.numpy as jnp
import numpy as np
from jax import lax
from jax.experimental import pallas as pl
from jax.experimental.pallas import tpu as pltpu
from jax.sharding import PartitionSpec as P

F32, BF16 = jnp.float32, jnp.bfloat16
HEAD = 128
THETA = 10000
NEG = -1e30
HIDDEN = 2 * NEG
LOG2E = 1.4426950408889634
VMEM = 62 * 2**20


def contract(a, b, ca, cb):
    return lax.dot_general(a, b, (((ca,), (cb,)), ((), ())), preferred_element_type=F32)


def dot(a, b):
    return contract(a, b, 1, 0)


def dot_t(a, b):
    return contract(a, b, 1, 1)


def comm_params(number):
    return pltpu.CompilerParams(dimension_semantics=("arbitrary",), vmem_limit_bytes=VMEM, collective_id=number, has_side_effects=number is not None)


def cost(flops, *arrays, exps=0):
    return pl.CostEstimate(flops=flops, transcendentals=exps, bytes_accessed=sum(a.size * a.dtype.itemsize for a in arrays))


def once(shape, index):
    return pl.BlockSpec(shape, index, pipeline_mode=pl.Buffered(1))


def fixed(*index):
    return lambda i: index


def held(a):
    return once(a.shape, fixed(*[0] * a.ndim))


def resident(a):
    return pl.BlockSpec(a.shape, fixed(*[0] * len(a.shape)))


ANYWHERE = pl.BlockSpec(memory_space=pl.ANY)


def inverse_rms(wide):
    return lax.rsqrt(jnp.mean(wide * wide, -1, keepdims=True) + 1e-6)


def sigmoid(x):
    return 1 / (1 + jnp.exp(-x))


def lower(keys, queries):
    place = lambda dim: lax.broadcasted_iota(jnp.int32, (keys, queries), dim)
    return place(1) >= place(0)


def due(timed, step, place):
    for at in sorted({t[0] for t in timed}):

        @pl.when(step == at)
        def _():
            for first, second, run in timed:
                if first == at and not isinstance(place, int):
                    pl.when(place == second)(run)
                elif first == at and place == second:
                    run()


class Ring:
    def __init__(self, axis):
        n, me = lax.axis_size(axis), lax.axis_index(axis)
        chip, core = lax.div(me, 2), lax.rem(me, 2)
        self.axis, self.me, self.far = axis, me, n // 4
        steps = range(-self.far, self.far + 1)
        chips = [2 * lax.rem(chip + by + n // 2, n // 2) for by in steps]
        self.own = {by: at + core for by, at in zip(steps, chips)}
        self.other = {by: at + 1 - core for by, at in zip(steps, chips)}

    def meet(self):
        barrier = pltpu.get_barrier_semaphore()
        for to in (self.own[1], self.own[-1], self.other[0]):
            pl.semaphore_signal(barrier, inc=1, device_id={self.axis: to}, device_id_type=pl.DeviceIdType.MESH)
        pl.semaphore_wait(barrier, 3)

    def copy(self, src, dst, sems, at, to):
        return pltpu.make_async_remote_copy(src, dst, sems.at[0, at], sems.at[1, at], device_id={self.axis: to}, device_id_type=pl.DeviceIdType.MESH)


class Gather:
    def __init__(self, ring, w_ref, first, pieces, sems, base):
        far, half = ring.far, pieces // 2
        every = slice(first, first + pieces)
        part = lambda number, way: every if number < far else slice(first, first + half) if way == 1 else slice(first + half, first + pieces)
        self.hops = [(number, way) for number in range(1, far + 1) for way in (1, -1)]
        self.table = {hop: (ring.own[hop[1]], ring.own[(1 - hop[0]) * hop[1]], ring.own[-hop[0] * hop[1]], part(*hop)) for hop in self.hops}
        for number, way in [(0, 1), *self.hops]:
            at = -number * way
            self.table["core", number, way] = ring.other[0], ring.own[at], ring.other[at], part(number, way)
        self.index = {key: base + at for at, key in enumerate(self.table)}
        self.ring, self.w_ref, self.sems = ring, w_ref, sems

    def copy(self, key, comes=False):
        to, sent, arriving, part = self.table[key]
        dst = self.w_ref.at[arriving if comes else sent, part]
        return self.ring.copy(dst, dst, self.sems, self.index[key], to)

    def begin(self):
        for way in (1, -1):
            self.copy((1, way)).start()
        self.copy(("core", 0, 1)).start()

    def step(self, number):
        for way in (1, -1):
            self.copy((number, way), True).wait_recv()
            if number < self.ring.far:
                self.copy((number + 1, way)).start()
            self.copy(("core", number, way)).start()

    def arrive(self):
        for key in self.table:
            if key[0] == "core":
                self.copy(key, True).wait_recv()

    def sent(self):
        for key in self.table:
            self.copy(key).wait_send()


def gather_copies(n):
    return 2 * 2 * (n // 4) + 1


PLACES = 64


def rotary_parts(tokens):
    half = HEAD // 2
    place = np.concatenate([np.arange(PLACES), np.arange(0, tokens, PLACES)]).astype(np.float32)
    angle = place[:, None] * np.float32(THETA) ** (-np.arange(half, dtype=np.float32) / half)
    return np.stack([np.concatenate([f(angle.astype(np.float64))] * 2, axis=1) for f in (np.cos, np.sin)]).astype(np.float32)


def tables(table_ref, first, count):
    near_cos, near_sin = table_ref[0, :PLACES], table_ref[1, :PLACES]
    sign = jnp.where(lax.broadcasted_iota(jnp.int32, (1, HEAD), 1) < HEAD // 2, -1.0, 1.0)
    cos, sin = [], []
    for i in range(count):
        far_cos, far_sin = (table_ref[f, pl.ds(PLACES + first + i, 1)] for f in range(2))
        cos.append(near_cos * far_cos - near_sin * far_sin)
        sin.append((near_sin * far_cos + near_cos * far_sin) * sign)
    return jnp.concatenate(cos), jnp.concatenate(sin)


class Forward:
    def __init__(self, layers, blocks):
        self.layers, self.blocks = layers, blocks
        self.steps = (3 * layers - 1) * blocks

    def at(self, step):
        layer = lax.div(step, 3 * self.blocks)
        return layer, step - 3 * self.blocks * layer

    def block(self, phase):
        return lambda step: (self.at(step)[0], jnp.clip(self.at(step)[1] - phase * self.blocks, 0, self.blocks - 1))


    def points(self):
        durations = {0: 1.6, 1: 1.75, 2: 1.15}
        time, out = 0.0, []
        for step in range(self.steps):
            phase, block = divmod(step % (3 * self.blocks), self.blocks)
            for place in range((1, block + 1, self.blocks)[phase]):
                out.append((time, step, place))
                time += durations[phase]
        return out

    def timed(self, rounds, far):
        hop, delay = 2.8, 2.2
        points, out, link, place = self.points(), [], 0.0, 0

        first_use = lambda job: 3 * self.blocks * job[0] + (2 * self.blocks if job[1] else 0)
        missing = [job for jobs in rounds for job in jobs]

        def add(time, kind, number, job):
            nonlocal place
            limit = min(map(first_use, missing))
            while place < len(points) - 1 and points[place][0] < time and points[place + 1][1:] <= (limit, 0):
                place += 1
            if kind == "arrive":
                missing.remove(job)
            out.append((*points[place][1:], kind, number, job))
            return max(time, points[place][0])

        def send(time, length):
            nonlocal link
            link = max(link, time) + length
            return link + delay

        came = {job: 0.0 for job in rounds[0]}
        for jobs, later in zip(rounds, rounds[1:] + [[]]):
            for number in range(1, far + 1):
                for job in jobs:
                    time = add(came[job], "step", number, job)
                    if number < far:
                        came[job] = send(time, hop if number + 1 < far else hop / 2)
                if number == far - 1:
                    for job in later:
                        came[job] = send(add(link - hop, "begin", 0, job), hop)
            for job in jobs:
                add(came[job] + 1, "arrive", 0, job)
        return out


def _forward(x_ref, table_ref, *rest, plan, scale, axis):
    shards, rest = rest[:7], rest[7:]
    q_ref, k_ref, v_ref, o_ref, lse_ref, at_ref, ot_ref, h1_ref, hs_ref, w_ref = rest[:10]
    w_s, h_s, q_s, k_s, v_s, top_s, mix_s, x_sem, w_sems, ring_sems = rest[10:]
    step = pl.program_id(0)
    blocks = plan.blocks
    layer, within = plan.at(step)
    bq, width = q_ref.shape[1:]
    n, pieces, rows, _ = w_s.shape[1:]
    group = 4
    heads = width // HEAD
    e = scale * LOG2E
    ring = Ring(axis)
    jobs = {}
    for number in range(plan.layers):
        for first in range(0, pieces, group):
            jobs[number, first // group] = Gather(ring, w_s.at[number], first, group, ring_sems, gather_copies(n) * len(jobs))

    def put(key):
        number, first = key[0], key[1] * group
        cut = lambda ref: ref.at[number, :, first : first + group]
        return pltpu.make_async_copy(cut(w_s), cut(w_ref), w_sems.at[number, key[1]])

    def event(kind, number, key):
        job = jobs[key]
        if kind == "begin":
            job.begin()
        elif kind == "step":
            job.step(number)
        else:
            job.arrive()
            put(key).start()

    groups = pieces // group
    rounds = [[(0, at) for at in range(1, groups)]]
    for number in range(1, plan.layers):
        rounds += [[(number, at), (number, at + 1)] for at in range(0, groups, 2)]
    timed = [(*t[:2], functools.partial(event, *t[2:])) for t in plan.timed(rounds, ring.far)]

    def events(phase, place):
        due([t for t in timed if t[0] % (3 * blocks) // blocks == phase], step, place)

    def pack(number, first):
        at = 0
        for shard in shards:
            for row in range(0, shard.shape[1], rows):
                for column in range(0, shard.shape[2], width):
                    if first <= at < first + group:
                        w_s[number, ring.me, at] = shard[number, row : row + rows, column : column + width]
                    at += 1

    @pl.when(step == 0)
    def _():
        x_copy = pltpu.make_async_copy(x_ref.at[0], h_s, x_sem)
        x_copy.start()
        pack(0, 0)
        ring.meet()
        jobs[0, 0].begin()
        for key in list(jobs)[1:]:
            pack(key[0], key[1] * group)
        for number in range(1, ring.far + 1):
            if number < pieces // group:
                jobs[0, number].begin()
            jobs[0, 0].step(number)
        event("arrive", 0, (0, 0))
        x_copy.wait()

    @pl.when(within < blocks)
    def _():
        events(0, 0)
        here = pl.ds(pl.multiple_of(within * bq, bq), bq)
        hs_ref[0] = h_s[here, :]
        wide = h_s[here, :].astype(F32)
        a = (wide * inverse_rms(wide)).astype(BF16)
        at_ref[0] = a.T
        cos, sin = tables(table_ref, within * (bq // PLACES), bq // PLACES)
        for piece, (out_ref, kept) in enumerate(((q_ref, q_s), (k_ref, k_s), (v_ref, v_s))):
            y = dot(a, w_s[layer, :, piece].reshape(width, width)).astype(BF16)
            if piece < 2:
                turned = []
                for at in range(0, width, HEAD):
                    t = y[:, at : at + HEAD].astype(F32)
                    turned.append((t * cos + pltpu.roll(t, HEAD // 2, 1) * sin).astype(BF16))
                y = jnp.concatenate(turned, 1)
            out_ref[0] = y
            kept[here, :] = y

    @pl.when((within >= blocks) & (within < 2 * blocks))
    def _():
        b = within - blocks
        first = pl.multiple_of(b * bq, bq)
        top_s[:] = jnp.full_like(top_s, NEG)
        mix_s[:] = jnp.zeros_like(mix_s)

        def block(at, keys, strips, gap):
            here = pl.ds(at, keys)
            ones = jnp.ones((8, keys), BF16)
            work = [(m, a, w) for m in range(heads) for a, w in strips]
            scores = [dot_t(k_s[here, m * HEAD : (m + 1) * HEAD], q_s[pl.ds(first + a, w), m * HEAD : (m + 1) * HEAD]) for m, a, w in work]
            weights, keeps = [], []
            for (m, a, w), s in zip(work, scores):
                if gap == a:
                    s = jnp.where(lower(keys, w), s, HIDDEN)
                old = top_s[m : m + 1, a : a + w]
                top = jnp.maximum(old, s.max(axis=0, keepdims=True))
                top_s[m : m + 1, a : a + w] = top
                weights.append(jnp.exp2((s - top) * e).astype(BF16))
                keeps.append(jnp.exp2((old - top) * e))
            for (m, a, w), p, keep in zip(work, weights, keeps):
                values = jnp.concatenate([v_s[here, m * HEAD : (m + 1) * HEAD].T, ones])
                mix_s[m, :, a : a + w] = mix_s[m, :, a : a + w] * keep + dot(values, p)

        def before(j, _):
            events(1, j)
            block(pl.multiple_of(j * bq, bq), bq, [(0, bq)], None)

        lax.fori_loop(0, b, before, None)
        events(1, b)
        half = bq // 2
        block(first, half, [(0, half), (half, half)], 0)
        block(pl.multiple_of(first + half, half), half, [(half, half)], half)
        for m in range(heads):
            top, total = top_s[m : m + 1, :], mix_s[m, HEAD : HEAD + 1, :]
            part = (mix_s[m, :HEAD, :] * (1 / total)).astype(BF16)
            ot_ref[0, m * HEAD : (m + 1) * HEAD, :] = part
            o_ref[0, :, m * HEAD : (m + 1) * HEAD] = part.T
            lse_ref[0, m : m + 1, :] = top * e + jnp.log2(total)
        here = pl.ds(first, bq)
        h1 = h_s[here, :] + dot(o_ref[0], w_s[layer, :, 3].reshape(width, width)).astype(BF16)
        h_s[here, :] = h1
        h1_ref[0] = h1

    @pl.when(within >= 2 * blocks)
    def _():
        here = pl.ds(pl.multiple_of((within - 2 * blocks) * bq, bq), bq)
        wide = h_s[here, :].astype(F32)
        b = (wide * inverse_rms(wide)).astype(BF16)
        parts = (pieces - group) // 3
        owners = n // parts
        y = None
        for j in range(parts):
            events(2, j)
            gate = dot(b, w_s[layer, :, group + j].reshape(width, width))
            up = dot(b, w_s[layer, :, group + parts + j].reshape(width, width))
            act = (gate * sigmoid(gate) * up).astype(BF16)
            part = dot(act, w_s[layer, owners * j : owners * (j + 1), group + 2 * parts :].reshape(width, width))
            y = part if y is None else y + part
        h_s[here, :] += y.astype(BF16)

    @pl.when(step == plan.steps - 1)
    def _():
        for key, job in jobs.items():
            job.sent()
            put(key).wait()


def forward(x, shards, axis, n, pieces, number, bq=512):
    _, s, d = x.shape
    layers, rows = shards[0].shape[:2]
    heads, plan = d // HEAD, Forward(layers, s // bq)
    table = rotary_parts(s)
    block = lambda index: pl.BlockSpec((1, bq, d), lambda i: (*index(i), 0))
    across = lambda height, index: pl.BlockSpec((1, height, bq), lambda i: (index(i)[0], 0, index(i)[1]))
    flat = jax.ShapeDtypeStruct((layers, d, s), BF16)
    out = jax.ShapeDtypeStruct((layers, s, d), BF16)
    weights = (layers, n, pieces, rows, d)
    return pl.pallas_call(
        functools.partial(_forward, plan=plan, scale=HEAD**-0.5, axis=axis),
        grid=(plan.steps,),
        in_specs=[ANYWHERE, held(table), *[held(a) for a in shards]],
        out_specs=[block(plan.block(0))] * 3 + [block(plan.block(1)), across(heads, plan.block(1)), across(d, plan.block(0)), across(d, plan.block(1)),
                   block(plan.block(1)), block(plan.block(0)), ANYWHERE],
        out_shape=[out] * 4 + [jax.ShapeDtypeStruct((layers, heads, s), F32), flat, flat, out, out, jax.ShapeDtypeStruct(weights, BF16)],
        scratch_shapes=[pltpu.VMEM(weights, BF16)] + [pltpu.VMEM((s, d), BF16)] * 4
        + [pltpu.VMEM((heads, bq), F32), pltpu.VMEM((heads, HEAD + 8, bq), F32), pltpu.SemaphoreType.DMA, pltpu.SemaphoreType.DMA((layers, pieces // 4)),
           pltpu.SemaphoreType.DMA((2, layers * (pieces // 4) * gather_copies(n)))],
        compiler_params=comm_params(number),
        cost_estimate=cost(layers * (2 * s * s * d + 32 * s * d * d), *[x] * 8, exps=layers * heads * s * s // 2),
        name="forward",
    )(x, table, *shards)


class Scatter:
    def __init__(self, ring, dw, out, core_s, come_s, core_sems, hop_sems):
        far, pieces = ring.far, dw.shape[1]
        halves = (slice(0, pieces // 2), slice(pieces // 2, pieces))
        targets = [far] + [way * by for by in range(far - 1, 0, -1) for way in (1, -1)] + [0]
        slot = {by: at for at, by in enumerate(targets)} | {-far: 0}
        ways = lambda number, half: (1, -1) if number > 1 else (1 - 2 * half,)
        hops = [(number, half, way) for number in range(1, far + 1) for half in (0, 1) for way in ways(number, half)]
        index = {hop: at for at, hop in enumerate(hops)}

        def share(by):
            return ring.copy(dw.at[ring.other[by]], core_s.at[slot[by]], core_sems, slot[by], ring.other[0])

        def going(hop):
            number, half, way = hop
            return dw.at[ring.own[way * (far - number + 1)], halves[half]]

        def move(hop):
            return ring.copy(going(hop), come_s.at[index[hop]], hop_sems, index[hop], ring.own[hop[2]])

        def total(dst, by, half, came):
            first = halves[half].start
            some = next(k for k in (3, 2, 1) if pieces // 2 % k == 0)

            def add(i, _):
                for p in (i * some + at for at in range(some)):
                    terms = [dw[ring.own[by], first + p], core_s[slot[by], first + p]] + [come_s[index[hop], p] for hop in came]
                    dst[p] = sum(x.astype(F32) for x in terms).astype(BF16)

            lax.fori_loop(0, pieces // 2 // some, add, None)

        def begin():
            for by in targets[:3]:
                share(by).start()

        def step(number, half):
            if half == 0:
                for at in sorted({slot[way * (far - number + 1)] for way in (1, -1)}):
                    share(targets[at]).wait_recv()
            for way in ways(number, half):
                came = [hop for hop in [(number - 1, half, way)] if hop in index]
                for hop in came:
                    move(hop).wait_recv()
                total(going((number, half, way)), way * (far - number + 1), half, came)
            for way in ways(number, half):
                move((number, half, way)).start()
            if half == 1:
                for by in targets[2 * number + 1 : 2 * number + 3]:
                    share(by).start()

        def finish(half):
            if half == 0:
                share(0).wait_recv()
            came = [(far, half, way) for way in (1, -1)]
            for hop in came:
                move(hop).wait_recv()
            total(out.at[halves[half]], 0, half, came)

        def end():
            for hop in hops:
                move(hop).wait_send()
            for by in targets:
                share(by).wait_send()

        self.events = [begin] + [functools.partial(step, number, half) for number in range(1, far + 1) for half in (0, 1)]
        self.events += [functools.partial(finish, half) for half in (0, 1)] + [end]

    @staticmethod
    def scratch(n, pieces, rows, d):
        hops = 2 + 4 * (n // 4 - 1)
        whole, half = (pltpu.VMEM((count, share, rows, d), BF16) for count, share in ((n // 2, pieces), (hops, pieces // 2)))
        return [whole, half, pltpu.SemaphoreType.DMA((2, n // 2)), pltpu.SemaphoreType.DMA((2, hops))]


def norm_back(wide, by_normed):
    r = inverse_rms(wide)
    normed = wide * r
    return r * (by_normed - normed * jnp.mean(normed * by_normed, -1, keepdims=True))


class Backward:
    def __init__(self, layers, hidden, blocks):
        self.layers, self.hidden, self.blocks = layers, hidden, blocks
        self.per = hidden + 2 * blocks

    def at(self, step):
        turn = lax.div(step, self.per)
        return self.layers - 1 - turn, step - self.per * turn

    def block(self, first):
        return lambda step: (self.at(step)[0], jnp.clip(self.at(step)[1] - first, 0, self.blocks - 1))

    def weights(self, step):
        layer, within = self.at(step)
        return jnp.where(within < self.hidden, layer, jnp.maximum(layer - 1, 0)), jnp.where(within < self.hidden, within, 0)


def _backward(dy_ref, h1_ref, wg_ref, wu_ref, wd_ref, q_ref, k_ref, v_ref, o_ref, lse_ref, at_ref, ot_ref, h_ref, wa_ref, table_ref, ga_ref, gf_ref,
              dh_s, lhs_s, rhs_s, sum_s, dv_s, dq_s, do_s, delta_s, dwa_s, dwf_s, load_sems, *scratch, plan, scale, axis):
    step = pl.program_id(0)
    layer, within = plan.at(step)
    hidden, blocks = plan.hidden, plan.blocks
    s, d = h1_ref.shape
    t = bq = s // blocks
    n, _, rows, _ = dwa_s.shape
    heads = d // HEAD
    e = scale * LOG2E
    cuts = [slice(m * HEAD, (m + 1) * HEAD) for m in range(heads)]
    flat = lambda w: w.reshape(d, d)
    rows_of = lambda block: slice(block * t, block * t + t) if isinstance(block, int) else pl.ds(pl.multiple_of(block * t, t), t)
    first_lhs, second_lhs = lhs_s.at[0], lhs_s.at[1]
    b_s, act_s, dup_s, dgate_s = (rhs_s.at[i] for i in range(4))
    dqs_s, k_s, v_s, was_s = b_s, act_s, dup_s, dgate_s

    ring = Ring(axis)
    third = len(scratch) // 3
    inside = [(hidden + b, place) for b in range(blocks) for place in range(b + 1)]
    after = [(hidden + blocks + b, 0) for b in range(blocks)]
    before = [(j, place) for j in range(hidden) for place in range(2)]

    def sums(layer):
        parts = ((dwa_s.at[:, :2], ga_ref.at[layer, :2]), (dwa_s.at[:, 2:], ga_ref.at[layer, 2:]), (dwf_s, gf_ref.at[layer]))
        return [Scatter(ring, *part, *scratch[third * i : third * (i + 1)]).events for i, part in enumerate(parts)]

    _, of_vo, of_f = sums(layer)
    soon_f, soon_vo = range(9), range(3)
    timed_f = [(*(inside + after)[max(i > 0, (3 * i - 3) // 2)], of_f[i]) for i in soon_f] + [(*after[1 + 2 * (i > 0)], of_vo[i]) for i in soon_vo]

    def later(layer):
        of_qk, of_vo, of_f = sums(layer)
        return itertools.zip_longest(of_qk, of_f[len(soon_f) :] + of_vo[len(soon_vo) :], fillvalue=lambda: None)

    timed_a = [(*before[2 * i // 3], event) for i, pair in enumerate(later(jnp.minimum(layer + 1, plan.layers - 1))) for event in pair]
    due_inside = lambda place: due([x for x in timed_f if x[:2] in inside], within, place)

    def due_before(place):
        @pl.when(layer < plan.layers - 1)
        def _():
            due(timed_a, within, place)

    def load(src, dst, at):
        return pltpu.make_async_copy(src, dst, load_sems.at[at])

    def loads():
        pairs = ((k_ref, k_s), (v_ref, v_s), (at_ref, first_lhs), (ot_ref, second_lhs))
        return [load(src.at[layer], dst, at) for at, (src, dst) in enumerate(pairs)]

    @pl.when(step == 0)
    def _():
        copy = load(dy_ref.at[0], dh_s, 0)
        copy.start()
        ring.meet()
        copy.wait()

    @pl.when(within < hidden)
    def _():
        j = within
        due_before(0)
        wg, wu, wd = (flat(r[:]) for r in (wg_ref, wu_ref, wd_ref))

        @pl.when(j == 0)
        def _():
            def strip(i, _):
                here = rows_of(i)
                wide = h1_ref[here, :].astype(F32)
                b = (wide * inverse_rms(wide)).astype(BF16)
                b_s[here, :] = b
                first_lhs[:, here] = b.T
                second_lhs[:, here] = dh_s[here, :].T
                sum_s[here, :] = jnp.zeros((t, d), F32)

            lax.fori_loop(0, blocks, strip, None)

        def products(here):
            b = b_s[here, :]
            return dot(b, wg), dot(b, wu), dot_t(dh_s[here, :], wd).astype(BF16)

        def bends(here, gate, up, dact):
            dact = dact.astype(F32)
            sig = sigmoid(gate)
            silu = gate * sig
            act_s[here, :] = (silu * up).astype(BF16)
            dup_s[here, :] = (dact * silu).astype(BF16)
            dgate_s[here, :] = (dact * up * (sig + silu * (1 - sig))).astype(BF16)

        def pass_on(here):
            sum_s[here, :] += dot_t(dgate_s[here, :], wg) + dot_t(dup_s[here, :], wu)

        made = {}
        for at in range(blocks + 2):
            if at < blocks:
                made[at] = products(rows_of(at))
            if 1 <= at <= blocks:
                bends(rows_of(at - 1), *made.pop(at - 1))
            if at >= 2:
                pass_on(rows_of(at - 2))
        due_before(1)

        def gradients(i, _):
            dwf_s[:, i * hidden + j] = dot(first_lhs[:], rhs_s[3 - i]).astype(BF16).reshape(n, rows, d)

        lax.fori_loop(0, 2, gradients, None)
        part = n // hidden
        dwf_s[pl.ds(j * part, part), 2 * hidden :] = dot(second_lhs[:], act_s[:]).T.astype(BF16).reshape(part, hidden, rows, d)

        @pl.when(j == hidden - 1)
        def _():
            for copy in loads():
                copy.start()

            def strip(i, _):
                here = rows_of(i)
                grad = norm_back(h1_ref[here, :].astype(F32), sum_s[here, :].astype(BF16).astype(F32))
                dh_s[here, :] = (dh_s[here, :].astype(F32) + grad).astype(BF16)

            lax.fori_loop(0, blocks, strip, None)
            for copy in loads()[:2]:
                copy.wait()

    @pl.when((within >= hidden) & (within < hidden + blocks))
    def _():
        i = within - hidden
        first = pl.multiple_of(i * bq, bq)
        mine = pl.ds(first, bq)
        dq_s[:] = jnp.zeros_like(dq_s)
        do = dot_t(dh_s[mine, :], flat(wa_ref[:, 3])).astype(BF16)
        do_s[:] = do
        for m, cut in enumerate(cuts):
            delta_s[m : m + 1, :] = (do[:, cut].astype(F32) * o_ref[:, cut].astype(F32)).T.sum(axis=0, keepdims=True)

        def block(at, keys, strips, gap):
            here = pl.ds(at, keys)
            work = [(cut, m, a, w) for m, cut in enumerate(cuts) for a, w in strips]
            scores = [dot_t(k_s[here, cut], q_ref[a : a + w, cut]) for cut, m, a, w in work]
            dps = [dot_t(v_s[here, cut], do_s[a : a + w, cut]) for cut, m, a, w in work]
            for (cut, m, a, w), score, dp in zip(work, scores, dps):
                p = jnp.exp2(score * e - lse_ref[m : m + 1, a : a + w])
                if gap == a:
                    p = jnp.where(lower(keys, w), p, 0.0)
                ds = (p * (dp - delta_s[m : m + 1, a : a + w])).astype(BF16)
                by_v, by_k = dot(p.astype(BF16), do_s[a : a + w, cut]), dot(ds, q_ref[a : a + w, cut])
                if gap == a:
                    dv_s[here, cut] = by_v
                    sum_s[here, cut] = by_k
                else:
                    dv_s[here, cut] += by_v
                    sum_s[here, cut] += by_k
                dq_s[m, :, a : a + w] += dot(k_s[here, cut].T, ds)

        def earlier(j, _):
            due_inside(j)
            block(pl.multiple_of(j * bq, bq), bq, [(0, bq)], None)

        lax.fori_loop(0, i, earlier, None)
        due_inside(i)
        half = bq // 2
        block(first, half, [(0, half), (half, half)], 0)
        block(pl.multiple_of(first + half, half), half, [(half, half)], half)
        for m, cut in enumerate(cuts):
            dqs_s[mine, cut] = (dq_s[m] * scale).T.astype(BF16)

    @pl.when(within >= hidden + blocks)
    def _():
        b = within - hidden - blocks
        due([x for x in timed_f if x[:2] in after], within, 0)
        here = rows_of(b)

        @pl.when(b == 0)
        def _():
            for copy in loads()[2:]:
                copy.wait()

            def strip(i, _):
                rhs_s[2, rows_of(i), :] = dv_s[rows_of(i), :].astype(BF16)
                was_s[rows_of(i), :] = dh_s[rows_of(i), :]

            lax.fori_loop(0, blocks, strip, None)

            def gradients(i, _):
                dwa_s[:, 2 + i] = dot(lhs_s[i], rhs_s[2 + i]).astype(BF16).reshape(n, rows, d)

            lax.fori_loop(0, 2, gradients, None)

        cos, sin = tables(table_ref, b * (bq // PLACES), bq // PLACES)
        for p, x in enumerate((dqs_s[here, :], (sum_s[here, :] * scale).astype(BF16))):
            for cut in cuts:
                part = x[:, cut].astype(F32)
                rhs_s[p, here, cut] = (part * cos - pltpu.roll(part, HEAD // 2, 1) * sin).astype(BF16)

        @pl.when(layer > 0)
        def _():
            by_a = sum(dot_t(rhs_s[p, here, :], flat(wa_ref[:, p])) for p in range(3)).astype(BF16).astype(F32)
            dh_s[here, :] = (dh_s[here, :].astype(F32) + norm_back(h_ref[:].astype(F32), by_a)).astype(BF16)

        @pl.when(b == blocks - 1)
        def _():
            def gradients(p, _):
                dwa_s[:, p] = dot(first_lhs[:], rhs_s[p]).astype(BF16).reshape(n, rows, d)

            lax.fori_loop(0, 2, gradients, None)

    @pl.when(step == plan.layers * plan.per - 1)
    def _():
        for event in itertools.chain(*later(0)):
            event()


def backward(dy, kept, h1, hs, w, axis, number, bq=512):
    layers, s, d = hs.shape
    _, n, pieces, rows, _ = w.shape
    own = 4
    heads, hidden, blocks = d // HEAD, (pieces - own) // 3, s // bq
    part = n // hidden
    plan = Backward(layers, hidden, blocks)
    table = rotary_parts(s)
    whole = lambda shape: once((None, *shape), lambda i: (plan.at(i)[0], *[0] * len(shape)))
    row = lambda first: pl.BlockSpec((None, bq, d), lambda i: (*plan.block(first)(i), 0))
    column = lambda first: pl.BlockSpec((None, n, 1, rows, d), lambda i: (plan.weights(i)[0], 0, first + plan.weights(i)[1], 0, 0))
    lse = lambda i: (plan.block(hidden)(i)[0], 0, plan.block(hidden)(i)[1])
    sums = [jax.ShapeDtypeStruct((layers, count, rows, d), BF16) for count in (own, pieces - own)]
    state, terms = pltpu.VMEM((s, d), F32), [(n, count, rows, d) for count in (own, pieces - own)]
    return pl.pallas_call(
        functools.partial(_backward, plan=plan, scale=HEAD**-0.5, axis=axis),
        grid=(layers * plan.per,),
        in_specs=[ANYWHERE, whole((s, d)), column(own), column(own + hidden),
                  pl.BlockSpec((None, part, hidden, rows, d), lambda i: (plan.weights(i)[0], plan.weights(i)[1], pieces // hidden - 1, 0, 0)),
                  row(hidden), ANYWHERE, ANYWHERE, row(hidden), pl.BlockSpec((None, heads, bq), lse), ANYWHERE, ANYWHERE, row(hidden + blocks),
                  whole((n, own, rows, d)), held(table)],
        out_specs=[*map(resident, sums)],
        out_shape=sums,
        scratch_shapes=[pltpu.VMEM((s, d), BF16), pltpu.VMEM((2, d, s), BF16), pltpu.VMEM((4, s, d), BF16), state, state,
                        pltpu.VMEM((heads, HEAD, bq), F32), pltpu.VMEM((bq, d), BF16), pltpu.VMEM((heads, bq), F32)]
        + [pltpu.VMEM(shape, BF16) for shape in terms] + [pltpu.SemaphoreType.DMA((4,))]
        + [x for count in (2, own - 2, pieces - own) for x in Scatter.scratch(n, count, rows, d)],
        compiler_params=comm_params(number),
        cost_estimate=cost(layers * (5 * s * s * d + 80 * s * d * d), *[dy] * 16, exps=layers * heads * s * s),
        name="backward",
    )(dy, h1, w, w, w, *kept, hs, w, table)


def _adamw(*refs):
    sums, w_refs, m_refs, v_refs, outs = refs[:2], refs[2:9], refs[9:16], refs[16:23], refs[23:]
    first, every = 0, slice(None)
    for i, (w_ref, m_ref, v_ref) in enumerate(zip(w_refs, m_refs, v_refs)):
        g_ref, first = sums[i >= 4], 0 if i == 4 else first
        rows, d = g_ref.shape[2:]
        pieces = w_ref.shape[1] * w_ref.shape[2] // (rows * d)
        for p in range(pieces):
            cut = lambda size: slice(p * size, p * size + size)
            at = (0, every, cut(d)) if w_ref.shape[2] > d else (0, cut(rows), every)
            g = g_ref[0, first + p].astype(F32)
            m = 0.9 * m_ref[at] + 0.1 * g
            v = 0.95 * v_ref[at] + 0.05 * g * g
            w = w_ref[at].astype(F32)
            outs[i][at] = (w - 0.02 * (m * lax.rsqrt(v + 1e-8) + 0.1 * w)).astype(BF16)
            outs[7 + i][at] = m
            outs[14 + i][at] = v
        first += pieces


def adamw(sums, weights, ms, vs):
    spec = lambda a: pl.BlockSpec((1, *a.shape[1:]), lambda i: (i, *[0] * (a.ndim - 1)))
    state = (*weights, *ms, *vs)
    return pl.pallas_call(
        _adamw,
        grid=(weights[0].shape[0],),
        in_specs=[spec(a) for a in (*sums, *state)],
        out_specs=[spec(a) for a in state],
        out_shape=[jax.ShapeDtypeStruct(a.shape, a.dtype) for a in state],
        compiler_params=comm_params(None),
        cost_estimate=cost(20 * sum(a.size for a in weights), *state, *state),
        name="adamw",
    )(*sums, *state)


def solution(mesh):
    axis, n = "dp", mesh.shape["dp"]

    def step(x, dy, *arrays):
        weights, ms, vs = (arrays[i : i + 7] for i in (0, 7, 14))
        d, ff = x.shape[2], weights[4].shape[2]
        *kept, h1, hs, w = forward(x, weights, axis, n, 4 + 3 * ff // d, 0)
        return tuple(adamw(backward(dy, kept, h1, hs, w, axis, 1), weights, ms, vs))

    states, cut = P(("rep", "dp"), None, None), P(None, "dp", None)
    return jax.shard_map(
        step,
        mesh=mesh,
        in_specs=(states, states) + (cut,) * 21,
        out_specs=(P("rep", "dp", None),) * 21,
        check_vma=False,
    )
```

```python
import functools
import itertools

import jax
import jax.numpy as jnp
import numpy as np
from jax import lax
from jax.experimental import pallas as pl
from jax.experimental.pallas import tpu as pltpu
from jax.sharding import PartitionSpec as P

F32, BF16 = jnp.float32, jnp.bfloat16
HEAD = 128
THETA = 10000
NEG = -1e30
HIDDEN = 2 * NEG
LOG2E = 1.4426950408889634
VMEM = 62 * 2**20


def contract(a, b, ca, cb):
    return lax.dot_general(a, b, (((ca,), (cb,)), ((), ())), preferred_element_type=F32)


def dot(a, b):
    return contract(a, b, 1, 0)


def dot_t(a, b):
    return contract(a, b, 1, 1)


def comm_params(number):
    return pltpu.CompilerParams(dimension_semantics=("arbitrary",), vmem_limit_bytes=VMEM, collective_id=number, has_side_effects=number is not None)


def cost(flops, *arrays, exps=0):
    return pl.CostEstimate(flops=flops, transcendentals=exps, bytes_accessed=sum(a.size * a.dtype.itemsize for a in arrays))


def once(shape, index):
    return pl.BlockSpec(shape, index, pipeline_mode=pl.Buffered(1))


def fixed(*index):
    return lambda i: index


def held(a):
    return once(a.shape, fixed(*[0] * a.ndim))


def resident(a):
    return pl.BlockSpec(a.shape, fixed(*[0] * len(a.shape)))


ANYWHERE = pl.BlockSpec(memory_space=pl.ANY)


def inverse_rms(wide):
    return lax.rsqrt(jnp.mean(wide * wide, -1, keepdims=True) + 1e-6)


def sigmoid(x):
    return 1 / (1 + jnp.exp(-x))


def lower(keys, queries):
    place = lambda dim: lax.broadcasted_iota(jnp.int32, (keys, queries), dim)
    return place(1) >= place(0)


def due(timed, step, place):
    if isinstance(place, int):
        timed = [t for t in timed if t[1] == place]
    for at in sorted({t[0] for t in timed}):

        @pl.when(step == at)
        def _():
            for first, second, run in timed:
                if first == at:
                    run() if isinstance(place, int) else pl.when(place == second)(run)


class Ring:
    def __init__(self, axis):
        n, me = lax.axis_size(axis), lax.axis_index(axis)
        chip, core = lax.div(me, 2), lax.rem(me, 2)
        self.axis, self.me, self.far = axis, me, n // 4
        steps = range(-self.far, self.far + 1)
        chips = [2 * lax.rem(chip + by + n // 2, n // 2) for by in steps]
        self.own = {by: at + core for by, at in zip(steps, chips)}
        self.other = {by: at + 1 - core for by, at in zip(steps, chips)}

    def meet(self):
        barrier = pltpu.get_barrier_semaphore()
        for to in (self.own[1], self.own[-1], self.other[0]):
            pl.semaphore_signal(barrier, inc=1, device_id={self.axis: to}, device_id_type=pl.DeviceIdType.MESH)
        pl.semaphore_wait(barrier, 3)

    def copy(self, src, dst, sems, at, to):
        return pltpu.make_async_remote_copy(src, dst, sems.at[0, at], sems.at[1, at], device_id={self.axis: to}, device_id_type=pl.DeviceIdType.MESH)


class Gather:
    def __init__(self, ring, w_ref, first, pieces, sems, base):
        far, half = ring.far, pieces // 2
        every = slice(first, first + pieces)
        part = lambda number, way: every if number < far else slice(first, first + half) if way == 1 else slice(first + half, first + pieces)
        self.hops = [(number, way) for number in range(1, far + 1) for way in (1, -1)]
        self.table = {hop: (ring.own[hop[1]], ring.own[(1 - hop[0]) * hop[1]], ring.own[-hop[0] * hop[1]], part(*hop)) for hop in self.hops}
        for number, way in [(0, 1), *self.hops]:
            at = -number * way
            self.table["core", number, way] = ring.other[0], ring.own[at], ring.other[at], part(number, way)
        self.index = {key: base + at for at, key in enumerate(self.table)}
        self.ring, self.w_ref, self.sems = ring, w_ref, sems

    def copy(self, key, comes=False):
        to, sent, arriving, part = self.table[key]
        dst = self.w_ref.at[arriving if comes else sent, part]
        return self.ring.copy(dst, dst, self.sems, self.index[key], to)

    def begin(self):
        for way in (1, -1):
            self.copy((1, way)).start()
        self.copy(("core", 0, 1)).start()

    def step(self, number):
        for way in (1, -1):
            self.copy((number, way), True).wait_recv()
            if number < self.ring.far:
                self.copy((number + 1, way)).start()
            self.copy(("core", number, way)).start()

    def arrive(self):
        for key in self.table:
            if key[0] == "core":
                self.copy(key, True).wait_recv()

    def sent(self):
        for key in self.table:
            self.copy(key).wait_send()


def gather_copies(n):
    return 2 * 2 * (n // 4) + 1


PLACES = 64


def rotary_parts(tokens):
    half = HEAD // 2
    place = np.concatenate([np.arange(PLACES), np.arange(0, tokens, PLACES)]).astype(np.float32)
    angle = place[:, None] * np.float32(THETA) ** (-np.arange(half, dtype=np.float32) / half)
    return np.stack([np.concatenate([f(angle.astype(np.float64))] * 2, axis=1) for f in (np.cos, np.sin)]).astype(np.float32)


def tables(table_ref, first, count):
    near_cos, near_sin = table_ref[0, :PLACES], table_ref[1, :PLACES]
    sign = jnp.where(lax.broadcasted_iota(jnp.int32, (1, HEAD), 1) < HEAD // 2, -1.0, 1.0)
    cos, sin = [], []
    for i in range(count):
        far_cos, far_sin = (table_ref[f, pl.ds(PLACES + first + i, 1)] for f in range(2))
        cos.append(near_cos * far_cos - near_sin * far_sin)
        sin.append((near_sin * far_cos + near_cos * far_sin) * sign)
    return jnp.concatenate(cos), jnp.concatenate(sin)


class Forward:
    def __init__(self, layers, blocks):
        self.layers, self.blocks = layers, blocks
        self.steps = (3 * layers - 1) * blocks

    def at(self, step):
        layer = lax.div(step, 3 * self.blocks)
        return layer, step - 3 * self.blocks * layer

    def block(self, phase):
        return lambda step: (self.at(step)[0], jnp.clip(self.at(step)[1] - phase * self.blocks, 0, self.blocks - 1))


    def points(self):
        durations = {0: 1.6, 1: 1.75, 2: 1.15}
        time, out = 0.0, []
        for step in range(self.steps):
            phase, block = divmod(step % (3 * self.blocks), self.blocks)
            for place in range((1, block + 1, self.blocks)[phase]):
                out.append((time, step, place))
                time += durations[phase]
        return out

    def timed(self, rounds, far):
        hop, delay = 2.8, 2.2
        points, out, link, place = self.points(), [], 0.0, 0

        first_use = lambda job: 3 * self.blocks * job[0] + (2 * self.blocks if job[1] else 0)
        missing = [job for jobs in rounds for job in jobs]

        def add(time, kind, number, job):
            nonlocal place
            limit = min(map(first_use, missing))
            while place < len(points) - 1 and points[place][0] < time and points[place + 1][1:] <= (limit, 0):
                place += 1
            if kind == "arrive":
                missing.remove(job)
            out.append((*points[place][1:], kind, number, job))
            return max(time, points[place][0])

        def send(time, length):
            nonlocal link
            link = max(link, time) + length
            return link + delay

        came = {job: 0.0 for job in rounds[0]}
        for jobs, later in zip(rounds, rounds[1:] + [[]]):
            for number in range(1, far + 1):
                for job in jobs:
                    time = add(came[job], "step", number, job)
                    if number < far:
                        came[job] = send(time, hop if number + 1 < far else hop / 2)
                if number == far - 1:
                    for job in later:
                        came[job] = send(add(link - hop, "begin", 0, job), hop)
            for job in jobs:
                add(came[job] + 1, "arrive", 0, job)
        return out


def _forward(x_ref, table_ref, *rest, plan, scale, axis):
    shards, rest = rest[:7], rest[7:]
    q_ref, k_ref, v_ref, o_ref, lse_ref, at_ref, ot_ref, h1_ref, hs_ref, w_ref = rest[:10]
    w_s, h_s, q_s, k_s, v_s, top_s, mix_s, x_sem, w_sems, ring_sems = rest[10:]
    step = pl.program_id(0)
    blocks = plan.blocks
    layer, within = plan.at(step)
    bq, width = q_ref.shape[1:]
    n, pieces, rows, _ = w_s.shape[1:]
    group = 4
    heads = width // HEAD
    e = scale * LOG2E
    ring = Ring(axis)
    jobs = {}
    for number in range(plan.layers):
        for first in range(0, pieces, group):
            jobs[number, first // group] = Gather(ring, w_s.at[number], first, group, ring_sems, gather_copies(n) * len(jobs))

    def put(key):
        number, first = key[0], key[1] * group
        cut = lambda ref: ref.at[number, :, first : first + group]
        return pltpu.make_async_copy(cut(w_s), cut(w_ref), w_sems.at[number, key[1]])

    def event(kind, number, key):
        job = jobs[key]
        if kind == "begin":
            job.begin()
        elif kind == "step":
            job.step(number)
        else:
            job.arrive()
            put(key).start()

    groups = pieces // group
    rounds = [[(0, at) for at in range(1, groups)]]
    for number in range(1, plan.layers):
        rounds += [[(number, at), (number, at + 1)] for at in range(0, groups, 2)]
    timed = [(*t[:2], functools.partial(event, *t[2:])) for t in plan.timed(rounds, ring.far)]

    def events(phase, place):
        due([t for t in timed if t[0] % (3 * blocks) // blocks == phase], step, place)

    def pack(number, first):
        at = 0
        for shard in shards:
            for row in range(0, shard.shape[1], rows):
                for column in range(0, shard.shape[2], width):
                    if first <= at < first + group:
                        w_s[number, ring.me, at] = shard[number, row : row + rows, column : column + width]
                    at += 1

    @pl.when(step == 0)
    def _():
        x_copy = pltpu.make_async_copy(x_ref.at[0], h_s, x_sem)
        x_copy.start()
        pack(0, 0)
        ring.meet()
        jobs[0, 0].begin()
        for key in list(jobs)[1:]:
            pack(key[0], key[1] * group)
        for number in range(1, ring.far + 1):
            if number < pieces // group:
                jobs[0, number].begin()
            jobs[0, 0].step(number)
        event("arrive", 0, (0, 0))
        x_copy.wait()

    @pl.when(within < blocks)
    def _():
        events(0, 0)
        here = pl.ds(pl.multiple_of(within * bq, bq), bq)
        hs_ref[0] = h_s[here, :]
        wide = h_s[here, :].astype(F32)
        a = (wide * inverse_rms(wide)).astype(BF16)
        at_ref[0] = a.T
        cos, sin = tables(table_ref, within * (bq // PLACES), bq // PLACES)
        for piece, (out_ref, kept) in enumerate(((q_ref, q_s), (k_ref, k_s), (v_ref, v_s))):
            y = dot(a, w_s[layer, :, piece].reshape(width, width)).astype(BF16)
            if piece < 2:
                turned = []
                for at in range(0, width, HEAD):
                    t = y[:, at : at + HEAD].astype(F32)
                    turned.append((t * cos + pltpu.roll(t, HEAD // 2, 1) * sin).astype(BF16))
                y = jnp.concatenate(turned, 1)
            out_ref[0] = y
            kept[here, :] = y

    @pl.when((within >= blocks) & (within < 2 * blocks))
    def _():
        b = within - blocks
        first = pl.multiple_of(b * bq, bq)
        top_s[:] = jnp.full_like(top_s, NEG)
        mix_s[:] = jnp.zeros_like(mix_s)

        def block(at, keys, strips, gap):
            here = pl.ds(at, keys)
            ones = jnp.ones((8, keys), BF16)
            work = [(m, a, w) for m in range(heads) for a, w in strips]
            scores = [dot_t(k_s[here, m * HEAD : (m + 1) * HEAD], q_s[pl.ds(first + a, w), m * HEAD : (m + 1) * HEAD]) for m, a, w in work]
            weights, keeps = [], []
            for (m, a, w), s in zip(work, scores):
                if gap == a:
                    s = jnp.where(lower(keys, w), s, HIDDEN)
                old = top_s[m : m + 1, a : a + w]
                top = jnp.maximum(old, s.max(axis=0, keepdims=True))
                top_s[m : m + 1, a : a + w] = top
                weights.append(jnp.exp2((s - top) * e).astype(BF16))
                keeps.append(jnp.exp2((old - top) * e))
            for (m, a, w), p, keep in zip(work, weights, keeps):
                values = jnp.concatenate([v_s[here, m * HEAD : (m + 1) * HEAD].T, ones])
                mix_s[m, :, a : a + w] = mix_s[m, :, a : a + w] * keep + dot(values, p)

        def before(j, _):
            events(1, j)
            block(pl.multiple_of(j * bq, bq), bq, [(0, bq)], None)

        lax.fori_loop(0, b, before, None)
        events(1, b)
        half = bq // 2
        block(first, half, [(0, half), (half, half)], 0)
        block(pl.multiple_of(first + half, half), half, [(half, half)], half)
        for m in range(heads):
            top, total = top_s[m : m + 1, :], mix_s[m, HEAD : HEAD + 1, :]
            part = (mix_s[m, :HEAD, :] * (1 / total)).astype(BF16)
            ot_ref[0, m * HEAD : (m + 1) * HEAD, :] = part
            o_ref[0, :, m * HEAD : (m + 1) * HEAD] = part.T
            lse_ref[0, m : m + 1, :] = top * e + jnp.log2(total)
        here = pl.ds(first, bq)
        h1 = h_s[here, :] + dot(o_ref[0], w_s[layer, :, 3].reshape(width, width)).astype(BF16)
        h_s[here, :] = h1
        h1_ref[0] = h1

    @pl.when(within >= 2 * blocks)
    def _():
        here = pl.ds(pl.multiple_of((within - 2 * blocks) * bq, bq), bq)
        wide = h_s[here, :].astype(F32)
        b = (wide * inverse_rms(wide)).astype(BF16)
        parts = (pieces - group) // 3
        owners = n // parts
        y = None
        for j in range(parts):
            events(2, j)
            gate = dot(b, w_s[layer, :, group + j].reshape(width, width))
            up = dot(b, w_s[layer, :, group + parts + j].reshape(width, width))
            act = (gate * sigmoid(gate) * up).astype(BF16)
            part = dot(act, w_s[layer, owners * j : owners * (j + 1), group + 2 * parts :].reshape(width, width))
            y = part if y is None else y + part
        h_s[here, :] += y.astype(BF16)

    @pl.when(step == plan.steps - 1)
    def _():
        for key, job in jobs.items():
            job.sent()
            put(key).wait()


def forward(x, shards, axis, n, pieces, number, bq=512):
    _, s, d = x.shape
    layers, rows = shards[0].shape[:2]
    heads, plan = d // HEAD, Forward(layers, s // bq)
    table = rotary_parts(s)
    block = lambda index: pl.BlockSpec((1, bq, d), lambda i: (*index(i), 0))
    across = lambda height, index: pl.BlockSpec((1, height, bq), lambda i: (index(i)[0], 0, index(i)[1]))
    flat = jax.ShapeDtypeStruct((layers, d, s), BF16)
    out = jax.ShapeDtypeStruct((layers, s, d), BF16)
    weights = (layers, n, pieces, rows, d)
    return pl.pallas_call(
        functools.partial(_forward, plan=plan, scale=HEAD**-0.5, axis=axis),
        grid=(plan.steps,),
        in_specs=[ANYWHERE, held(table), *[held(a) for a in shards]],
        out_specs=[block(plan.block(0))] * 3 + [block(plan.block(1)), across(heads, plan.block(1)), across(d, plan.block(0)), across(d, plan.block(1)),
                   block(plan.block(1)), block(plan.block(0)), ANYWHERE],
        out_shape=[out] * 4 + [jax.ShapeDtypeStruct((layers, heads, s), F32), flat, flat, out, out, jax.ShapeDtypeStruct(weights, BF16)],
        scratch_shapes=[pltpu.VMEM(weights, BF16)] + [pltpu.VMEM((s, d), BF16)] * 4
        + [pltpu.VMEM((heads, bq), F32), pltpu.VMEM((heads, HEAD + 8, bq), F32), pltpu.SemaphoreType.DMA, pltpu.SemaphoreType.DMA((layers, pieces // 4)),
           pltpu.SemaphoreType.DMA((2, layers * (pieces // 4) * gather_copies(n)))],
        compiler_params=comm_params(number),
        cost_estimate=cost(layers * (s * s * d + 32 * s * d * d), *[x] * 8, exps=layers * heads * s * s // 2),
        name="forward",
    )(x, table, *shards)


class Scatter:
    def __init__(self, ring, dw, out, core_s, come_s, core_sems, hop_sems):
        far, pieces = ring.far, dw.shape[1]
        halves = (slice(0, pieces // 2), slice(pieces // 2, pieces))
        targets = [far] + [way * by for by in range(far - 1, 0, -1) for way in (1, -1)] + [0]
        slot = {by: at for at, by in enumerate(targets)} | {-far: 0}
        ways = lambda number, half: (1, -1) if number > 1 else (1 - 2 * half,)
        hops = [(number, half, way) for number in range(1, far + 1) for half in (0, 1) for way in ways(number, half)]
        index = {hop: at for at, hop in enumerate(hops)}

        def share(by):
            return ring.copy(dw.at[ring.other[by]], core_s.at[slot[by]], core_sems, slot[by], ring.other[0])

        def going(hop):
            number, half, way = hop
            return dw.at[ring.own[way * (far - number + 1)], halves[half]]

        def move(hop):
            return ring.copy(going(hop), come_s.at[index[hop]], hop_sems, index[hop], ring.own[hop[2]])

        def total(dst, by, half, came):
            first = halves[half].start
            some = next(k for k in (3, 2, 1) if pieces // 2 % k == 0)

            def add(i, _):
                for p in (i * some + at for at in range(some)):
                    terms = [dw[ring.own[by], first + p], core_s[slot[by], first + p]] + [come_s[index[hop], p] for hop in came]
                    dst[p] = sum(x.astype(F32) for x in terms).astype(BF16)

            lax.fori_loop(0, pieces // 2 // some, add, None)

        def begin():
            for by in targets[:3]:
                share(by).start()

        def step(number, half):
            if half == 0:
                for at in sorted({slot[way * (far - number + 1)] for way in (1, -1)}):
                    share(targets[at]).wait_recv()
            for way in ways(number, half):
                came = [hop for hop in [(number - 1, half, way)] if hop in index]
                for hop in came:
                    move(hop).wait_recv()
                total(going((number, half, way)), way * (far - number + 1), half, came)
            for way in ways(number, half):
                move((number, half, way)).start()
            if half == 1:
                for by in targets[2 * number + 1 : 2 * number + 3]:
                    share(by).start()

        def finish(half):
            if half == 0:
                share(0).wait_recv()
            came = [(far, half, way) for way in (1, -1)]
            for hop in came:
                move(hop).wait_recv()
            total(out.at[halves[half]], 0, half, came)

        def end():
            for hop in hops:
                move(hop).wait_send()
            for by in targets:
                share(by).wait_send()

        self.events = [begin] + [functools.partial(step, number, half) for number in range(1, far + 1) for half in (0, 1)]
        self.events += [functools.partial(finish, half) for half in (0, 1)] + [end]

    @staticmethod
    def scratch(n, pieces, rows, d):
        hops = 2 + 4 * (n // 4 - 1)
        whole, half = (pltpu.VMEM((count, share, rows, d), BF16) for count, share in ((n // 2, pieces), (hops, pieces // 2)))
        return [whole, half, pltpu.SemaphoreType.DMA((2, n // 2)), pltpu.SemaphoreType.DMA((2, hops))]


def norm_back(wide, by_normed):
    r = inverse_rms(wide)
    normed = wide * r
    return r * (by_normed - normed * jnp.mean(normed * by_normed, -1, keepdims=True))


class Backward:
    def __init__(self, layers, hidden, blocks):
        self.layers, self.hidden, self.blocks = layers, hidden, blocks
        self.per = hidden + 2 * blocks

    def at(self, step):
        turn = lax.div(step, self.per)
        return self.layers - 1 - turn, step - self.per * turn

    def block(self, first):
        return lambda step: (self.at(step)[0], jnp.clip(self.at(step)[1] - first, 0, self.blocks - 1))

    def weights(self, step):
        layer, within = self.at(step)
        return jnp.where(within < self.hidden, layer, jnp.maximum(layer - 1, 0)), jnp.where(within < self.hidden, within, 0)


def _backward(dy_ref, h1_all, wg_ref, wu_ref, wd_ref, q_ref, k_ref, v_ref, o_ref, lse_ref, at_ref, ot_ref, h_ref, w_ref, table_ref, ga_ref, gf_ref,
              h1_ref, wa_ref, dh_s, lhs_s, rhs_s, sum_s, dv_s, dq_s, do_s, delta_s, dwa_s, dwf_s, load_sems, *scratch, plan, scale, axis):
    step = pl.program_id(0)
    layer, within = plan.at(step)
    hidden, blocks = plan.hidden, plan.blocks
    s, d = h1_ref.shape
    t = bq = s // blocks
    n, _, rows, _ = dwa_s.shape
    heads = d // HEAD
    e = scale * LOG2E
    cuts = [slice(m * HEAD, (m + 1) * HEAD) for m in range(heads)]
    flat = lambda w: w.reshape(d, d)
    rows_of = lambda block: slice(block * t, block * t + t) if isinstance(block, int) else pl.ds(pl.multiple_of(block * t, t), t)
    first_lhs, second_lhs = lhs_s.at[0], lhs_s.at[1]
    b_s, act_s, dup_s, dgate_s = (rhs_s.at[i] for i in range(4))
    dqs_s, k_s, v_s, was_s = b_s, act_s, dup_s, dgate_s

    ring = Ring(axis)
    third = len(scratch) // 3
    inside = [(hidden + b, place) for b in range(blocks) for place in range(b + 1)]
    after = [(hidden + blocks + b, 0) for b in range(blocks)]
    before = [(j, place) for j in range(hidden) for place in range(2)]

    def sums(layer):
        parts = ((dwa_s.at[:, :2], ga_ref.at[layer, :2]), (dwa_s.at[:, 2:], ga_ref.at[layer, 2:]), (dwf_s, gf_ref.at[layer]))
        return [Scatter(ring, *part, *scratch[third * i : third * (i + 1)]).events for i, part in enumerate(parts)]

    _, of_vo, of_f = sums(layer)
    soon_f, soon_vo = range(9), range(3)
    timed_f = [(*(inside + after)[max(i > 0, (3 * i - 3) // 2)], of_f[i]) for i in soon_f] + [(*after[1 + 2 * (i > 0)], of_vo[i]) for i in soon_vo]

    def later(layer):
        of_qk, of_vo, of_f = sums(layer)
        return itertools.zip_longest(of_qk, of_f[len(soon_f) :] + of_vo[len(soon_vo) :], fillvalue=lambda: None)

    timed_a = [(*before[2 * i // 3], event) for i, pair in enumerate(later(jnp.minimum(layer + 1, plan.layers - 1))) for event in pair]
    due_inside = lambda place: due([x for x in timed_f if x[:2] in inside], within, place)

    def due_before(place):
        @pl.when(layer < plan.layers - 1)
        def _():
            due(timed_a, within, place)

    def load(src, dst, at):
        return pltpu.make_async_copy(src, dst, load_sems.at[at])

    def loads():
        pairs = ((k_ref, k_s), (v_ref, v_s), (at_ref, first_lhs), (ot_ref, second_lhs))
        return [load(src.at[layer], dst, at) for at, (src, dst) in enumerate(pairs)]

    attention_weights = lambda: load(w_ref.at[layer, :, : wa_ref.shape[1]], wa_ref, 4)
    states = lambda layer: load(h1_all.at[layer], h1_ref, 5)

    @pl.when(step == 0)
    def _():
        copy = load(dy_ref.at[0], dh_s, 0)
        copy.start()
        states(layer).start()
        ring.meet()
        copy.wait()

    @pl.when(within < hidden)
    def _():
        j = within
        due_before(0)
        wg, wu, wd = (flat(r[:]) for r in (wg_ref, wu_ref, wd_ref))

        @pl.when(j == 0)
        def _():
            attention_weights().start()
            states(layer).wait()

            def strip(i, _):
                here = rows_of(i)
                wide = h1_ref[here, :].astype(F32)
                b = (wide * inverse_rms(wide)).astype(BF16)
                b_s[here, :] = b
                first_lhs[:, here] = b.T
                second_lhs[:, here] = dh_s[here, :].T
                sum_s[here, :] = jnp.zeros((t, d), F32)

            lax.fori_loop(0, blocks, strip, None)

        def products(here):
            b = b_s[here, :]
            return dot(b, wg), dot(b, wu), dot_t(dh_s[here, :], wd).astype(BF16)

        def bends(here, gate, up, dact):
            dact = dact.astype(F32)
            sig = sigmoid(gate)
            silu = gate * sig
            act_s[here, :] = (silu * up).astype(BF16)
            dup_s[here, :] = (dact * silu).astype(BF16)
            dgate_s[here, :] = (dact * up * (sig + silu * (1 - sig))).astype(BF16)

        def pass_on(here):
            sum_s[here, :] += dot_t(dgate_s[here, :], wg) + dot_t(dup_s[here, :], wu)

        made = {}
        for at in range(blocks + 2):
            if at < blocks:
                made[at] = products(rows_of(at))
            if 1 <= at <= blocks:
                bends(rows_of(at - 1), *made.pop(at - 1))
            if at >= 2:
                pass_on(rows_of(at - 2))
        due_before(1)

        def gradients(i, _):
            dwf_s[:, i * hidden + j] = dot(first_lhs[:], rhs_s[3 - i]).astype(BF16).reshape(n, rows, d)

        lax.fori_loop(0, 2, gradients, None)
        part = n // hidden
        dwf_s[pl.ds(j * part, part), 2 * hidden :] = dot(second_lhs[:], act_s[:]).T.astype(BF16).reshape(part, hidden, rows, d)

        @pl.when(j == hidden - 1)
        def _():
            for copy in loads():
                copy.start()

            def strip(i, _):
                here = rows_of(i)
                grad = norm_back(h1_ref[here, :].astype(F32), sum_s[here, :].astype(BF16).astype(F32))
                dh_s[here, :] = (dh_s[here, :].astype(F32) + grad).astype(BF16)

            lax.fori_loop(0, blocks, strip, None)
            for copy in (*loads()[:2], attention_weights()):
                copy.wait()
            pl.when(layer > 0)(lambda: states(layer - 1).start())

    @pl.when((within >= hidden) & (within < hidden + blocks))
    def _():
        i = within - hidden
        first = pl.multiple_of(i * bq, bq)
        mine = pl.ds(first, bq)
        dq_s[:] = jnp.zeros_like(dq_s)
        do = dot_t(dh_s[mine, :], flat(wa_ref[:, 3])).astype(BF16)
        do_s[:] = do
        for m, cut in enumerate(cuts):
            delta_s[m : m + 1, :] = (do[:, cut].astype(F32) * o_ref[:, cut].astype(F32)).T.sum(axis=0, keepdims=True)

        def block(at, keys, strips, gap):
            here = pl.ds(at, keys)
            work = [(cut, m, a, w) for m, cut in enumerate(cuts) for a, w in strips]
            scores = [dot_t(k_s[here, cut], q_ref[a : a + w, cut]) for cut, m, a, w in work]
            dps = [dot_t(v_s[here, cut], do_s[a : a + w, cut]) for cut, m, a, w in work]
            for (cut, m, a, w), score, dp in zip(work, scores, dps):
                p = jnp.exp2(score * e - lse_ref[m : m + 1, a : a + w])
                if gap == a:
                    p = jnp.where(lower(keys, w), p, 0.0)
                ds = (p * (dp - delta_s[m : m + 1, a : a + w])).astype(BF16)
                by_v, by_k = dot(p.astype(BF16), do_s[a : a + w, cut]), dot(ds, q_ref[a : a + w, cut])
                if gap == a:
                    dv_s[here, cut] = by_v
                    sum_s[here, cut] = by_k
                else:
                    dv_s[here, cut] += by_v
                    sum_s[here, cut] += by_k
                dq_s[m, :, a : a + w] += dot(k_s[here, cut].T, ds)

        def earlier(j, _):
            due_inside(j)
            block(pl.multiple_of(j * bq, bq), bq, [(0, bq)], None)

        lax.fori_loop(0, i, earlier, None)
        due_inside(i)
        half = bq // 2
        block(first, half, [(0, half), (half, half)], 0)
        block(pl.multiple_of(first + half, half), half, [(half, half)], half)
        for m, cut in enumerate(cuts):
            dqs_s[mine, cut] = (dq_s[m] * scale).T.astype(BF16)

    @pl.when(within >= hidden + blocks)
    def _():
        b = within - hidden - blocks
        due([x for x in timed_f if x[:2] in after], within, 0)
        here = rows_of(b)

        @pl.when(b == 0)
        def _():
            for copy in loads()[2:]:
                copy.wait()

            def strip(i, _):
                rhs_s[2, rows_of(i), :] = dv_s[rows_of(i), :].astype(BF16)
                was_s[rows_of(i), :] = dh_s[rows_of(i), :]

            lax.fori_loop(0, blocks, strip, None)

            def gradients(i, _):
                dwa_s[:, 2 + i] = dot(lhs_s[i], rhs_s[2 + i]).astype(BF16).reshape(n, rows, d)

            lax.fori_loop(0, 2, gradients, None)

        cos, sin = tables(table_ref, b * (bq // PLACES), bq // PLACES)
        for p, x in enumerate((dqs_s[here, :], (sum_s[here, :] * scale).astype(BF16))):
            for cut in cuts:
                part = x[:, cut].astype(F32)
                rhs_s[p, here, cut] = (part * cos - pltpu.roll(part, HEAD // 2, 1) * sin).astype(BF16)

        @pl.when(layer > 0)
        def _():
            by_a = sum(dot_t(rhs_s[p, here, :], flat(wa_ref[:, p])) for p in range(3)).astype(BF16).astype(F32)
            dh_s[here, :] = (dh_s[here, :].astype(F32) + norm_back(h_ref[:].astype(F32), by_a)).astype(BF16)

        @pl.when(b == blocks - 1)
        def _():
            def gradients(p, _):
                dwa_s[:, p] = dot(first_lhs[:], rhs_s[p]).astype(BF16).reshape(n, rows, d)

            lax.fori_loop(0, 2, gradients, None)

    @pl.when(step == plan.layers * plan.per - 1)
    def _():
        for event in itertools.chain(*later(0)):
            event()


def backward(dy, kept, h1, hs, w, axis, number, bq=512):
    layers, s, d = hs.shape
    _, n, pieces, rows, _ = w.shape
    own = 4
    heads, hidden, blocks = d // HEAD, (pieces - own) // 3, s // bq
    part = n // hidden
    plan = Backward(layers, hidden, blocks)
    table = rotary_parts(s)
    row = lambda first: pl.BlockSpec((None, bq, d), lambda i: (*plan.block(first)(i), 0))
    column = lambda first: pl.BlockSpec((None, n, 1, rows, d), lambda i: (plan.weights(i)[0], 0, first + plan.weights(i)[1], 0, 0))
    lse = lambda i: (plan.block(hidden)(i)[0], 0, plan.block(hidden)(i)[1])
    sums = [jax.ShapeDtypeStruct((layers, count, rows, d), BF16) for count in (own, pieces - own)]
    state, terms = pltpu.VMEM((s, d), F32), [(n, count, rows, d) for count in (own, pieces - own)]
    return pl.pallas_call(
        functools.partial(_backward, plan=plan, scale=HEAD**-0.5, axis=axis),
        grid=(layers * plan.per,),
        in_specs=[ANYWHERE, ANYWHERE, column(own), column(own + hidden),
                  pl.BlockSpec((None, part, hidden, rows, d), lambda i: (plan.weights(i)[0], plan.weights(i)[1], pieces // hidden - 1, 0, 0)),
                  row(hidden), ANYWHERE, ANYWHERE, row(hidden), pl.BlockSpec((None, heads, bq), lse), ANYWHERE, ANYWHERE, row(hidden + blocks),
                  ANYWHERE, held(table)],
        out_specs=[*map(resident, sums)],
        out_shape=sums,
        scratch_shapes=[pltpu.VMEM((s, d), BF16), pltpu.VMEM(terms[0], BF16), pltpu.VMEM((s, d), BF16), pltpu.VMEM((2, d, s), BF16), pltpu.VMEM((4, s, d), BF16), state, state,
                        pltpu.VMEM((heads, HEAD, bq), F32), pltpu.VMEM((bq, d), BF16), pltpu.VMEM((heads, bq), F32)]
        + [pltpu.VMEM(shape, BF16) for shape in terms] + [pltpu.SemaphoreType.DMA((6,))]
        + [x for count in (2, own - 2, pieces - own) for x in Scatter.scratch(n, count, rows, d)],
        compiler_params=comm_params(number),
        cost_estimate=cost(layers * (5 * s * s * d + 80 * s * d * d), *[dy] * 16, exps=layers * heads * s * s),
        name="backward",
    )(dy, h1, w, w, w, *kept, hs, w, table)


def _adamw(*refs):
    sums, w_refs, m_refs, v_refs, outs = refs[:2], refs[2:9], refs[9:16], refs[16:23], refs[23:]
    first, every = 0, slice(None)
    for i, (w_ref, m_ref, v_ref) in enumerate(zip(w_refs, m_refs, v_refs)):
        g_ref, first = sums[i >= 4], 0 if i == 4 else first
        rows, d = g_ref.shape[2:]
        pieces = w_ref.shape[1] * w_ref.shape[2] // (rows * d)
        for p in range(pieces):
            cut = lambda size: slice(p * size, p * size + size)
            at = (0, every, cut(d)) if w_ref.shape[2] > d else (0, cut(rows), every)
            g = g_ref[0, first + p].astype(F32)
            m = 0.9 * m_ref[at] + 0.1 * g
            v = 0.95 * v_ref[at] + 0.05 * g * g
            w = w_ref[at].astype(F32)
            outs[i][at] = (w - 0.02 * (m * lax.rsqrt(v + 1e-8) + 0.1 * w)).astype(BF16)
            outs[7 + i][at] = m
            outs[14 + i][at] = v
        first += pieces


def adamw(sums, weights, ms, vs):
    spec = lambda a: pl.BlockSpec((1, *a.shape[1:]), lambda i: (i, *[0] * (a.ndim - 1)))
    state = (*weights, *ms, *vs)
    return pl.pallas_call(
        _adamw,
        grid=(weights[0].shape[0],),
        in_specs=[spec(a) for a in (*sums, *state)],
        out_specs=[spec(a) for a in state],
        out_shape=[jax.ShapeDtypeStruct(a.shape, a.dtype) for a in state],
        compiler_params=comm_params(None),
        cost_estimate=cost(sum(a.size for a in state), *state, *state),
        name="adamw",
    )(*sums, *state)


def solution(mesh):
    axis, n = "dp", mesh.shape["dp"]

    def step(x, dy, *arrays):
        weights, ms, vs = (arrays[i : i + 7] for i in (0, 7, 14))
        d, ff = x.shape[2], weights[4].shape[2]
        *kept, h1, hs, w = forward(x, weights, axis, n, 4 + 3 * ff // d, 0)
        return tuple(adamw(backward(dy, kept, h1, hs, w, axis, 1), weights, ms, vs))

    states, cut = P(("rep", "dp"), None, None), P(None, "dp", None)
    return jax.shard_map(
        step,
        mesh=mesh,
        in_specs=(states, states) + (cut,) * 21,
        out_specs=(P("rep", "dp", None),) * 21,
        check_vma=False,
    )
```
